128 devices in a mesh: patch: 32 (over x, z, core), grp: 4 (over y).
Axes of the slice: x: 4, y: 4, z: 4, core: 2. Of those that a mesh axis runs over, the one named last changes fastest.
Arguments:
- previous: float32 [4, 32, 12, 21, 256], P('grp', 'patch'), may hold values from -4 to 4
- predicted: float32 [4, 32, 12, 21, 256], P('grp', 'patch'), may hold values from -4 to 4
- new_owner: int32 [4, 32, 12], replicated, may hold values from 0 to 31, as said below
- levels: int32 [4, 32, 12], replicated, may hold values from 0 to 2
- diffusion: float32 [21], replicated, may hold values from 0.05 to 0.5
- decay: float32 [21], replicated, may hold values from 0.1 to 1
- reaction: float32 [21, 21], replicated, may hold values from -1.25 to 1.25
Outputs:
- solution: float32 [4, 32, 16, 21, 256], P('grp', 'patch')
The draws below stay inside these ranges and needn't reach their ends.
Inputs may be any that keep to these rules, and one draw needn't show every extreme that they name: new_owner[b, o, s] is o, except that a patch of the last column of an owner o < 31 may get o + 1 and a patch of the first column of an owner o > 0 may get o - 1; at most 2 patches of one owner get o + 1 and at most 2 get o - 1; owner (0, 0) hands exactly 2 to o + 1 and owner (0, 31) exactly 2 to o - 1.
All inputs are finite; a program needn't handle non-finite values.
Results may differ from the reference program's by a relative error of at most 0.0003.
Values sent between devices are 32-bit elements; how exact they have to be, the bound alone decides.
No kernel may reach another device: no remote copies, remote signals or barrier semaphores. Data moves between devices by JAX's collectives and lax.ppermute only.
A program may use at most 128 MiB of HBM per device.

```python
import math
import jax
import jax.numpy as jnp
from jax import lax

SPECIES = 21
CELLS = 16
ROWS_DEV = 4
COLS_DEV = 3
MOVE_CAP = 2
KRYLOV = 3
NEWTON = 2
PATCH_DEV = 12
BANDS = 4
OWNERS = 32


def draw_new_owner(key, part):
    key_right = jax.random.fold_in(key, 11)
    key_left = jax.random.fold_in(key, 12)
    key_rank_right = jax.random.fold_in(key, 13)
    key_rank_left = jax.random.fold_in(key, 14)
    owner_line = jnp.arange(OWNERS, dtype=jnp.int32)[None, :]
    right_count = jax.random.randint(key_right, (BANDS, OWNERS), 0, MOVE_CAP + 1)
    left_count = jax.random.randint(key_left, (BANDS, OWNERS), 0, MOVE_CAP + 1)
    right_count = right_count.at[0, 0].set(MOVE_CAP)
    left_count = left_count.at[0, OWNERS - 1].set(MOVE_CAP)
    right_count = jnp.where(owner_line == OWNERS - 1, 0, right_count)
    left_count = jnp.where(owner_line == 0, 0, left_count)

    def ranks_of(subkey):
        scores = jax.random.randint(subkey, (BANDS, OWNERS, ROWS_DEV), 0, 1 << 20) * ROWS_DEV + jnp.arange(ROWS_DEV, dtype=jnp.int32)
        return jnp.argsort(jnp.argsort(scores, axis=-1), axis=-1).astype(jnp.int32)
    right_move = (ranks_of(key_rank_right) < right_count[:, :, None]).astype(jnp.int32)
    left_move = (ranks_of(key_rank_left) < left_count[:, :, None]).astype(jnp.int32)
    offset = jnp.zeros((BANDS, OWNERS, ROWS_DEV, COLS_DEV), jnp.int32)
    offset = offset.at[:, :, :, COLS_DEV - 1].set(right_move)
    offset = offset.at[:, :, :, 0].add(-left_move)
    return (owner_line[:, :, None, None] + offset).reshape(BANDS, OWNERS, ROWS_DEV * COLS_DEV).astype(jnp.int32)


def with_ends(array, own_key, low, largest):
    dims = array.shape
    place = [jax.random.randint(jax.random.fold_in(own_key, axis), (), 0, dims[axis]) for axis in range(len(dims))]
    array = array.at[tuple(place)].set(low)
    longest = dims.index(max(dims))
    place[longest] = (place[longest] + 1) % dims[longest]
    return array.at[tuple(place)].set(largest)


def level_of(key, extent, pieces, low, top_value):
    factor_of, own = 1.0, jax.random.fold_in(key, 6)
    for dim, shards_of in pieces:
        draws = jnp.exp(jax.random.uniform(jax.random.fold_in(own, dim), (shards_of,), jnp.float32, low / len(pieces), top_value / len(pieces)))
        factor_of = factor_of * jnp.repeat(draws, extent[dim] // shards_of).reshape([-1 if axis == dim else 1 for axis in range(len(extent))])
    return factor_of


def normal_values(own_key, shape, scale, reach, cuts=(), kind=jnp.bfloat16):
    array = scale * jax.random.normal(own_key, shape, jnp.float32)
    if cuts:
        array = array * level_of(own_key, shape, cuts, -0.22, 0.18)
    return jnp.clip(array, -reach, reach).astype(kind)


def setup_inputs(seed: int = 0) -> dict:
    arg_keys = jax.random.split(jax.random.key(seed), 8)
    return {
        "previous": normal_values(arg_keys[0], (BANDS, OWNERS, PATCH_DEV, SPECIES, CELLS * CELLS), 1.0, 4.0, ((0, 4), (1, 32)), jnp.float32),
        "predicted": normal_values(arg_keys[1], (BANDS, OWNERS, PATCH_DEV, SPECIES, CELLS * CELLS), 1.0, 4.0, ((0, 4), (1, 32)), jnp.float32),
        "new_owner": draw_new_owner(jax.random.fold_in(arg_keys[7], 71), 0),
        "levels": with_ends(jax.random.randint(arg_keys[3], (BANDS, OWNERS, PATCH_DEV), 0, 3), jax.random.fold_in(arg_keys[3], 1), 0, 2).astype(jnp.int32),
        "diffusion": jnp.clip(jnp.exp(jax.random.uniform(arg_keys[4], (SPECIES,), jnp.float32, math.log(0.05), math.log(0.5))), 0.05, 0.5),
        "decay": jnp.clip(jnp.exp(jax.random.uniform(arg_keys[5], (SPECIES,), jnp.float32, math.log(0.1), math.log(1.0))), 0.1, 1.0),
        "reaction": normal_values(arg_keys[6], (SPECIES, SPECIES), SPECIES ** -0.5, 1.25, (), jnp.float32),
    }


step_rate = 4.0
epsilon = 1e-12
highest = lax.Precision.HIGHEST

def slot_layout(new_owner, device_rows, capacity):
    band_total, owner_total, patch_count = new_owner.shape
    device_cols = patch_count // device_rows
    owner_line = jnp.arange(owner_total, dtype=jnp.int32)[None, :, None]
    offset = new_owner - owner_line
    patch_ids = jnp.arange(band_total * owner_total * patch_count, dtype=jnp.int32).reshape(band_total, owner_total, patch_count)
    staying = jnp.where(offset == 0, patch_ids, -1)
    grid_ids = patch_ids.reshape(band_total, owner_total, device_rows, device_cols)
    grid_off = offset.reshape(band_total, owner_total, device_rows, device_cols)

    def packed(column_at, sign):
        moving = (grid_off[:, :, :, column_at] == sign).astype(jnp.int32)
        ranks = jnp.cumsum(moving, axis=-1) - 1
        choose = (moving[..., None] == 1) & (ranks[..., None] == jnp.arange(capacity, dtype=jnp.int32))
        present = jnp.any(choose, axis=2)
        summed = lax.optimization_barrier(jnp.sum(jnp.where(choose, grid_ids[:, :, :, column_at][..., None], 0), axis=2))
        return jnp.where(present, summed, -1).astype(jnp.int32)
    rightward = packed(device_cols - 1, 1)
    leftward = packed(0, -1)
    filler = jnp.full((band_total, 1, capacity), -1, jnp.int32)
    from_left = jnp.concatenate([filler, rightward[:, :-1]], axis=1)
    from_right = jnp.concatenate([leftward[:, 1:], filler], axis=1)
    return jnp.concatenate([staying, from_left, from_right], axis=2)

def conductance(level_vals):
    return jnp.where(level_vals == 0, 1.0, jnp.where(level_vals == 1, 4.0, 16.0)).astype(jnp.float32)

def to_grid(patches):
    band_total, owner_total, patch_count, species_n, surface = patches.shape
    shaped = patches.reshape(band_total, owner_total, ROWS_DEV, COLS_DEV, species_n, CELLS, CELLS)
    moved = jnp.transpose(shaped, (4, 0, 2, 5, 1, 3, 6))
    return moved.reshape(species_n, band_total * ROWS_DEV * CELLS, owner_total * COLS_DEV * CELLS)

def from_grid(grid, band_total, owner_total):
    species_n = grid.shape[0]
    shaped = grid.reshape(species_n, band_total, ROWS_DEV, CELLS, owner_total, COLS_DEV, CELLS)
    moved = jnp.transpose(shaped, (1, 4, 2, 5, 0, 3, 6))
    return moved.reshape(band_total * owner_total * ROWS_DEV * COLS_DEV, species_n, CELLS * CELLS)

def laplace(values, coeff_pad):
    padded = jnp.pad(values, ((0, 0), (1, 1), (1, 1)))
    horiz = 0.5 * (coeff_pad[1:-1, :-1] + coeff_pad[1:-1, 1:])
    vertical = 0.5 * (coeff_pad[:-1, 1:-1] + coeff_pad[1:, 1:-1])
    return horiz[:, :-1] * (padded[:, 1:-1, :-2] - values) + horiz[:, 1:] * (padded[:, 1:-1, 2:] - values) + vertical[:-1] * (padded[:, :-2, 1:-1] - values) + vertical[1:] * (padded[:, 2:, 1:-1] - values)

def small_solve(gram, rhs):
    dimension = gram.shape[0]
    matrix = gram
    vector = rhs
    for column_at in range(dimension):
        for target in range(column_at + 1, dimension):
            factor = matrix[target, column_at] / matrix[column_at, column_at]
            matrix = matrix.at[target].add(-factor * matrix[column_at])
            vector = vector.at[target].add(-factor * vector[column_at])
    answer = [None] * dimension
    for column_at in reversed(range(dimension)):
        running = vector[column_at]
        for later in range(column_at + 1, dimension):
            running = running - matrix[column_at, later] * answer[later]
        answer[column_at] = running / matrix[column_at, column_at]
    return jnp.stack(answer)

def reference(previous, predicted, new_owner, levels, diffusion, decay, reaction):
    band_total, owner_total, patch_count = new_owner.shape
    prev_grid = to_grid(previous)
    state = to_grid(predicted)
    kappa_patches = jnp.broadcast_to(conductance(levels)[:, :, :, None, None], (band_total, owner_total, patch_count, 1, CELLS * CELLS))
    coeff_pad = jnp.pad(to_grid(kappa_patches)[0], 1, mode='edge')
    differential = (jnp.arange(SPECIES) < SPECIES - 1).astype(jnp.float32)[:, None, None]
    diff_col = diffusion[:, None, None]
    decay_col = decay[:, None, None]

    def mixing(values):
        return jnp.einsum('st,tyx->syx', reaction, values, precision=highest)
    for newton_step in range(NEWTON):
        resid = differential * step_rate * (state - prev_grid) - diff_col * laplace(state, coeff_pad) - mixing(state) + decay_col * (state * state * state)
        scale = jnp.sqrt(jnp.sum(resid * resid) + epsilon)
        basis = [-resid / scale]
        curvature = 3.0 * decay_col * (state * state)
        hess = jnp.zeros((KRYLOV + 1, KRYLOV), jnp.float32)
        for column_at in range(KRYLOV):
            current = basis[column_at]
            image = differential * step_rate * current - diff_col * laplace(current, coeff_pad) - mixing(current) + curvature * current
            coeffs = [jnp.sum(image * vector) for vector in basis]
            for position in range(len(basis)):
                image = image - coeffs[position] * basis[position]
            height = jnp.sqrt(jnp.sum(image * image) + epsilon)
            hess = hess.at[:column_at + 1, column_at].set(jnp.stack(coeffs))
            hess = hess.at[column_at + 1, column_at].set(height)
            basis.append(image / height)
        gram = jnp.dot(hess.T, hess, precision=highest)
        weights = small_solve(gram, scale * hess[0])
        update = weights[0] * basis[0]
        for position in range(1, KRYLOV):
            update = update + weights[position] * basis[position]
        state = state + update
    solved = from_grid(state, band_total, owner_total)
    slot_ids = slot_layout(new_owner, ROWS_DEV, MOVE_CAP)
    picked = jnp.take(solved, jnp.maximum(slot_ids, 0).reshape(-1), axis=0)
    picked = picked.reshape(band_total, owner_total, slot_ids.shape[2], SPECIES, CELLS * CELLS)
    return jnp.where((slot_ids >= 0)[:, :, :, None, None], picked, 0.0)
```

```python
import jax
import jax.numpy as jnp
from jax import lax
from jax.experimental import pallas as pl
from jax.experimental.pallas import tpu as pltpu
from jax.sharding import Mesh
from jax.sharding import PartitionSpec as P

SPECIES = 21
COLS_DEV = 3
ROWS_DEV = 4
MOVE_CAP = 2
PATCH_DEV = 12
BANDS = 4
OWNERS = 32
PATCH = ("patch_0", "patch_1", "patch_2")
EVERY = ("patch_0", "patch_1", "patch_2", "grp")
DEVICES = 128

ROWS = 80
OWN_LO, OWN_HI = 8, 72
LANES = 128
TILES = 10
MSG = TILES + TILES // 2

SIGMA = 32.0
THETA = 14.0
EPSILON = 1e-12
BREAKDOWN = 3e-7

f32 = jnp.float32
bf16 = jnp.bfloat16
STATE = (ROWS, 3, 8, LANES)


def lanes_of(shape=(8, LANES)):
    return lax.broadcasted_iota(jnp.int32, shape, len(shape) - 1)


def roll(x, amount):
    return pltpu.roll(x, amount % LANES, axis=x.ndim - 1)


def swap_blocks(tiles, group):
    tiles = list(tiles)
    for bit in (1, 2, 4):
        high = (group & bit) != 0
        for i in range(8):
            if i & bit:
                continue
            a, b = tiles[i], tiles[i + bit]
            tiles[i] = jnp.where(high, roll(b, 16 * bit), a)
            tiles[i + bit] = jnp.where(high, b, roll(a, -16 * bit))
    return tiles


def face_kernel(levels_ref, where_ref, out_ref):
    band, owner = where_ref[0], where_ref[1]
    lane_group = lanes_of() // 16
    kappas = []
    for idx in range(6):
        patch_row = band * ROWS_DEV + idx - 1
        row_in = (patch_row >= 0) & (patch_row < BANDS * ROWS_DEV)
        row_safe = jnp.clip(patch_row, 0, BANDS * ROWS_DEV - 1)
        row_base = (row_safe // ROWS_DEV) * (OWNERS * PATCH_DEV) + (row_safe % ROWS_DEV) * COLS_DEV
        kap = jnp.zeros((8, LANES), f32)
        for g in range(8):
            near_owner = owner + (g - 2 - (g - 2) % COLS_DEV) // COLS_DEV
            inside = row_in & (near_owner >= 0) & (near_owner < OWNERS)
            safe = jnp.clip(near_owner, 0, OWNERS - 1)
            level = levels_ref[row_base + safe * PATCH_DEV + (g - 2) % COLS_DEV]
            value = jnp.where(level == 0, 1.0, jnp.where(level == 1, 4.0, 16.0))
            value = jnp.where(inside, value, 0.0).astype(f32)
            kap = jnp.where(lane_group == g, value, kap)
        kappas.append(kap)

    def face(own, near):
        return jnp.where(own == 0.0, 0.0, jnp.where(near == 0.0, own, 0.5 * (own + near)))

    for idx in range(6):
        kap = kappas[idx]
        out_ref[idx, 0] = face(kap, roll(kap, 1))
        out_ref[idx, 1] = face(kap, roll(kap, -1))
        out_ref[idx, 2] = face(kap, kappas[max(idx - 1, 0)])
        out_ref[idx, 3] = face(kap, kappas[min(idx + 1, 5)])
        out_ref[idx, 4] = kap


def tile_of(patch_ref, south_ref, north_ref, which, k, c):
    if k == 0:
        return south_ref[which, c]
    if k == TILES - 1:
        return north_ref[which, c]
    half = (k - 1) % 2
    return patch_ref[((k - 1) // 2) * COLS_DEV + c, :, half * LANES : (half + 1) * LANES]


def pack_kernel(pred_ref, prev_ref, south_ref, north_ref, right_ref, left_ref):
    odd = (lax.broadcasted_iota(jnp.int32, (SPECIES, LANES), 1) // 8) % 2 == 1
    for which, patch_ref in enumerate((pred_ref, prev_ref)):
        for ref in (right_ref, left_ref):
            ref[which, :, SPECIES:24, :] = jnp.zeros((MSG, 24 - SPECIES, LANES), f32)
        for k in range(TILES):
            right_ref[which, k, 0:SPECIES, :] = tile_of(patch_ref, south_ref, north_ref, which, k, 2)
            left_ref[which, k, 0:SPECIES, :] = tile_of(patch_ref, south_ref, north_ref, which, k, 0)
        for pair in range(TILES // 2):
            low = tile_of(patch_ref, south_ref, north_ref, which, 2 * pair, 1)
            high = tile_of(patch_ref, south_ref, north_ref, which, 2 * pair + 1, 1)
            right_ref[which, TILES + pair, 0:SPECIES, :] = jnp.where(odd, high, roll(low, -8))
            left_ref[which, TILES + pair, 0:SPECIES, :] = jnp.where(odd, roll(high, 8), low)


def row_faces(face_ref, row):
    idx = (row + 8) // 16
    kap = face_ref[idx, 4]
    south = face_ref[idx, 2] if row % 16 == 8 else kap
    north = face_ref[idx, 3] if row % 16 == 7 else kap
    return face_ref[idx, 0], face_ref[idx, 1], south, north


def mixed_rows(source, first, blocks):
    x = jnp.concatenate(
        [source[first : first + 2].reshape(48, LANES), source[first + 2 : first + 4].reshape(48, LANES)],
        axis=1,
    )
    high = x.astype(bf16)
    low = (x - high.astype(f32)).astype(bf16)
    m = jnp.dot(blocks, jnp.concatenate([high, low, high], axis=0), preferred_element_type=f32)
    m = m.reshape(2, 3, 8, 2 * LANES)
    return [m[0, :, :, :LANES], m[1, :, :, :LANES], m[0, :, :, LANES:], m[1, :, :, LANES:]]


def spread(source, row, faces):
    west, east, south, north = faces
    v = source[row]
    return (west * roll(v, 1) + east * roll(v, -1)) + (
        south * source[row - 1] + north * source[row + 1]
    )


def apply_rows(source, lo, hi, start, blocks, face_ref, diff, emit):
    for first in range(start, hi, 4):
        mixed = mixed_rows(source, first, blocks)
        for off in range(4):
            row = first + off
            if row < lo or row >= hi:
                continue
            faces = row_faces(face_ref, row)
            emit(row, faces, diff * spread(source, row, faces) + mixed[off])


class Dots:
    def __init__(self):
        self.sums = {}

    def add(self, key, value):
        self.sums[key] = value if key not in self.sums else self.sums[key] + value

    def write(self, out_ref):
        lane = lanes_of((1, LANES))
        own = (lanes_of() >= 32) & (lanes_of() < 80)
        total = jnp.zeros((1, LANES), f32)
        for at, key in enumerate(PAIRS):
            value = jnp.where(own, jnp.sum(self.sums[key], axis=0), 0.0)
            value = jnp.sum(jnp.sum(value, axis=0, keepdims=True), axis=1, keepdims=True)
            total = jnp.where(lane == at, value, total)
        out_ref[...] = total


PAIRS = [(i, j) for j in range(4) for i in range(j + 1)]


def krylov(refs, diag_ref, face_ref, diff, blocks, dots, reach, last_ref):
    for k in range(3):
        source, target = refs[k], last_ref if k == 2 else refs[k + 1]
        width = reach - k - 1
        lo, hi = OWN_LO - width, OWN_HI + width
        start = lo - (lo % 2)

        def emit(row, faces, rest, source=source, target=target, k=k):
            new = diag_ref[row] * source[row] - rest
            if target is not None:
                target[row] = new
            if OWN_LO <= row < OWN_HI:
                for i in range(k + 1):
                    dots.add((i, k + 1), refs[i][row] * new)
                dots.add((k + 1, k + 1), new * new)

        apply_rows(source, lo, hi, start, blocks, face_ref, diff, emit)


def first_kernel(
    pred_ref, prev_ref, south_ref, north_ref, from_left_ref, from_right_ref, face_ref, param_ref,
    block_ref, state_ref, p0_ref, p1_ref, p2_ref, p3_ref, gram_ref, own_ref, old_ref, diag_ref,
):
    group = lanes_of() // 16
    own_ref[:, SPECIES:24, :] = jnp.zeros((TILES * COLS_DEV, 24 - SPECIES, LANES), f32)
    for which, (patch_ref, target) in enumerate(((pred_ref, state_ref), (prev_ref, old_ref))):
        for k in range(TILES):
            for c in range(COLS_DEV):
                own_ref[k * COLS_DEV + c, 0:SPECIES, :] = tile_of(
                    patch_ref, south_ref, north_ref, which, k, c
                )
        for k in range(TILES):
            far_left = from_left_ref[which, TILES + k // 2].reshape(3, 8, LANES)
            far_right = from_right_ref[which, TILES + k // 2].reshape(3, 8, LANES)
            tiles = [
                far_left if k % 2 else roll(far_left, 8),
                from_left_ref[which, k].reshape(3, 8, LANES),
                own_ref[k * COLS_DEV].reshape(3, 8, LANES),
                own_ref[k * COLS_DEV + 1].reshape(3, 8, LANES),
                own_ref[k * COLS_DEV + 2].reshape(3, 8, LANES),
                from_right_ref[which, k].reshape(3, 8, LANES),
                roll(far_right, -8) if k % 2 else far_right,
                jnp.zeros((3, 8, LANES), f32),
            ]
            for a, row in enumerate(swap_blocks(tiles, group)):
                target[k * 8 + a] = row
    rate, diff, decay = param_ref[0], param_ref[1], param_ref[2]
    blocks = block_ref[...]
    dots = Dots()

    def emit(row, faces, rest):
        u = state_ref[row]
        west, east, south, north = faces
        base = rate + diff * ((west + east) + (south + north))
        cubic = decay * (u * u)
        new = (base + cubic) * u - rate * old_ref[row] - rest
        diag_ref[row] = base + 3.0 * cubic - THETA / SIGMA
        p0_ref[row] = new
        if OWN_LO <= row < OWN_HI:
            dots.add((0, 0), new * new)

    apply_rows(state_ref, 2, 78, 2, blocks, face_ref, diff, emit)
    krylov((p0_ref, p1_ref, p2_ref), diag_ref, face_ref, diff, blocks, dots, 6, p3_ref)
    dots.write(gram_ref)


def small_solve(matrix, vector):
    matrix = [list(row) for row in matrix]
    vector = list(vector)
    size = len(vector)
    for col in range(size):
        for target in range(col + 1, size):
            factor = matrix[target][col] / matrix[col][col]
            for at in range(col, size):
                matrix[target][at] = matrix[target][at] - factor * matrix[col][at]
            vector[target] = vector[target] - factor * vector[col]
    answer = [None] * size
    for col in reversed(range(size)):
        running = vector[col]
        for later in range(col + 1, size):
            running = running - matrix[col][later] * answer[later]
        answer[col] = running / matrix[col][col]
    return answer


def combine(parts_ref):
    totals = jnp.sum(parts_ref[...], axis=0, keepdims=True)
    gram = [[None] * 4 for _ in range(4)]
    for at, (i, j) in enumerate(PAIRS):
        gram[i][j] = gram[j][i] = jnp.broadcast_to(totals[:, at : at + 1], (8, LANES))
    zero = jnp.zeros((8, LANES), f32)
    beta = jnp.sqrt(gram[0][0] * (SIGMA * SIGMA) + EPSILON)
    basis = [[-SIGMA / beta]]
    hess = [[zero] * 3 for _ in range(4)]

    def dot(x, y):
        total = x[0] * y[0]
        for at in range(1, len(x)):
            total = total + x[at] * y[at]
        return total

    for j in range(3):
        last = basis[j]
        w = [THETA * last[at] for at in range(j + 1)] + [SIGMA * last[j]]
        for at in range(j):
            w[at + 1] = w[at + 1] + SIGMA * last[at]
        gw = [dot(w, gram[at]) for at in range(j + 2)]
        size = dot(w, gw)
        for i in range(j + 1):
            hess[i][j] = dot(basis[i], gw)
        for i in range(j + 1):
            for at in range(i + 1):
                w[at] = w[at] - hess[i][j] * basis[i][at]
        rest = dot(w, [dot(w, gram[at]) for at in range(j + 2)])
        alive = rest > BREAKDOWN * size
        height = jnp.sqrt(jnp.where(alive, rest, 0.0) + EPSILON)
        hess[j + 1][j] = height
        basis.append([jnp.where(alive, value / height, 0.0) for value in w])
    normal = [[dot([h[i] for h in hess], [h[j] for h in hess]) for j in range(3)] for i in range(3)]
    y = small_solve(normal, [beta * hess[0][i] for i in range(3)])
    out = []
    for at in range(3):
        total = None
        for j in range(at, 3):
            term = y[j] * basis[j][at]
            total = term if total is None else total + term
        out.append(total)
    return out


def second_kernel(
    parts_ref, state_ref, p0_ref, p1_ref, p2_ref, p3_ref, face_ref, param_ref, block_ref,
    next_ref, q0_ref, q1_ref, q2_ref, gram_ref, diag_ref,
):
    c0, c1, c2 = combine(parts_ref)
    shift = THETA / SIGMA
    rate, diff, decay = param_ref[0], param_ref[1], param_ref[2]
    blocks = block_ref[...]
    dots = Dots()
    a0, a1, a2 = 1.0 + shift * c0, c0 + shift * c1, c1 + shift * c2
    for row in range(5, 75):
        p0, p1, p2, u = p0_ref[row], p1_ref[row], p2_ref[row], state_ref[row]
        d = c0 * p0 + c1 * p1 + c2 * p2
        linear = (a0 * p0 + a1 * p1) + (a2 * p2 + c2 * p3_ref[row])
        new = linear + (decay * (d * d)) * (3.0 * u + d)
        west, east, south, north = row_faces(face_ref, row)
        u = u + d
        diag_ref[row] = (
            rate + diff * ((west + east) + (south + north)) + 3.0 * decay * (u * u) - shift
        )
        next_ref[row] = u
        q0_ref[row] = new
        if OWN_LO <= row < OWN_HI:
            dots.add((0, 0), new * new)
    krylov((q0_ref, q1_ref, q2_ref), diag_ref, face_ref, diff, blocks, dots, 3, None)
    dots.write(gram_ref)


def last_kernel(parts_ref, next_ref, q0_ref, q1_ref, q2_ref, owner_ref, where_ref, out_ref):
    band, owner = where_ref[0], where_ref[1]
    c0, c1, c2 = combine(parts_ref)
    group = lanes_of() // 16
    for slot in range(PATCH_DEV, PATCH_DEV + 2 * MOVE_CAP):
        out_ref[slot] = jnp.zeros((SPECIES, 2 * LANES), f32)
    base = (band * OWNERS + owner) * PATCH_DEV
    stays = [owner_ref[base + s] == owner for s in range(PATCH_DEV)]
    left_base = jnp.maximum(base - PATCH_DEV, 0)
    right_base = jnp.minimum(base + PATCH_DEV, BANDS * OWNERS * PATCH_DEV - PATCH_DEV)
    left_in = [
        (owner > 0) & (owner_ref[left_base + r * COLS_DEV + COLS_DEV - 1] == owner)
        for r in range(ROWS_DEV)
    ]
    right_in = [
        (owner < OWNERS - 1) & (owner_ref[right_base + r * COLS_DEV] == owner)
        for r in range(ROWS_DEV)
    ]
    for r in range(ROWS_DEV):
        halves = []
        for half in range(2):
            rows = []
            for a in range(8):
                row = OWN_LO + r * 16 + half * 8 + a
                rows.append(
                    next_ref[row] + (c0 * q0_ref[row] + c1 * q1_ref[row] + c2 * q2_ref[row])
                )
            halves.append([t.reshape(24, LANES)[:SPECIES] for t in swap_blocks(rows, group)])
        for c in range(COLS_DEV):
            keep = stays[r * COLS_DEV + c]
            for half in range(2):
                out_ref[r * COLS_DEV + c, :, half * LANES : (half + 1) * LANES] = jnp.where(
                    keep, halves[half][2 + c], 0.0
                )
        for moving, g, first in ((left_in, 1, PATCH_DEV), (right_in, 5, PATCH_DEV + MOVE_CAP)):
            rank = jnp.int32(0)
            for before in range(r):
                rank = rank + moving[before].astype(jnp.int32)
            for place in range(min(r + 1, MOVE_CAP)):

                @pl.when(moving[r] & (rank == place))
                def _(place=place, g=g, first=first):
                    for half in range(2):
                        out_ref[first + place, :, half * LANES : (half + 1) * LANES] = halves[half][g]


def call(kernel, out_shape, in_specs, scratch=(), limit=40):
    return pl.pallas_call(
        kernel,
        out_shape=out_shape,
        in_specs=in_specs,
        out_specs=jax.tree.map(lambda _: pl.BlockSpec(memory_space=pltpu.VMEM), out_shape),
        scratch_shapes=list(scratch),
        compiler_params=pltpu.CompilerParams(vmem_limit_bytes=limit << 20),
    )


def vm():
    return pl.BlockSpec(memory_space=pltpu.VMEM)


def sm():
    return pl.BlockSpec(memory_space=pltpu.SMEM)


def shifted(x, axis, step):
    count = lax.axis_size(axis)
    return lax.ppermute(
        x, axis, [(i, i + step) for i in range(count) if 0 <= i + step < count]
    )


def summed(gram):
    spread_out = jnp.broadcast_to(gram[None], (DEVICES, 1, LANES))
    return lax.all_to_all(spread_out, EVERY, 0, 0).reshape(DEVICES, LANES)


def per_device(previous, predicted, new_owner, levels, diffusion, decay, reaction):
    where = jnp.stack([lax.axis_index("grp"), lax.axis_index(PATCH)]).astype(jnp.int32)
    prev, pred = previous[0, 0], predicted[0, 0]
    up = jnp.stack([pred[9:12, :, LANES:], prev[9:12, :, LANES:]])
    down = jnp.stack([pred[0:3, :, :LANES], prev[0:3, :, :LANES]])
    south, north = shifted(up, "grp", 1), shifted(down, "grp", -1)

    rate = jnp.where(jnp.arange(24) < SPECIES - 1, 4.0, 0.0)
    pad = (0, 24 - SPECIES)
    params = jnp.stack([rate, jnp.pad(diffusion, pad), jnp.pad(decay, pad)]) / SIGMA
    params = jnp.broadcast_to(params.astype(f32)[:, :, None], (3, 24, LANES)).reshape(3, 3, 8, LANES)
    matrix = jnp.pad(reaction / SIGMA, (pad, pad))
    high = matrix.astype(bf16)
    low = (matrix - high.astype(f32)).astype(bf16)
    none = jnp.zeros_like(high)

    def two(x):
        return jnp.concatenate(
            [jnp.concatenate([x, none], axis=1), jnp.concatenate([none, x], axis=1)], axis=0
        )

    blocks = jnp.concatenate([two(high), two(high), two(low)], axis=1)

    shape = jax.ShapeDtypeStruct
    faces = call(face_kernel, shape((6, 5, 8, LANES), f32), [sm(), sm()])(levels.reshape(-1), where)
    message = shape((2, MSG, 24, LANES), f32)
    to_right, to_left = call(pack_kernel, (message, message), [vm()] * 4)(pred, prev, south, north)
    from_left, from_right = shifted(to_right, PATCH, 1), shifted(to_left, PATCH, -1)
    state = shape(STATE, f32)
    gram = shape((1, LANES), f32)
    u0, p0, p1, p2, p3, gram1 = call(
        first_kernel,
        (state,) * 5 + (gram,),
        [vm()] * 9,
        [
            pltpu.VMEM((TILES * COLS_DEV, 24, LANES), f32),
            pltpu.VMEM(STATE, f32),
            pltpu.VMEM(STATE, f32),
        ],
    )(pred, prev, south, north, from_left, from_right, faces, params, blocks)
    u1, q0, q1, q2, gram2 = call(
        second_kernel, (state,) * 4 + (gram,), [vm()] * 9, [pltpu.VMEM(STATE, f32)]
    )(summed(gram1), u0, p0, p1, p2, p3, faces, params, blocks)
    out = call(
        last_kernel,
        shape((PATCH_DEV + 2 * MOVE_CAP, SPECIES, 2 * LANES), f32),
        [vm()] * 5 + [sm(), sm()],
    )(summed(gram2), u1, q0, q1, q2, new_owner.reshape(-1), where)
    return out[None, None]


def solution(mesh):
    torus = Mesh(
        mesh.devices.reshape(4, 4, 2, mesh.shape["grp"]), ("patch_0", "patch_1", "patch_2", "grp")
    )
    spec = P("grp", PATCH, None, None, None)
    in_specs = (spec, spec, P(), P(), P(), P(), P())
    return jax.shard_map(
        per_device, mesh=torus, in_specs=in_specs, out_specs=spec, check_vma=False
    )
```

```python
import jax
import jax.numpy as jnp
from jax import lax
from jax.experimental import pallas as pl
from jax.experimental.pallas import tpu as pltpu
from jax.sharding import Mesh
from jax.sharding import PartitionSpec as P

SPECIES = 21
COLS_DEV = 3
ROWS_DEV = 4
MOVE_CAP = 2
PATCH_DEV = 12
BANDS = 4
OWNERS = 32
PATCH = ("patch_0", "patch_1", "patch_2")
EVERY = ("patch_0", "patch_1", "patch_2", "grp")
DEVICES = 128

ROWS = 80
OWN_LO, OWN_HI = 8, 72
LANES = 128
TILES = 10
MSG = TILES + TILES // 2

SIGMA = 32.0
THETA = 14.0
EPSILON = 1e-12
BREAKDOWN = 3e-7

f32 = jnp.float32
bf16 = jnp.bfloat16
STATE = (ROWS, 3, 8, LANES)


def lanes_of(shape=(8, LANES)):
    return lax.broadcasted_iota(jnp.int32, shape, len(shape) - 1)


def roll(x, amount):
    return pltpu.roll(x, amount % LANES, axis=x.ndim - 1)


def swap_blocks(rolled, wanted):
    group = lanes_of() // 16
    tiles = list(rolled)
    for bit in (1, 2, 4):
        high = (group & bit) != 0
        tiles = [jnp.where(high, tiles[(i + bit) % 8], tiles[i]) for i in range(8)]
    return {a: roll(tiles[-a % 8], -16 * a) for a in wanted}


def face_kernel(levels_ref, where_ref, face_ref, stencil_ref):
    band, owner = where_ref[0], where_ref[1]
    lane_group = lanes_of() // 16
    kappas = []
    for idx in range(6):
        patch_row = band * ROWS_DEV + idx - 1
        row_in = (patch_row >= 0) & (patch_row < BANDS * ROWS_DEV)
        row_safe = jnp.clip(patch_row, 0, BANDS * ROWS_DEV - 1)
        row_base = (row_safe // ROWS_DEV) * (OWNERS * PATCH_DEV) + (row_safe % ROWS_DEV) * COLS_DEV
        kap = jnp.zeros((8, LANES), f32)
        for g in range(8):
            near_owner = owner + (g - 2 - (g - 2) % COLS_DEV) // COLS_DEV
            inside = row_in & (near_owner >= 0) & (near_owner < OWNERS)
            safe = jnp.clip(near_owner, 0, OWNERS - 1)
            level = levels_ref[row_base + safe * PATCH_DEV + (g - 2) % COLS_DEV]
            value = jnp.where(level == 0, 1.0, jnp.where(level == 1, 4.0, 16.0))
            value = jnp.where(inside, value, 0.0).astype(f32)
            kap = jnp.where(lane_group == g, value, kap)
        kappas.append(kap)

    def face(own, near):
        return jnp.where(own == 0.0, 0.0, jnp.where(near == 0.0, own, 0.5 * (own + near)))

    source = lax.broadcasted_iota(jnp.int32, (LANES, LANES), 0)
    target = lax.broadcasted_iota(jnp.int32, (LANES, LANES), 1)
    for idx in range(6):
        kap = kappas[idx]
        west, east = face(kap, roll(kap, 1)), face(kap, roll(kap, -1))
        face_ref[idx, 0] = west + east
        face_ref[idx, 1] = face(kap, kappas[max(idx - 1, 0)])
        face_ref[idx, 2] = face(kap, kappas[min(idx + 1, 5)])
        face_ref[idx, 3] = kap
        weights = jnp.where(
            source == target - 1,
            jnp.broadcast_to(west[0:1], (LANES, LANES)),
            jnp.where(source == target + 1, jnp.broadcast_to(east[0:1], (LANES, LANES)), 0.0),
        ).astype(bf16)
        stencil_ref[idx, 0:LANES, :] = weights
        stencil_ref[idx, LANES : 2 * LANES, :] = weights


def half_tile(patch_ref, slot, half):
    return patch_ref[pl.ds(slot * 2 * SPECIES + half, SPECIES, stride=2), :]


def row_strip_kernel(pred_ref, prev_ref, where_ref, first_ref, second_ref):
    even = where_ref[0] % 2 == 0
    pad = jnp.zeros((24 - SPECIES, LANES), f32)
    for which, patch_ref in enumerate((pred_ref, prev_ref)):
        for c in range(COLS_DEV):
            up = half_tile(patch_ref, 3 * COLS_DEV + c, 1)
            down = half_tile(patch_ref, c, 0)
            first_ref[which, c, 0:SPECIES, :] = jnp.where(even, up, down)
            second_ref[which, c, 0:SPECIES, :] = jnp.where(even, down, up)
            first_ref[which, c, SPECIES:24, :] = pad
            second_ref[which, c, SPECIES:24, :] = pad


def tile_of(patch_ref, rows_ref, where_ref, which, k, c):
    if k in (0, TILES - 1):
        band = where_ref[0]
        even = band % 2 == 0
        first, second = (ref[which, c, 0:SPECIES, :] for ref in rows_ref)
        south, inside = k == 0, (band > 0) if k == 0 else (band < BANDS - 1)
        tile = jnp.where(even, second, first) if south else jnp.where(even, first, second)
        return jnp.where(inside, tile, 0.0)
    return half_tile(patch_ref, ((k - 1) // 2) * COLS_DEV + c, (k - 1) % 2)


def pack_kernel(pred_ref, prev_ref, row1_ref, row2_ref, where_ref, first_ref, second_ref):
    odd = (lax.broadcasted_iota(jnp.int32, (SPECIES, LANES), 1) // 8) % 2 == 1
    even_owner = where_ref[1] % 2 == 0
    rows_ref = (row1_ref, row2_ref)
    for which, patch_ref in enumerate((pred_ref, prev_ref)):
        for ref in (first_ref, second_ref):
            ref[which, :, SPECIES:24, :] = jnp.zeros((MSG, 24 - SPECIES, LANES), f32)

        def put(at, right, left, which=which):
            first_ref[which, at, 0:SPECIES, :] = jnp.where(even_owner, right, left)
            second_ref[which, at, 0:SPECIES, :] = jnp.where(even_owner, left, right)

        def tile(k, c, which=which, patch_ref=patch_ref):
            return tile_of(patch_ref, rows_ref, where_ref, which, k, c)

        for k in range(TILES):
            put(k, tile(k, 2), tile(k, 0))
        for pair in range(TILES // 2):
            low, high = tile(2 * pair, 1), tile(2 * pair + 1, 1)
            put(
                TILES + pair,
                jnp.where(odd, high, roll(low, -8)),
                jnp.where(odd, roll(high, 8), low),
            )


def row_faces(face_ref, row):
    idx = (row + 8) // 16
    kap = face_ref[idx, 3]
    south = face_ref[idx, 1] if row % 16 == 8 else kap
    north = face_ref[idx, 2] if row % 16 == 7 else kap
    return face_ref[idx, 0], south, north


def vertical(source, row, faces):
    _, south, north = faces
    if row % 16 in (7, 8):
        return south * source[row - 1] + north * source[row + 1]
    return south * (source[row - 1] + source[row + 1])


def apply_rows(source, lo, hi, blocks, stencil_ref, face_ref, diff, emit):
    for idx in range(6):
        first, last = max(lo, idx * 16 - 8), min(hi, idx * 16 + 8)
        if first >= last:
            continue
        start, stop = first - first % 2, last + last % 2
        parts = []
        for row in range(start, stop, 2):
            x = source[row : row + 2].reshape(48, LANES)
            high = x.astype(bf16)
            parts.append((high, (x - high.astype(f32)).astype(bf16)))
        beside = jnp.dot(
            jnp.concatenate([jnp.concatenate(part, axis=1) for part in parts], axis=0),
            stencil_ref[idx],
            preferred_element_type=f32,
        ).reshape(stop - start, 3, 8, LANES)
        mixed = []
        for at in range(0, len(parts), 2):
            group = parts[at : at + 2]
            high = jnp.concatenate([part[0] for part in group], axis=1)
            low = jnp.concatenate([part[1] for part in group], axis=1)
            m = jnp.dot(
                blocks, jnp.concatenate([high, low, high], axis=0), preferred_element_type=f32
            ).reshape(2, 3, 8, len(group) * LANES)
            for pair in range(len(group)):
                for off in range(2):
                    mixed.append(m[off, :, :, pair * LANES : (pair + 1) * LANES])
        for row in range(first, last):
            faces = row_faces(face_ref, row)
            near = beside[row - start] + vertical(source, row, faces)
            emit(row, faces, diff * near + mixed[row - start])


class Dots:
    def __init__(self):
        self.sums = {}

    def add(self, key, value):
        self.sums[key] = value if key not in self.sums else self.sums[key] + value

    def write(self, out_ref):
        lane = lanes_of((1, LANES))
        own = (lanes_of() >= 32) & (lanes_of() < 80)
        total = jnp.zeros((1, LANES), f32)
        for at, key in enumerate(PAIRS):
            value = jnp.where(own, jnp.sum(self.sums[key], axis=0), 0.0)
            value = jnp.sum(jnp.sum(value, axis=0, keepdims=True), axis=1, keepdims=True)
            total = jnp.where(lane == at, value, total)
        out_ref[...] = total


PAIRS = [(i, j) for j in range(4) for i in range(j + 1)]


def krylov(refs, diag_ref, tables, diff, dots, reach, last_ref):
    for k in range(3):
        source, target = refs[k], last_ref if k == 2 else refs[k + 1]
        width = reach - k - 1
        lo, hi = OWN_LO - width, OWN_HI + width

        def emit(row, faces, rest, source=source, target=target, k=k):
            new = diag_ref[row] * source[row] - rest
            if target is not None:
                target[row] = new
            if OWN_LO <= row < OWN_HI:
                for i in range(k + 1):
                    dots.add((i, k + 1), refs[i][row] * new)
                dots.add((k + 1, k + 1), new * new)

        apply_rows(source, lo, hi, *tables, diff, emit)


def first_kernel(
    pred_ref, prev_ref, row1_ref, row2_ref, col1_ref, col2_ref, where_ref, face_ref, stencil_ref,
    param_ref, block_ref, state_ref, p0_ref, p1_ref, p2_ref, p3_ref, gram_ref, own_ref, old_ref,
    diag_ref,
):
    owner = where_ref[1]
    even_owner, has_left, has_right = owner % 2 == 0, owner > 0, owner < OWNERS - 1
    rows_ref = (row1_ref, row2_ref)
    own_ref[:, SPECIES:24, :] = jnp.zeros((2 * TILES * COLS_DEV, 24 - SPECIES, LANES), f32)
    for which, patch_ref in enumerate((pred_ref, prev_ref)):
        for k in range(TILES):
            for c in range(COLS_DEV):
                own_ref[(which * TILES + k) * COLS_DEV + c, 0:SPECIES, :] = tile_of(
                    patch_ref, rows_ref, where_ref, which, k, c
                )
    for which, target in enumerate((state_ref, old_ref)):

        def beside(at, which=which):
            first, second = (ref[which, at].reshape(3, 8, LANES) for ref in (col1_ref, col2_ref))
            left, right = jnp.where(even_owner, second, first), jnp.where(even_owner, first, second)
            return jnp.where(has_left, left, 0.0), jnp.where(has_right, right, 0.0)

        for k in range(TILES):
            if k % 2 == 0:
                far_left, far_right = beside(TILES + k // 2)
            left, right = beside(k)
            own = [
                own_ref[(which * TILES + k) * COLS_DEV + c].reshape(3, 8, LANES)
                for c in range(COLS_DEV)
            ]
            tiles = [
                far_left if k % 2 else roll(far_left, 8),
                roll(left, 16),
                roll(own[0], 32),
                roll(own[1], 48),
                roll(own[2], 64),
                roll(right, 80),
                roll(far_right, 88 if k % 2 else 96),
                jnp.zeros((3, 8, LANES), f32),
            ]
            for a, row in swap_blocks(tiles, range(8)).items():
                target[k * 8 + a] = row
    rate, diff, decay = param_ref[0], param_ref[1], param_ref[2]
    tables = (block_ref[...], stencil_ref, face_ref)
    dots = Dots()

    def emit(row, faces, rest):
        u = state_ref[row]
        base = rate + diff * (faces[0] + (faces[1] + faces[2]))
        cubic = decay * (u * u)
        new = (base + cubic) * u - rate * old_ref[row] - rest
        diag_ref[row] = (base - THETA / SIGMA) + 3.0 * cubic
        p0_ref[row] = new
        if OWN_LO <= row < OWN_HI:
            dots.add((0, 0), new * new)

    apply_rows(state_ref, 2, 78, *tables, diff, emit)
    krylov((p0_ref, p1_ref, p2_ref), diag_ref, tables, diff, dots, 6, p3_ref)
    dots.write(gram_ref)


def small_solve(matrix, vector):
    matrix = [list(row) for row in matrix]
    vector = list(vector)
    size = len(vector)
    for col in range(size):
        for target in range(col + 1, size):
            factor = matrix[target][col] / matrix[col][col]
            for at in range(col, size):
                matrix[target][at] = matrix[target][at] - factor * matrix[col][at]
            vector[target] = vector[target] - factor * vector[col]
    answer = [None] * size
    for col in reversed(range(size)):
        running = vector[col]
        for later in range(col + 1, size):
            running = running - matrix[col][later] * answer[later]
        answer[col] = running / matrix[col][col]
    return answer


def combine(parts_ref):
    totals = jnp.sum(parts_ref[...], axis=0, keepdims=True)
    gram = [[None] * 4 for _ in range(4)]
    for at, (i, j) in enumerate(PAIRS):
        gram[i][j] = gram[j][i] = jnp.broadcast_to(totals[:, at : at + 1], (8, LANES))
    zero = jnp.zeros((8, LANES), f32)
    beta = jnp.sqrt(gram[0][0] * (SIGMA * SIGMA) + EPSILON)
    basis = [[-SIGMA / beta]]
    hess = [[zero] * 3 for _ in range(4)]

    def dot(x, y):
        total = x[0] * y[0]
        for at in range(1, len(x)):
            total = total + x[at] * y[at]
        return total

    for j in range(3):
        last = basis[j]
        w = [THETA * last[at] for at in range(j + 1)] + [SIGMA * last[j]]
        for at in range(j):
            w[at + 1] = w[at + 1] + SIGMA * last[at]
        gw = [dot(w, gram[at]) for at in range(j + 2)]
        size = dot(w, gw)
        for i in range(j + 1):
            hess[i][j] = dot(basis[i], gw)
        for i in range(j + 1):
            for at in range(i + 1):
                w[at] = w[at] - hess[i][j] * basis[i][at]
        rest = dot(w, [dot(w, gram[at]) for at in range(j + 2)])
        alive = rest > BREAKDOWN * size
        height = jnp.sqrt(jnp.where(alive, rest, 0.0) + EPSILON)
        hess[j + 1][j] = height
        basis.append([jnp.where(alive, value / height, 0.0) for value in w])
    normal = [[dot([h[i] for h in hess], [h[j] for h in hess]) for j in range(3)] for i in range(3)]
    y = small_solve(normal, [beta * hess[0][i] for i in range(3)])
    out = []
    for at in range(3):
        total = None
        for j in range(at, 3):
            term = y[j] * basis[j][at]
            total = term if total is None else total + term
        out.append(total)
    return out


def second_kernel(
    parts_ref, state_ref, p0_ref, p1_ref, p2_ref, p3_ref, face_ref, stencil_ref, param_ref,
    block_ref, next_ref, q0_ref, q1_ref, q2_ref, gram_ref, diag_ref,
):
    c0, c1, c2 = combine(parts_ref)
    shift = THETA / SIGMA
    rate, diff, decay = param_ref[0], param_ref[1], param_ref[2]
    tables = (block_ref[...], stencil_ref, face_ref)
    dots = Dots()
    a0, a1, a2 = 1.0 + shift * c0, c0 + shift * c1, c1 + shift * c2
    triple = 3.0 * decay
    for row in range(5, 75):
        p0, p1, p2, u = p0_ref[row], p1_ref[row], p2_ref[row], state_ref[row]
        d = c0 * p0 + c1 * p1 + c2 * p2
        linear = (a0 * p0 + a1 * p1) + (a2 * p2 + c2 * p3_ref[row])
        new = linear + (decay * (d * d)) * (3.0 * u + d)
        beside, south, north = row_faces(face_ref, row)
        u = u + d
        base = rate + diff * (beside + (south + north)) - shift
        diag_ref[row] = base + triple * (u * u)
        next_ref[row] = u
        q0_ref[row] = new
        if OWN_LO <= row < OWN_HI:
            dots.add((0, 0), new * new)
    krylov((q0_ref, q1_ref, q2_ref), diag_ref, tables, diff, dots, 3, None)
    dots.write(gram_ref)


SLOTS = PATCH_DEV + 2 * MOVE_CAP


def last_kernel(
    parts_ref, next_ref, q0_ref, q1_ref, q2_ref, owner_ref, where_ref, out_ref, low_ref, high_ref
):
    band, owner = where_ref[0], where_ref[1]
    c0, c1, c2 = combine(parts_ref)
    slots_ref = (low_ref, high_ref)
    for ref in slots_ref:
        ref[PATCH_DEV * 24 : SLOTS * 24, :] = jnp.zeros((2 * MOVE_CAP * 24, LANES), f32)
    base = (band * OWNERS + owner) * PATCH_DEV
    stays = [owner_ref[base + s] == owner for s in range(PATCH_DEV)]
    left_base = jnp.maximum(base - PATCH_DEV, 0)
    right_base = jnp.minimum(base + PATCH_DEV, BANDS * OWNERS * PATCH_DEV - PATCH_DEV)
    left_in = [
        (owner > 0) & (owner_ref[left_base + r * COLS_DEV + COLS_DEV - 1] == owner)
        for r in range(ROWS_DEV)
    ]
    right_in = [
        (owner < OWNERS - 1) & (owner_ref[right_base + r * COLS_DEV] == owner)
        for r in range(ROWS_DEV)
    ]
    for r in range(ROWS_DEV):
        halves = []
        for half in range(2):
            rows = []
            for a in range(8):
                row = OWN_LO + r * 16 + half * 8 + a
                value = next_ref[row] + (c0 * q0_ref[row] + c1 * q1_ref[row] + c2 * q2_ref[row])
                rows.append(roll(value, 16 * a) if a else value)
            halves.append(
                {g: t.reshape(24, LANES) for g, t in swap_blocks(rows, range(1, 6)).items()}
            )
        for c in range(COLS_DEV):
            slot = r * COLS_DEV + c
            for half in range(2):
                slots_ref[half][slot * 24 : slot * 24 + 24, :] = jnp.where(
                    stays[slot], halves[half][2 + c], 0.0
                )
        for moving, g, first in ((left_in, 1, PATCH_DEV), (right_in, 5, PATCH_DEV + MOVE_CAP)):
            rank = jnp.int32(0)
            for before in range(r):
                rank = rank + moving[before].astype(jnp.int32)
            for place in range(min(r + 1, MOVE_CAP)):

                @pl.when(moving[r] & (rank == place))
                def _(slot=first + place, g=g):
                    for half in range(2):
                        slots_ref[half][slot * 24 : slot * 24 + 24, :] = halves[half][g]

    for s in range(SPECIES):
        for part in range(SLOTS // 8):
            for half in range(2):
                out_ref[s, part * 8 : part * 8 + 8, half * LANES : (half + 1) * LANES] = slots_ref[
                    half
                ][pl.ds(part * 8 * 24 + s, 8, stride=24), :]


def call(kernel, out_shape, in_specs, scratch=(), limit=16):
    return pl.pallas_call(
        kernel,
        out_shape=out_shape,
        in_specs=in_specs,
        out_specs=jax.tree.map(lambda _: pl.BlockSpec(memory_space=pltpu.VMEM), out_shape),
        scratch_shapes=list(scratch),
        compiler_params=pltpu.CompilerParams(vmem_limit_bytes=limit << 20),
    )


def vm():
    return pl.BlockSpec(memory_space=pltpu.VMEM)


def sm():
    return pl.BlockSpec(memory_space=pltpu.SMEM)


def exchanged(x, axis, odd):
    count = lax.axis_size(axis)
    mates = [((i - odd) ^ 1) + odd for i in range(odd, count + odd)]
    return lax.ppermute(x, axis, [((i + odd) % count, m % count) for i, m in enumerate(mates)])


def summed(gram):
    spread_out = jnp.broadcast_to(gram[None], (DEVICES, 1, LANES))
    return lax.all_to_all(spread_out, EVERY, 0, 0).reshape(DEVICES, LANES)


def per_device(previous, predicted, new_owner, levels, diffusion, decay, reaction):
    where = jnp.stack([lax.axis_index("grp"), lax.axis_index(PATCH)]).astype(jnp.int32)
    prev, pred = (x.reshape(PATCH_DEV * SPECIES * 2, LANES) for x in (previous, predicted))
    shape = jax.ShapeDtypeStruct
    strip = shape((2, COLS_DEV, 24, LANES), f32)
    strips = call(row_strip_kernel, (strip, strip), [vm(), vm(), sm()])(pred, prev, where)
    row1, row2 = (exchanged(x, "grp", odd) for odd, x in enumerate(strips))

    rate = jnp.where(jnp.arange(24) < SPECIES - 1, 4.0, 0.0)
    pad = (0, 24 - SPECIES)
    params = jnp.stack([rate, jnp.pad(diffusion, pad), jnp.pad(decay, pad)]) / SIGMA
    params = jnp.broadcast_to(params.astype(f32)[:, :, None], (3, 24, LANES)).reshape(3, 3, 8, LANES)
    matrix = jnp.pad(reaction / SIGMA, (pad, pad))
    rounded = lax.reduce_precision(matrix, 8, 7)
    high = rounded.astype(bf16)
    low = (matrix - rounded).astype(bf16)
    none = jnp.zeros_like(high)

    def two(x):
        return jnp.concatenate(
            [jnp.concatenate([x, none], axis=1), jnp.concatenate([none, x], axis=1)], axis=0
        )

    blocks = jnp.concatenate([two(high), two(high), two(low)], axis=1)

    faces, stencil = call(
        face_kernel, (shape((6, 4, 8, LANES), f32), shape((6, 2 * LANES, LANES), bf16)), [sm(), sm()]
    )(levels.reshape(-1), where)
    message = shape((2, MSG, 24, LANES), f32)
    messages = call(pack_kernel, (message, message), [vm()] * 4 + [sm()])(
        pred, prev, row1, row2, where
    )
    col1, col2 = (exchanged(x, PATCH, odd) for odd, x in enumerate(messages))
    state = shape(STATE, f32)
    gram = shape((1, LANES), f32)
    u0, p0, p1, p2, p3, gram1 = call(
        first_kernel,
        (state,) * 5 + (gram,),
        [vm()] * 6 + [sm()] + [vm()] * 4,
        [
            pltpu.VMEM((2 * TILES * COLS_DEV, 24, LANES), f32),
            pltpu.VMEM(STATE, f32),
            pltpu.VMEM(STATE, f32),
        ],
    )(pred, prev, row1, row2, col1, col2, where, faces, stencil, params, blocks)
    u1, q0, q1, q2, gram2 = call(
        second_kernel, (state,) * 4 + (gram,), [vm()] * 10, [pltpu.VMEM(STATE, f32)]
    )(summed(gram1), u0, p0, p1, p2, p3, faces, stencil, params, blocks)
    out = call(
        last_kernel,
        shape((SPECIES, SLOTS, 2 * LANES), f32),
        [vm()] * 5 + [sm(), sm()],
        [pltpu.VMEM((SLOTS * 24, LANES), f32)] * 2,
    )(summed(gram2), u1, q0, q1, q2, new_owner.reshape(-1), where)
    return jnp.transpose(out, (1, 0, 2))[None, None]


def solution(mesh):
    torus = Mesh(
        mesh.devices.reshape(4, 4, 2, mesh.shape["grp"]), ("patch_0", "patch_1", "patch_2", "grp")
    )
    spec = P("grp", PATCH, None, None, None)
    in_specs = (spec, spec, P(), P(), P(), P(), P())
    return jax.shard_map(
        per_device, mesh=torus, in_specs=in_specs, out_specs=spec, check_vma=False
    )
```

```python
import jax
import jax.numpy as jnp
from jax import lax
from jax.experimental import pallas as pl
from jax.experimental.pallas import tpu as pltpu
from jax.sharding import Mesh
from jax.sharding import PartitionSpec as P

SPECIES = 21
COLS_DEV = 3
ROWS_DEV = 4
MOVE_CAP = 2
PATCH_DEV = 12
BANDS = 4
OWNERS = 32
PATCH = ("patch_0", "patch_1", "patch_2")
EVERY = ("patch_0", "patch_1", "patch_2", "grp")
DEVICES = 128

ROWS = 80
OWN_LO, OWN_HI = 8, 72
LANES = 128
TILES = 10
MSG = TILES + TILES // 2

SIGMA = 32.0
THETA = 14.0
EPSILON = 1e-12
BREAKDOWN = 3e-7

f32 = jnp.float32
bf16 = jnp.bfloat16
STATE = (ROWS, 3, 8, LANES)


def position():
    return lax.axis_index("grp"), lax.axis_index(PATCH)


def lanes_of(shape=(8, LANES)):
    return lax.broadcasted_iota(jnp.int32, shape, len(shape) - 1)


def roll(x, amount):
    return pltpu.roll(x, amount % LANES, axis=x.ndim - 1)


def mix_blocks(rolled):
    group = lanes_of() // 16
    tiles = list(rolled)
    for bit in (1, 2, 4):
        high = (group & bit) != 0
        tiles = [jnp.where(high, tiles[(i + bit) % 8], tiles[i]) for i in range(8)]
    return tiles


def swap_blocks(rolled, wanted):
    tiles = mix_blocks(rolled)
    return {a: roll(tiles[-a % 8], -16 * a) if a else tiles[0] for a in wanted}


STAYS = PATCH_DEV
ARRIVALS = [(r, m) for r in range(ROWS_DEV) for m in range(min(r + 1, MOVE_CAP))]
FLAGS = STAYS + 2 * len(ARRIVALS)


def write_flags(owners_ref, flag_ref, band, owner):
    base = (band * OWNERS + owner) * PATCH_DEV

    def put(at, condition):
        flag_ref[at] = jnp.full((8, LANES), jnp.where(condition, 1, 0), jnp.int32)

    for slot in range(PATCH_DEV):
        put(slot, owners_ref[base + slot] == owner)
    left_base = jnp.maximum(base - PATCH_DEV, 0)
    right_base = jnp.minimum(base + PATCH_DEV, (BANDS * OWNERS - 1) * PATCH_DEV)
    sides = ((owner > 0, left_base + COLS_DEV - 1), (owner < OWNERS - 1, right_base))
    for side, (exists, first) in enumerate(sides):
        moving = [
            jnp.where(exists & (owners_ref[first + r * COLS_DEV] == owner), 1, 0)
            for r in range(ROWS_DEV)
        ]
        for at, (r, m) in enumerate(ARRIVALS):
            rank = jnp.int32(0)
            for before in range(r):
                rank = rank + moving[before]
            put(STAYS + side * len(ARRIVALS) + at, (moving[r] == 1) & (rank == m))


def face_kernel(levels_ref, owners_ref, face_ref, stencil_ref, flag_ref):
    band, owner = position()
    write_flags(owners_ref, flag_ref, band, owner)
    lane_group = lanes_of() // 16
    kappas = []
    for idx in range(6):
        patch_row = band * ROWS_DEV + idx - 1
        row_in = (patch_row >= 0) & (patch_row < BANDS * ROWS_DEV)
        row_safe = jnp.clip(patch_row, 0, BANDS * ROWS_DEV - 1)
        row_base = (row_safe // ROWS_DEV) * (OWNERS * PATCH_DEV) + (row_safe % ROWS_DEV) * COLS_DEV
        kap = jnp.zeros((8, LANES), f32)
        for g in range(8):
            near_owner = owner + (g - 2 - (g - 2) % COLS_DEV) // COLS_DEV
            inside = row_in & (near_owner >= 0) & (near_owner < OWNERS)
            safe = jnp.clip(near_owner, 0, OWNERS - 1)
            level = levels_ref[row_base + safe * PATCH_DEV + (g - 2) % COLS_DEV]
            value = jnp.where(level == 0, 1.0, jnp.where(level == 1, 4.0, 16.0))
            value = jnp.where(inside, value, 0.0).astype(f32)
            kap = jnp.where(lane_group == g, value, kap)
        kappas.append(kap)

    def face(own, near):
        return jnp.where(own == 0.0, 0.0, jnp.where(near == 0.0, own, 0.5 * (own + near)))

    source = lax.broadcasted_iota(jnp.int32, (LANES, LANES), 0)
    target = lax.broadcasted_iota(jnp.int32, (LANES, LANES), 1)
    for idx in range(6):
        kap = kappas[idx]
        west, east = face(kap, roll(kap, 1)), face(kap, roll(kap, -1))
        face_ref[idx, 0] = west + east
        face_ref[idx, 1] = face(kap, kappas[max(idx - 1, 0)])
        face_ref[idx, 2] = face(kap, kappas[min(idx + 1, 5)])
        face_ref[idx, 3] = kap
        weights = jnp.where(
            source == target - 1,
            jnp.broadcast_to(west[0:1], (LANES, LANES)),
            jnp.where(source == target + 1, jnp.broadcast_to(east[0:1], (LANES, LANES)), 0.0),
        ).astype(bf16)
        stencil_ref[idx, 0:LANES, :] = weights
        stencil_ref[idx, LANES : 2 * LANES, :] = weights


def half_tile(patch_ref, slot, half):
    return patch_ref[pl.ds(slot * 2 * SPECIES + half, SPECIES, stride=2), :]


ROW_TILES = 2 * COLS_DEV
COL_TILES = 2 * MSG


def dense(tiles):
    return -(-(tiles * SPECIES + 24 - SPECIES) // 8) * 8


def put_tile(ref, at, tile):
    ref[at * SPECIES : (at + 1) * SPECIES, :] = tile


def finish(ref, tiles):
    ref[tiles * SPECIES :, :] = jnp.zeros((dense(tiles) - tiles * SPECIES, LANES), f32)


def get_tile(ref, at):
    tile = ref[at * SPECIES : at * SPECIES + 24, :]
    species = lax.broadcasted_iota(jnp.int32, (24, LANES), 0)
    return jnp.where(species < SPECIES, tile, 0.0)


INPUT_ROWS = PATCH_DEV * 2 * SPECIES
EDGE = 128


def row_strip_kernel(pred_hbm, prev_hbm, pred_ref, prev_ref, first_ref, second_ref, sems):
    band, _ = position()
    even = band % 2 == 0
    top = INPUT_ROWS - EDGE
    spans = ((0, EDGE), (top, EDGE), (EDGE, top - EDGE))
    pairs = ((pred_hbm, pred_ref), (prev_hbm, prev_ref))
    copies = [
        [
            pltpu.make_async_copy(
                source.at[pl.ds(start, size), :],
                target.at[pl.ds(start, size), :],
                sems.at[3 * which + at],
            )
            for at, (start, size) in enumerate(spans)
        ]
        for which, (source, target) in enumerate(pairs)
    ]
    for at in range(3):
        for which in range(2):
            copies[which][at].start()
    for which, (_, patch_ref) in enumerate(pairs):
        copies[which][0].wait()
        copies[which][1].wait()
        for c in range(COLS_DEV):
            up = half_tile(patch_ref, PATCH_DEV - COLS_DEV + c, 1)
            down = half_tile(patch_ref, c, 0)
            put_tile(first_ref, which * COLS_DEV + c, jnp.where(even, up, down))
            put_tile(second_ref, which * COLS_DEV + c, jnp.where(even, down, up))
    finish(first_ref, ROW_TILES)
    finish(second_ref, ROW_TILES)
    copies[0][2].wait()
    copies[1][2].wait()


def tile_of(patch_ref, rows_ref, which, k, c):
    if k in (0, TILES - 1):
        band, _ = position()
        even = band % 2 == 0
        at = (which * COLS_DEV + c) * SPECIES
        first, second = (ref[at : at + SPECIES, :] for ref in rows_ref)
        south, inside = k == 0, (band > 0) if k == 0 else (band < BANDS - 1)
        tile = jnp.where(even, second, first) if south else jnp.where(even, first, second)
        return jnp.where(inside, tile, 0.0)
    return half_tile(patch_ref, ((k - 1) // 2) * COLS_DEV + c, (k - 1) % 2)


def pack_kernel(pred_ref, prev_ref, row1_ref, row2_ref, first_ref, second_ref):
    odd = (lax.broadcasted_iota(jnp.int32, (SPECIES, LANES), 1) // 8) % 2 == 1
    _, owner = position()
    even_owner = owner % 2 == 0
    for which, patch_ref in enumerate((pred_ref, prev_ref)):

        def put(at, right, left, which=which):
            put_tile(first_ref, which * MSG + at, jnp.where(even_owner, right, left))
            put_tile(second_ref, which * MSG + at, jnp.where(even_owner, left, right))

        def tile(k, c, which=which, patch_ref=patch_ref):
            return tile_of(patch_ref, (row1_ref, row2_ref), which, k, c)

        for k in range(TILES):
            put(k, tile(k, 2), tile(k, 0))
        for pair in range(TILES // 2):
            low, high = tile(2 * pair, 1), tile(2 * pair + 1, 1)
            put(
                TILES + pair,
                jnp.where(odd, high, roll(low, -8)),
                jnp.where(odd, roll(high, 8), low),
            )
    finish(first_ref, COL_TILES)
    finish(second_ref, COL_TILES)


def own_kernel(pred_ref, prev_ref, row1_ref, row2_ref, own_ref, tile_ref):
    tile_ref[:, SPECIES:24, :] = jnp.zeros((2 * TILES * COLS_DEV, 24 - SPECIES, LANES), f32)
    for which, patch_ref in enumerate((pred_ref, prev_ref)):
        for k in range(TILES):
            for c in range(COLS_DEV):
                tile_ref[(which * TILES + k) * COLS_DEV + c, 0:SPECIES, :] = tile_of(
                    patch_ref, (row1_ref, row2_ref), which, k, c
                )
    blank = jnp.zeros((3, 8, LANES), f32)
    for which in range(2):
        for k in range(TILES):
            tiles = [blank] * 8
            for c in range(COLS_DEV):
                tile = tile_ref[(which * TILES + k) * COLS_DEV + c].reshape(3, 8, LANES)
                tiles[2 + c] = roll(tile, 16 * (2 + c))
            for a, tile in enumerate(mix_blocks(tiles)):
                own_ref[which, k * 8 + a] = tile


def row_faces(face_ref, row):
    idx = (row + 8) // 16
    kap = face_ref[idx, 3]
    south = face_ref[idx, 1] if row % 16 == 8 else kap
    north = face_ref[idx, 2] if row % 16 == 7 else kap
    return face_ref[idx, 0], south, north


def vertical(source, row, faces):
    _, south, north = faces
    if row % 16 in (7, 8):
        return south * source[row - 1] + north * source[row + 1]
    return south * (source[row - 1] + source[row + 1])


def apply_rows(source, lo, hi, blocks, stencil_ref, face_ref, diff, emit):
    for idx in range(6):
        first, last = max(lo, idx * 16 - 8), min(hi, idx * 16 + 8)
        if first >= last:
            continue
        start, stop = first - first % 2, last + last % 2
        parts = []
        for row in range(start, stop, 2):
            x = source[row : row + 2].reshape(48, LANES)
            high = x.astype(bf16)
            parts.append((high, (x - high.astype(f32)).astype(bf16)))
        beside = jnp.dot(
            jnp.concatenate([jnp.concatenate(part, axis=1) for part in parts], axis=0),
            stencil_ref[idx],
            preferred_element_type=f32,
        ).reshape(stop - start, 3, 8, LANES)
        mixed = []
        for at in range(0, len(parts), 2):
            group = parts[at : at + 2]
            high = jnp.concatenate([part[0] for part in group], axis=1)
            low = jnp.concatenate([part[1] for part in group], axis=1)
            m = jnp.dot(
                blocks, jnp.concatenate([high, low, high], axis=0), preferred_element_type=f32
            ).reshape(2, 3, 8, len(group) * LANES)
            for pair in range(len(group)):
                for off in range(2):
                    mixed.append(m[off, :, :, pair * LANES : (pair + 1) * LANES])
        for row in range(first, last):
            faces = row_faces(face_ref, row)
            near = beside[row - start] + vertical(source, row, faces)
            emit(row, faces, diff * near + mixed[row - start])


PAIRS = [(i, j) for j in range(4) for i in range(j + 1)]


class Dots:
    def __init__(self, packed_ref):
        self.sums = {}
        self.packed_ref = packed_ref
        self.half = None
        lane = lanes_of()
        self.own = (lane >= 32) & (lane < 80)
        self.both = self.own | (lane >= 96) | (lane < 16)

    def add(self, basis, row, value):
        if not OWN_LO <= row < OWN_HI:
            return
        if row % 2 == 0:
            self.half = value
            return
        at = (row - OWN_LO) // 2
        value = jnp.where(self.own, self.half, roll(value, 64))
        if basis < 3:
            self.packed_ref[basis, at] = value
        for before in range(basis + 1):
            other = value if before == basis else self.packed_ref[before, at]
            key, term = (before, basis), other * value
            self.sums[key] = self.sums[key] + term if key in self.sums else term

    def write(self, out_ref):
        lane = lanes_of((1, LANES))
        total = jnp.zeros((1, LANES), f32)
        for at, key in enumerate(PAIRS):
            value = jnp.where(self.both, jnp.sum(self.sums[key], axis=0), 0.0)
            value = jnp.sum(jnp.sum(value, axis=0, keepdims=True), axis=1, keepdims=True)
            total = jnp.where(lane == at, value, total)
        out_ref[...] = total


PACKED = (3, (OWN_HI - OWN_LO) // 2, 3, 8, LANES)


def krylov(refs, diag_ref, tables, diff, dots, reach, last_ref):
    for k in range(3):
        source, target = refs[k], last_ref if k == 2 else refs[k + 1]
        width = reach - k - 1
        lo, hi = OWN_LO - width, OWN_HI + width

        def emit(row, faces, rest, source=source, target=target, k=k):
            new = diag_ref[row] * source[row] - rest
            if target is not None:
                target[row] = new
            dots.add(k + 1, row, new)

        apply_rows(source, lo, hi, *tables, diff, emit)


def row_base(face_ref, rate, diff):
    cache = {}

    def base(row):
        kind = ((row + 8) // 16, {7: 1, 8: 2}.get(row % 16, 0))
        if kind not in cache:
            beside, south, north = row_faces(face_ref, row)
            cache[kind] = rate + diff * (beside + (south + north))
        return cache[kind]

    return base


def first_kernel(
    own_ref, col1_ref, col2_ref, face_ref, stencil_ref, param_ref, block_ref,
    state_ref, p0_ref, p1_ref, p2_ref, p3_ref, gram_ref, old_ref, diag_ref, packed_ref,
):
    _, owner = position()
    even_owner, has_left, has_right = owner % 2 == 0, owner > 0, owner < OWNERS - 1
    blank = jnp.zeros((3, 8, LANES), f32)
    for which, target in enumerate((state_ref, old_ref)):

        def beside(at, which=which):
            first, second = (
                get_tile(ref, which * MSG + at).reshape(3, 8, LANES) for ref in (col1_ref, col2_ref)
            )
            left, right = jnp.where(even_owner, second, first), jnp.where(even_owner, first, second)
            return jnp.where(has_left, left, 0.0), jnp.where(has_right, right, 0.0)

        for k in range(TILES):
            if k % 2 == 0:
                far_left, far_right = beside(TILES + k // 2)
            left, right = beside(k)
            tiles = mix_blocks(
                [
                    far_left if k % 2 else roll(far_left, 8),
                    roll(left, 16),
                    blank,
                    blank,
                    blank,
                    roll(right, 80),
                    roll(far_right, 88 if k % 2 else 96),
                    blank,
                ]
            )
            for a in range(8):
                tile = tiles[-a % 8] + own_ref[which, k * 8 + (-a % 8)]
                target[k * 8 + a] = roll(tile, -16 * a) if a else tile
    rate, diff, decay = param_ref[0], param_ref[1], param_ref[2]
    tables = (block_ref[...], stencil_ref, face_ref)
    dots = Dots(packed_ref)
    base_of = row_base(face_ref, rate, diff)

    def emit(row, faces, rest):
        u = state_ref[row]
        base = base_of(row)
        cubic = decay * (u * u)
        new = (base + cubic) * u - rate * old_ref[row] - rest
        diag_ref[row] = (base - THETA / SIGMA) + 3.0 * cubic
        p0_ref[row] = new
        dots.add(0, row, new)

    apply_rows(state_ref, 2, 78, *tables, diff, emit)
    krylov((p0_ref, p1_ref, p2_ref), diag_ref, tables, diff, dots, 6, p3_ref)
    dots.write(gram_ref)


def small_solve(matrix, vector):
    matrix = [list(row) for row in matrix]
    vector = list(vector)
    size = len(vector)
    for col in range(size):
        for target in range(col + 1, size):
            factor = matrix[target][col] / matrix[col][col]
            for at in range(col, size):
                matrix[target][at] = matrix[target][at] - factor * matrix[col][at]
            vector[target] = vector[target] - factor * vector[col]
    answer = [None] * size
    for col in reversed(range(size)):
        running = vector[col]
        for later in range(col + 1, size):
            running = running - matrix[col][later] * answer[later]
        answer[col] = running / matrix[col][col]
    return answer


def combine(parts_ref):
    totals = jnp.sum(parts_ref[...], axis=0, keepdims=True)
    gram = [[None] * 4 for _ in range(4)]
    for at, (i, j) in enumerate(PAIRS):
        gram[i][j] = gram[j][i] = jnp.broadcast_to(totals[:, at : at + 1], (8, LANES))
    zero = jnp.zeros((8, LANES), f32)
    beta = jnp.sqrt(gram[0][0] * (SIGMA * SIGMA) + EPSILON)
    basis = [[-SIGMA / beta]]
    hess = [[zero] * 3 for _ in range(4)]

    def dot(x, y):
        total = x[0] * y[0]
        for at in range(1, len(x)):
            total = total + x[at] * y[at]
        return total

    for j in range(3):
        last = basis[j]
        w = [THETA * last[at] for at in range(j + 1)] + [SIGMA * last[j]]
        for at in range(j):
            w[at + 1] = w[at + 1] + SIGMA * last[at]
        gw = [dot(w, gram[at]) for at in range(j + 2)]
        size = dot(w, gw)
        for i in range(j + 1):
            hess[i][j] = dot(basis[i], gw)
        for i in range(j + 1):
            for at in range(i + 1):
                w[at] = w[at] - hess[i][j] * basis[i][at]
        rest = dot(w, [dot(w, gram[at]) for at in range(j + 2)])
        alive = rest > BREAKDOWN * size
        height = jnp.sqrt(jnp.where(alive, rest, 0.0) + EPSILON)
        hess[j + 1][j] = height
        basis.append([jnp.where(alive, value / height, 0.0) for value in w])
    normal = [[dot([h[i] for h in hess], [h[j] for h in hess]) for j in range(3)] for i in range(3)]
    y = small_solve(normal, [beta * hess[0][i] for i in range(3)])
    out = []
    for at in range(3):
        total = None
        for j in range(at, 3):
            term = y[j] * basis[j][at]
            total = term if total is None else total + term
        out.append(total)
    return out


def second_kernel(
    parts_ref, state_ref, p0_ref, p1_ref, p2_ref, p3_ref, face_ref, stencil_ref, param_ref,
    block_ref, next_ref, q0_ref, q1_ref, q2_ref, gram_ref, diag_ref, packed_ref,
):
    c0, c1, c2 = combine(parts_ref)
    shift = THETA / SIGMA
    rate, diff, decay = param_ref[0], param_ref[1], param_ref[2]
    tables = (block_ref[...], stencil_ref, face_ref)
    dots = Dots(packed_ref)
    base_of = row_base(face_ref, rate - shift, diff)
    a0, a1, a2 = 1.0 + shift * c0, c0 + shift * c1, c1 + shift * c2
    triple = 3.0 * decay
    for row in range(5, 75):
        p0, p1, p2, u = p0_ref[row], p1_ref[row], p2_ref[row], state_ref[row]
        d = c0 * p0 + c1 * p1 + c2 * p2
        linear = (a0 * p0 + a1 * p1) + (a2 * p2 + c2 * p3_ref[row])
        new = linear + (decay * (d * d)) * (3.0 * u + d)
        u = u + d
        diag_ref[row] = base_of(row) + triple * (u * u)
        next_ref[row] = u
        q0_ref[row] = new
        dots.add(0, row, new)
    krylov((q0_ref, q1_ref, q2_ref), diag_ref, tables, diff, dots, 3, None)
    dots.write(gram_ref)


SLOTS = PATCH_DEV + 2 * MOVE_CAP


def last_kernel(parts_ref, next_ref, q0_ref, q1_ref, q2_ref, flag_ref, out_ref, low_ref, high_ref):
    c0, c1, c2 = combine(parts_ref)
    slots_ref = (low_ref, high_ref)
    blank = jnp.zeros((3, 8, LANES), f32)

    def put(half, slot, tile):
        slots_ref[half][slot * 24 : slot * 24 + 24, :] = tile.reshape(24, LANES)

    arrived = {}
    for r in range(ROWS_DEV):
        for half in range(2):
            rows = []
            for a in range(8):
                row = OWN_LO + r * 16 + half * 8 + a
                value = next_ref[row] + (c0 * q0_ref[row] + c1 * q1_ref[row] + c2 * q2_ref[row])
                rows.append(roll(value, 16 * a) if a else value)
            tiles = swap_blocks(rows, range(1, 6))
            for c in range(COLS_DEV):
                slot = r * COLS_DEV + c
                put(half, slot, jnp.where(flag_ref[slot] == 1, tiles[2 + c], 0.0))
            for side, g in enumerate((1, 5)):
                for at, (row_of, m) in enumerate(ARRIVALS):
                    if row_of == r:
                        flag = flag_ref[STAYS + side * len(ARRIVALS) + at] == 1
                        key = (half, PATCH_DEV + side * MOVE_CAP + m)
                        arrived[key] = jnp.where(flag, tiles[g], arrived.get(key, blank))
    for (half, slot), tile in arrived.items():
        put(half, slot, tile)

    for s in range(SPECIES):
        for part in range(SLOTS // 8):
            for half in range(2):
                out_ref[s, part * 8 : part * 8 + 8, half * LANES : (half + 1) * LANES] = slots_ref[
                    half
                ][pl.ds(part * 8 * 24 + s, 8, stride=24), :]


def call(kernel, out_shape, in_specs, scratch=(), limit=16):
    return pl.pallas_call(
        kernel,
        out_shape=out_shape,
        in_specs=in_specs,
        out_specs=jax.tree.map(lambda _: pl.BlockSpec(memory_space=pltpu.VMEM), out_shape),
        scratch_shapes=list(scratch),
        compiler_params=pltpu.CompilerParams(vmem_limit_bytes=limit << 20),
    )


def vm():
    return pl.BlockSpec(memory_space=pltpu.VMEM)


def sm():
    return pl.BlockSpec(memory_space=pltpu.SMEM)


def exchanged(x, axis, odd):
    count = lax.axis_size(axis)
    mates = [((i - odd) ^ 1) + odd for i in range(odd, count + odd)]
    return lax.ppermute(x, axis, [((i + odd) % count, m % count) for i, m in enumerate(mates)])


def summed(gram):
    spread_out = jnp.broadcast_to(gram[None], (DEVICES, 1, LANES))
    return lax.all_to_all(spread_out, EVERY, 0, 0).reshape(DEVICES, LANES)


def per_device(previous, predicted, new_owner, levels, diffusion, decay, reaction):
    prev, pred = (x.reshape(PATCH_DEV * SPECIES * 2, LANES) for x in (previous, predicted))
    shape = jax.ShapeDtypeStruct
    strip = shape((dense(ROW_TILES), LANES), f32)
    local = shape((INPUT_ROWS + 8, LANES), f32)
    far = pl.BlockSpec(memory_space=pltpu.HBM)
    pred, prev, *strips = call(
        row_strip_kernel,
        (local, local, strip, strip),
        [far, far],
        [pltpu.SemaphoreType.DMA((6,))],
    )(pred, prev)
    row1, row2 = (exchanged(x, "grp", odd) for odd, x in enumerate(strips))

    rate = jnp.where(jnp.arange(24) < SPECIES - 1, 4.0, 0.0)
    pad = (0, 24 - SPECIES)
    params = jnp.stack([rate, jnp.pad(diffusion, pad), jnp.pad(decay, pad)]) / SIGMA
    params = jnp.broadcast_to(params.astype(f32)[:, :, None], (3, 24, LANES)).reshape(3, 3, 8, LANES)
    matrix = jnp.pad(reaction / SIGMA, (pad, pad))
    rounded = lax.reduce_precision(matrix, 8, 7)
    high = rounded.astype(bf16)
    low = (matrix - rounded).astype(bf16)
    none = jnp.zeros_like(high)

    def two(x):
        return jnp.concatenate(
            [jnp.concatenate([x, none], axis=1), jnp.concatenate([none, x], axis=1)], axis=0
        )

    blocks = jnp.concatenate([two(high), two(high), two(low)], axis=1)

    faces, stencil, flags = call(
        face_kernel,
        (
            shape((6, 4, 8, LANES), f32),
            shape((6, 2 * LANES, LANES), bf16),
            shape((FLAGS, 8, LANES), jnp.int32),
        ),
        [sm(), sm()],
    )(levels.reshape(-1), new_owner.reshape(-1))
    message = shape((dense(COL_TILES), LANES), f32)
    messages = call(pack_kernel, (message, message), [vm()] * 4)(pred, prev, row1, row2)
    col1, col2 = (exchanged(x, PATCH, odd) for odd, x in enumerate(messages))
    state = shape(STATE, f32)
    gram = shape((1, LANES), f32)
    own = call(
        own_kernel,
        shape((2,) + STATE, f32),
        [vm()] * 4,
        [pltpu.VMEM((2 * TILES * COLS_DEV, 24, LANES), f32)],
    )(pred, prev, row1, row2)
    u0, p0, p1, p2, p3, gram1 = call(
        first_kernel,
        (state,) * 5 + (gram,),
        [vm()] * 7,
        [pltpu.VMEM(STATE, f32), pltpu.VMEM(STATE, f32), pltpu.VMEM(PACKED, f32)],
    )(own, col1, col2, faces, stencil, params, blocks)
    u1, q0, q1, q2, gram2 = call(
        second_kernel,
        (state,) * 4 + (gram,),
        [vm()] * 10,
        [pltpu.VMEM(STATE, f32), pltpu.VMEM(PACKED, f32)],
    )(summed(gram1), u0, p0, p1, p2, p3, faces, stencil, params, blocks)
    out = call(
        last_kernel,
        shape((SPECIES, SLOTS, 2 * LANES), f32),
        [vm()] * 6,
        [pltpu.VMEM((SLOTS * 24, LANES), f32)] * 2,
    )(summed(gram2), u1, q0, q1, q2, flags)
    return jnp.transpose(out, (1, 0, 2))[None, None]


def solution(mesh):
    torus = Mesh(
        mesh.devices.reshape(4, 4, 2, mesh.shape["grp"]), ("patch_0", "patch_1", "patch_2", "grp")
    )
    spec = P("grp", PATCH, None, None, None)
    in_specs = (spec, spec, P(), P(), P(), P(), P())
    return jax.shard_map(
        per_device, mesh=torus, in_specs=in_specs, out_specs=spec, check_vma=False
    )
```

```python
import jax
import jax.numpy as jnp
from jax import lax
from jax.experimental import pallas as pl
from jax.experimental.pallas import tpu as pltpu
from jax.sharding import Mesh
from jax.sharding import PartitionSpec as P

SPECIES = 21
COLS_DEV = 3
ROWS_DEV = 4
MOVE_CAP = 2
PATCH_DEV = 12
BANDS = 4
OWNERS = 32
PATCH = ("patch_0", "patch_1", "patch_2")
EVERY = ("patch_0", "patch_1", "patch_2", "grp")
DEVICES = 128

ROWS = 80
OWN_LO, OWN_HI = 8, 72
LANES = 128
TILES = 10
MSG = TILES + TILES // 2

SIGMA = 32.0
THETA = 14.0
EPSILON = 1e-12
BREAKDOWN = 3e-7

f32 = jnp.float32
bf16 = jnp.bfloat16
STATE = (ROWS, 3, 8, LANES)


def position():
    return lax.axis_index("grp"), lax.axis_index(PATCH)


def lanes_of(shape=(8, LANES)):
    return lax.broadcasted_iota(jnp.int32, shape, len(shape) - 1)


def roll(x, amount):
    return pltpu.roll(x, amount % LANES, axis=x.ndim - 1)


def mix_blocks(rolled):
    group = lanes_of() // 16
    tiles = list(rolled)
    for bit in (1, 2, 4):
        high = (group & bit) != 0
        tiles = [jnp.where(high, tiles[(i + bit) % 8], tiles[i]) for i in range(8)]
    return tiles


def swap_blocks(rolled, wanted):
    tiles = mix_blocks(rolled)
    return {a: roll(tiles[-a % 8], -16 * a) if a else tiles[0] for a in wanted}


STAYS = PATCH_DEV
ARRIVALS = [(r, m) for r in range(ROWS_DEV) for m in range(min(r + 1, MOVE_CAP))]
FLAGS = STAYS + 2 * len(ARRIVALS)


def write_flags(owners_ref, flag_ref, band, owner):
    def put(at, condition):
        flag_ref[at] = jnp.full((8, LANES), jnp.where(condition, 1, 0), jnp.int32)

    for slot in range(PATCH_DEV):
        put(slot, owners_ref[slot, band, owner] == owner)
    sides = (
        (owner > 0, jnp.maximum(owner - 1, 0), COLS_DEV - 1),
        (owner < OWNERS - 1, jnp.minimum(owner + 1, OWNERS - 1), 0),
    )
    for side, (exists, beside, column) in enumerate(sides):
        moving = [
            jnp.where(exists & (owners_ref[r * COLS_DEV + column, band, beside] == owner), 1, 0)
            for r in range(ROWS_DEV)
        ]
        for at, (r, m) in enumerate(ARRIVALS):
            rank = jnp.int32(0)
            for before in range(r):
                rank = rank + moving[before]
            put(STAYS + side * len(ARRIVALS) + at, (moving[r] == 1) & (rank == m))


def write_params(diffusion_ref, decay_ref, param_ref):
    row = lax.broadcasted_iota(jnp.int32, (8, LANES), 0)
    for part in range(3):
        rate = jnp.where(row + 8 * part < SPECIES - 1, 4.0, 0.0)
        diff = decay = jnp.zeros((8, LANES), f32)
        for i in range(min(8, SPECIES - 8 * part)):
            diff = jnp.where(row == i, diffusion_ref[8 * part + i], diff)
            decay = jnp.where(row == i, decay_ref[8 * part + i], decay)
        for at, value in enumerate((rate, diff, decay)):
            param_ref[at, part] = value * (1.0 / SIGMA)


def write_blocks(reaction_ref, block_ref, wide_ref):
    wide_ref[...] = jnp.zeros((24, LANES), f32)
    wide_ref[0:SPECIES, 0:SPECIES] = reaction_ref[...] * (1.0 / SIGMA)
    matrix = wide_ref[...]
    high = matrix.astype(bf16).astype(f32)
    low = matrix - high
    tail = lax.broadcasted_iota(jnp.int32, (24, LANES), 1) < 16
    upper = (high + roll(high, 48)) + roll(low, 96)
    lower = roll(high + roll(high, 48), 24)
    turned = roll(low, 120)
    block_ref[:, 0:LANES] = jnp.concatenate(
        [upper, lower + jnp.where(tail, 0.0, turned)], axis=0
    ).astype(bf16)
    block_ref[:, LANES : 2 * LANES] = jnp.concatenate(
        [jnp.zeros((24, LANES), f32), jnp.where(tail, turned, 0.0)], axis=0
    ).astype(bf16)


def table_kernel(
    levels_ref, owners_ref, diffusion_ref, decay_ref, reaction_ref,
    face_ref, stencil_ref, flag_ref, param_ref, block_ref, wide_ref,
):
    band, owner = position()
    write_flags(owners_ref, flag_ref, band, owner)
    write_params(diffusion_ref, decay_ref, param_ref)
    write_blocks(reaction_ref, block_ref, wide_ref)
    lane_group = lanes_of() // 16
    kappas = []
    for idx in range(6):
        patch_row = band * ROWS_DEV + idx - 1
        row_in = (patch_row >= 0) & (patch_row < BANDS * ROWS_DEV)
        row_safe = jnp.clip(patch_row, 0, BANDS * ROWS_DEV - 1)
        near_band, near_row = row_safe // ROWS_DEV, row_safe % ROWS_DEV
        kap = jnp.zeros((8, LANES), f32)
        for g in range(8):
            near_owner = owner + (g - 2 - (g - 2) % COLS_DEV) // COLS_DEV
            inside = row_in & (near_owner >= 0) & (near_owner < OWNERS)
            safe = jnp.clip(near_owner, 0, OWNERS - 1)
            level = levels_ref[near_row * COLS_DEV + (g - 2) % COLS_DEV, near_band, safe]
            value = jnp.where(level == 0, 1.0, jnp.where(level == 1, 4.0, 16.0))
            value = jnp.where(inside, value, 0.0).astype(f32)
            kap = jnp.where(lane_group == g, value, kap)
        kappas.append(kap)

    def face(own, near):
        return jnp.where(own == 0.0, 0.0, jnp.where(near == 0.0, own, 0.5 * (own + near)))

    source = lax.broadcasted_iota(jnp.int32, (LANES, LANES), 0)
    target = lax.broadcasted_iota(jnp.int32, (LANES, LANES), 1)
    for idx in range(6):
        kap = kappas[idx]
        west, east = face(kap, roll(kap, 1)), face(kap, roll(kap, -1))
        face_ref[idx, 0] = west + east
        face_ref[idx, 1] = face(kap, kappas[max(idx - 1, 0)])
        face_ref[idx, 2] = face(kap, kappas[min(idx + 1, 5)])
        face_ref[idx, 3] = kap
        weights = jnp.where(
            source == target - 1,
            jnp.broadcast_to(west[0:1], (LANES, LANES)),
            jnp.where(source == target + 1, jnp.broadcast_to(east[0:1], (LANES, LANES)), 0.0),
        ).astype(bf16)
        stencil_ref[idx, 0:LANES, :] = weights
        stencil_ref[idx, LANES : 2 * LANES, :] = weights


def half_tile(patch_ref, slot, half):
    return patch_ref[pl.ds(slot * 2 * SPECIES + half, SPECIES, stride=2), :]


ROW_TILES = 2 * COLS_DEV
COL_TILES = 2 * MSG


def dense(tiles):
    return -(-(tiles * SPECIES + 24 - SPECIES) // 8) * 8


def put_tile(ref, at, tile):
    ref[at * SPECIES : (at + 1) * SPECIES, :] = tile


def finish(ref, tiles):
    ref[tiles * SPECIES :, :] = jnp.zeros((dense(tiles) - tiles * SPECIES, LANES), f32)


def get_tile(ref, at):
    tile = ref[at * SPECIES : at * SPECIES + 24, :]
    species = lax.broadcasted_iota(jnp.int32, (24, LANES), 0)
    return jnp.where(species < SPECIES, tile, 0.0)


INPUT_ROWS = PATCH_DEV * 2 * SPECIES
EDGE = 128


def row_strip_kernel(pred_hbm, prev_hbm, pred_ref, prev_ref, first_ref, second_ref, sems):
    band, _ = position()
    even = band % 2 == 0
    top = INPUT_ROWS - EDGE
    spans = ((0, EDGE), (top, EDGE), (EDGE, top - EDGE))
    pairs = ((pred_hbm, pred_ref), (prev_hbm, prev_ref))
    copies = [
        [
            pltpu.make_async_copy(
                source.at[pl.ds(start, size), :],
                target.at[pl.ds(start, size), :],
                sems.at[3 * which + at],
            )
            for at, (start, size) in enumerate(spans)
        ]
        for which, (source, target) in enumerate(pairs)
    ]
    for at in range(3):
        for which in range(2):
            copies[which][at].start()
    for which, (_, patch_ref) in enumerate(pairs):
        copies[which][0].wait()
        copies[which][1].wait()
        for c in range(COLS_DEV):
            up = half_tile(patch_ref, PATCH_DEV - COLS_DEV + c, 1)
            down = half_tile(patch_ref, c, 0)
            put_tile(first_ref, which * COLS_DEV + c, jnp.where(even, up, down))
            put_tile(second_ref, which * COLS_DEV + c, jnp.where(even, down, up))
    finish(first_ref, ROW_TILES)
    finish(second_ref, ROW_TILES)
    copies[0][2].wait()
    copies[1][2].wait()


def tile_of(patch_ref, rows_ref, which, k, c):
    if k in (0, TILES - 1):
        band, _ = position()
        even = band % 2 == 0
        at = (which * COLS_DEV + c) * SPECIES
        first, second = (ref[at : at + SPECIES, :] for ref in rows_ref)
        south, inside = k == 0, (band > 0) if k == 0 else (band < BANDS - 1)
        tile = jnp.where(even, second, first) if south else jnp.where(even, first, second)
        return jnp.where(inside, tile, 0.0)
    return half_tile(patch_ref, ((k - 1) // 2) * COLS_DEV + c, (k - 1) % 2)


def pack_kernel(pred_ref, prev_ref, row1_ref, row2_ref, first_ref, second_ref):
    odd = (lax.broadcasted_iota(jnp.int32, (SPECIES, LANES), 1) // 8) % 2 == 1
    _, owner = position()
    even_owner = owner % 2 == 0
    for which, patch_ref in enumerate((pred_ref, prev_ref)):

        def put(at, right, left, which=which):
            put_tile(first_ref, which * MSG + at, jnp.where(even_owner, right, left))
            put_tile(second_ref, which * MSG + at, jnp.where(even_owner, left, right))

        def tile(k, c, which=which, patch_ref=patch_ref):
            return tile_of(patch_ref, (row1_ref, row2_ref), which, k, c)

        for k in range(TILES):
            put(k, tile(k, 2), tile(k, 0))
        for pair in range(TILES // 2):
            low, high = tile(2 * pair, 1), tile(2 * pair + 1, 1)
            put(
                TILES + pair,
                jnp.where(odd, high, roll(low, -8)),
                jnp.where(odd, roll(high, 8), low),
            )
    finish(first_ref, COL_TILES)
    finish(second_ref, COL_TILES)


def own_kernel(pred_ref, prev_ref, row1_ref, row2_ref, own_ref, tile_ref):
    tile_ref[:, SPECIES:24, :] = jnp.zeros((2 * TILES * COLS_DEV, 24 - SPECIES, LANES), f32)
    for which, patch_ref in enumerate((pred_ref, prev_ref)):
        for k in range(TILES):
            for c in range(COLS_DEV):
                tile_ref[(which * TILES + k) * COLS_DEV + c, 0:SPECIES, :] = tile_of(
                    patch_ref, (row1_ref, row2_ref), which, k, c
                )
    blank = jnp.zeros((3, 8, LANES), f32)
    for which in range(2):
        for k in range(TILES):
            tiles = [blank] * 8
            for c in range(COLS_DEV):
                tile = tile_ref[(which * TILES + k) * COLS_DEV + c].reshape(3, 8, LANES)
                tiles[2 + c] = roll(tile, 16 * (2 + c))
            for a, tile in enumerate(mix_blocks(tiles)):
                own_ref[which, k * 8 + a] = tile


def row_faces(face_ref, row):
    idx = (row + 8) // 16
    kap = face_ref[idx, 3]
    south = face_ref[idx, 1] if row % 16 == 8 else kap
    north = face_ref[idx, 2] if row % 16 == 7 else kap
    return face_ref[idx, 0], south, north


def vertical(source, row, faces):
    _, south, north = faces
    if row % 16 in (7, 8):
        return south * source[row - 1] + north * source[row + 1]
    return south * (source[row - 1] + source[row + 1])


def apply_rows(source, lo, hi, blocks, stencil_ref, face_ref, diff, emit):
    for idx in range(6):
        first, last = max(lo, idx * 16 - 8), min(hi, idx * 16 + 8)
        if first >= last:
            continue
        start, stop = first - first % 2, last + last % 2
        parts = []
        for row in range(start, stop, 2):
            x = source[row : row + 2].reshape(48, LANES)
            high = x.astype(bf16)
            parts.append((high, (x - high.astype(f32)).astype(bf16)))
        beside = jnp.dot(
            jnp.concatenate([jnp.concatenate(part, axis=1) for part in parts], axis=0),
            stencil_ref[idx],
            preferred_element_type=f32,
        ).reshape(stop - start, 3, 8, LANES)
        mixed = []
        for at in range(0, len(parts), 2):
            group = parts[at : at + 2]
            high = jnp.concatenate([part[0] for part in group], axis=1)
            low = jnp.concatenate([part[1] for part in group], axis=1)
            m = jnp.dot(
                blocks, jnp.concatenate([high, low, high], axis=0), preferred_element_type=f32
            ).reshape(2, 3, 8, len(group) * LANES)
            for pair in range(len(group)):
                for off in range(2):
                    mixed.append(m[off, :, :, pair * LANES : (pair + 1) * LANES])
        for row in range(first, last):
            faces = row_faces(face_ref, row)
            near = beside[row - start] + vertical(source, row, faces)
            emit(row, faces, diff * near + mixed[row - start])


PAIRS = [(i, j) for j in range(4) for i in range(j + 1)]


class Dots:
    def __init__(self, packed_ref):
        self.sums = {}
        self.packed_ref = packed_ref
        self.half = None
        lane = lanes_of()
        self.own = (lane >= 32) & (lane < 80)
        self.both = self.own | (lane >= 96) | (lane < 16)

    def add(self, basis, row, value):
        if not OWN_LO <= row < OWN_HI:
            return
        if row % 2 == 0:
            self.half = value
            return
        at = (row - OWN_LO) // 2
        value = jnp.where(self.own, self.half, roll(value, 64))
        if basis < 3:
            self.packed_ref[basis, at] = value
        for before in range(basis + 1):
            other = value if before == basis else self.packed_ref[before, at]
            key, term = (before, basis), other * value
            self.sums[key] = self.sums[key] + term if key in self.sums else term

    def write(self, out_ref):
        lane = lanes_of((1, LANES))
        total = jnp.zeros((1, LANES), f32)
        for at, key in enumerate(PAIRS):
            value = jnp.where(self.both, jnp.sum(self.sums[key], axis=0), 0.0)
            value = jnp.sum(jnp.sum(value, axis=0, keepdims=True), axis=1, keepdims=True)
            total = jnp.where(lane == at, value, total)
        out_ref[...] = total


PACKED = (3, (OWN_HI - OWN_LO) // 2, 3, 8, LANES)


def krylov(refs, diag_ref, tables, diff, dots, reach, last_ref):
    for k in range(3):
        source, target = refs[k], last_ref if k == 2 else refs[k + 1]
        width = reach - k - 1
        lo, hi = OWN_LO - width, OWN_HI + width

        def emit(row, faces, rest, source=source, target=target, k=k):
            new = diag_ref[row] * source[row] - rest
            if target is not None:
                target[row] = new
            dots.add(k + 1, row, new)

        apply_rows(source, lo, hi, *tables, diff, emit)


def row_base(face_ref, rate, diff):
    cache = {}

    def base(row):
        kind = ((row + 8) // 16, {7: 1, 8: 2}.get(row % 16, 0))
        if kind not in cache:
            beside, south, north = row_faces(face_ref, row)
            cache[kind] = rate + diff * (beside + (south + north))
        return cache[kind]

    return base


def first_kernel(
    own_ref, col1_ref, col2_ref, face_ref, stencil_ref, param_ref, block_ref,
    state_ref, p0_ref, p1_ref, p2_ref, p3_ref, gram_ref, old_ref, diag_ref, packed_ref,
):
    _, owner = position()
    even_owner, has_left, has_right = owner % 2 == 0, owner > 0, owner < OWNERS - 1
    blank = jnp.zeros((3, 8, LANES), f32)
    for which, target in enumerate((state_ref, old_ref)):

        def beside(at, which=which):
            first, second = (
                get_tile(ref, which * MSG + at).reshape(3, 8, LANES) for ref in (col1_ref, col2_ref)
            )
            left, right = jnp.where(even_owner, second, first), jnp.where(even_owner, first, second)
            return jnp.where(has_left, left, 0.0), jnp.where(has_right, right, 0.0)

        for k in range(TILES):
            if k % 2 == 0:
                far_left, far_right = beside(TILES + k // 2)
            left, right = beside(k)
            tiles = mix_blocks(
                [
                    far_left if k % 2 else roll(far_left, 8),
                    roll(left, 16),
                    blank,
                    blank,
                    blank,
                    roll(right, 80),
                    roll(far_right, 88 if k % 2 else 96),
                    blank,
                ]
            )
            for a in range(8):
                tile = tiles[-a % 8] + own_ref[which, k * 8 + (-a % 8)]
                target[k * 8 + a] = roll(tile, -16 * a) if a else tile
    rate, diff, decay = param_ref[0], param_ref[1], param_ref[2]
    tables = (block_ref[:, 0:144], stencil_ref, face_ref)
    dots = Dots(packed_ref)
    base_of = row_base(face_ref, rate, diff)

    def emit(row, faces, rest):
        u = state_ref[row]
        base = base_of(row)
        cubic = decay * (u * u)
        new = (base + cubic) * u - rate * old_ref[row] - rest
        diag_ref[row] = (base - THETA / SIGMA) + 3.0 * cubic
        p0_ref[row] = new
        dots.add(0, row, new)

    apply_rows(state_ref, 2, 78, *tables, diff, emit)
    krylov((p0_ref, p1_ref, p2_ref), diag_ref, tables, diff, dots, 6, p3_ref)
    dots.write(gram_ref)


def small_solve(matrix, vector):
    matrix = [list(row) for row in matrix]
    vector = list(vector)
    size = len(vector)
    for col in range(size):
        for target in range(col + 1, size):
            factor = matrix[target][col] / matrix[col][col]
            for at in range(col, size):
                matrix[target][at] = matrix[target][at] - factor * matrix[col][at]
            vector[target] = vector[target] - factor * vector[col]
    answer = [None] * size
    for col in reversed(range(size)):
        running = vector[col]
        for later in range(col + 1, size):
            running = running - matrix[col][later] * answer[later]
        answer[col] = running / matrix[col][col]
    return answer


def combine(parts_ref):
    totals = jnp.sum(parts_ref[...], axis=0, keepdims=True)
    gram = [[None] * 4 for _ in range(4)]
    for at, (i, j) in enumerate(PAIRS):
        gram[i][j] = gram[j][i] = jnp.broadcast_to(totals[:, at : at + 1], (8, LANES))
    zero = jnp.zeros((8, LANES), f32)
    beta = jnp.sqrt(gram[0][0] * (SIGMA * SIGMA) + EPSILON)
    basis = [[-SIGMA / beta]]
    hess = [[zero] * 3 for _ in range(4)]

    def dot(x, y):
        total = x[0] * y[0]
        for at in range(1, len(x)):
            total = total + x[at] * y[at]
        return total

    for j in range(3):
        last = basis[j]
        w = [THETA * last[at] for at in range(j + 1)] + [SIGMA * last[j]]
        for at in range(j):
            w[at + 1] = w[at + 1] + SIGMA * last[at]
        gw = [dot(w, gram[at]) for at in range(j + 2)]
        size = dot(w, gw)
        for i in range(j + 1):
            hess[i][j] = dot(basis[i], gw)
        for i in range(j + 1):
            for at in range(i + 1):
                w[at] = w[at] - hess[i][j] * basis[i][at]
        rest = dot(w, [dot(w, gram[at]) for at in range(j + 2)])
        alive = rest > BREAKDOWN * size
        height = jnp.sqrt(jnp.where(alive, rest, 0.0) + EPSILON)
        hess[j + 1][j] = height
        basis.append([jnp.where(alive, value / height, 0.0) for value in w])
    normal = [[dot([h[i] for h in hess], [h[j] for h in hess]) for j in range(3)] for i in range(3)]
    y = small_solve(normal, [beta * hess[0][i] for i in range(3)])
    out = []
    for at in range(3):
        total = None
        for j in range(at, 3):
            term = y[j] * basis[j][at]
            total = term if total is None else total + term
        out.append(total)
    return out


def second_kernel(
    parts_ref, state_ref, p0_ref, p1_ref, p2_ref, p3_ref, face_ref, stencil_ref, param_ref,
    block_ref, next_ref, q0_ref, q1_ref, q2_ref, gram_ref, diag_ref, packed_ref,
):
    c0, c1, c2 = combine(parts_ref)
    shift = THETA / SIGMA
    rate, diff, decay = param_ref[0], param_ref[1], param_ref[2]
    tables = (block_ref[:, 0:144], stencil_ref, face_ref)
    dots = Dots(packed_ref)
    base_of = row_base(face_ref, rate - shift, diff)
    a0, a1, a2 = 1.0 + shift * c0, c0 + shift * c1, c1 + shift * c2
    triple = 3.0 * decay
    for row in range(5, 75):
        p0, p1, p2, u = p0_ref[row], p1_ref[row], p2_ref[row], state_ref[row]
        d = c0 * p0 + c1 * p1 + c2 * p2
        linear = (a0 * p0 + a1 * p1) + (a2 * p2 + c2 * p3_ref[row])
        new = linear + (decay * (d * d)) * (3.0 * u + d)
        u = u + d
        diag_ref[row] = base_of(row) + triple * (u * u)
        next_ref[row] = u
        q0_ref[row] = new
        dots.add(0, row, new)
    krylov((q0_ref, q1_ref, q2_ref), diag_ref, tables, diff, dots, 3, None)
    dots.write(gram_ref)


SLOTS = PATCH_DEV + 2 * MOVE_CAP


def last_kernel(parts_ref, next_ref, q0_ref, q1_ref, q2_ref, flag_ref, out_ref, low_ref, high_ref):
    c0, c1, c2 = combine(parts_ref)
    slots_ref = (low_ref, high_ref)
    blank = jnp.zeros((3, 8, LANES), f32)

    def put(half, slot, tile):
        slots_ref[half][slot * 24 : slot * 24 + 24, :] = tile.reshape(24, LANES)

    arrived = {}
    for r in range(ROWS_DEV):
        for half in range(2):
            rows = []
            for a in range(8):
                row = OWN_LO + r * 16 + half * 8 + a
                value = next_ref[row] + (c0 * q0_ref[row] + c1 * q1_ref[row] + c2 * q2_ref[row])
                rows.append(roll(value, 16 * a) if a else value)
            tiles = swap_blocks(rows, range(1, 6))
            for c in range(COLS_DEV):
                slot = r * COLS_DEV + c
                put(half, slot, jnp.where(flag_ref[slot] == 1, tiles[2 + c], 0.0))
            for side, g in enumerate((1, 5)):
                for at, (row_of, m) in enumerate(ARRIVALS):
                    if row_of == r:
                        flag = flag_ref[STAYS + side * len(ARRIVALS) + at] == 1
                        key = (half, PATCH_DEV + side * MOVE_CAP + m)
                        arrived[key] = jnp.where(flag, tiles[g], arrived.get(key, blank))
    for (half, slot), tile in arrived.items():
        put(half, slot, tile)

    for s in range(SPECIES):
        for part in range(SLOTS // 8):
            for half in range(2):
                out_ref[s, part * 8 : part * 8 + 8, half * LANES : (half + 1) * LANES] = slots_ref[
                    half
                ][pl.ds(part * 8 * 24 + s, 8, stride=24), :]


def call(kernel, out_shape, in_specs, scratch=(), limit=16):
    return pl.pallas_call(
        kernel,
        out_shape=out_shape,
        in_specs=in_specs,
        out_specs=jax.tree.map(lambda _: pl.BlockSpec(memory_space=pltpu.VMEM), out_shape),
        scratch_shapes=list(scratch),
        compiler_params=pltpu.CompilerParams(vmem_limit_bytes=limit << 20),
    )


def vm():
    return pl.BlockSpec(memory_space=pltpu.VMEM)


def sm():
    return pl.BlockSpec(memory_space=pltpu.SMEM)


def in_hbm(x):
    return pltpu.with_memory_space_constraint(x, pltpu.HBM)


def exchanged(x, axis, odd):
    count = lax.axis_size(axis)
    mates = [((i - odd) ^ 1) + odd for i in range(count)]
    pairs = [(i, m if 0 <= m < count else i) for i, m in enumerate(mates)]
    return lax.ppermute(x, axis, pairs)


def summed(gram):
    spread_out = jnp.broadcast_to(gram[None], (DEVICES, 1, LANES))
    return lax.all_to_all(spread_out, EVERY, 0, 0).reshape(DEVICES, LANES)


def per_device(previous, predicted, new_owner, levels, diffusion, decay, reaction):
    prev, pred = (x.reshape(PATCH_DEV * SPECIES * 2, LANES) for x in (previous, predicted))
    shape = jax.ShapeDtypeStruct
    strip = shape((dense(ROW_TILES), LANES), f32)
    local = shape((INPUT_ROWS + 8, LANES), f32)
    far = pl.BlockSpec(memory_space=pltpu.HBM)
    pred, prev, *strips = call(
        row_strip_kernel,
        (local, local, strip, strip),
        [far, far],
        [pltpu.SemaphoreType.DMA((6,))],
    )(in_hbm(pred), in_hbm(prev))
    row1, row2 = (exchanged(x, "grp", odd) for odd, x in enumerate(strips))

    message = shape((dense(COL_TILES), LANES), f32)
    messages = call(pack_kernel, (message, message), [vm()] * 4)(pred, prev, row1, row2)
    inputs = (new_owner, levels, diffusion, decay, reaction)
    messages, inputs = lax.optimization_barrier((tuple(messages), inputs))
    new_owner, levels, diffusion, decay, reaction = inputs
    col1, col2 = (exchanged(x, PATCH, odd) for odd, x in enumerate(messages))
    faces, stencil, flags, params, blocks = call(
        table_kernel,
        (
            shape((6, 4, 8, LANES), f32),
            shape((6, 2 * LANES, LANES), bf16),
            shape((FLAGS, 8, LANES), jnp.int32),
            shape((3, 3, 8, LANES), f32),
            shape((48, 2 * LANES), bf16),
        ),
        [sm()] * 4 + [vm()],
        [pltpu.VMEM((24, LANES), f32)],
    )(
        *(
            in_hbm(x)
            for x in (
                levels.transpose(2, 0, 1),
                new_owner.transpose(2, 0, 1),
                diffusion,
                decay,
                reaction,
            )
        )
    )
    state = shape(STATE, f32)
    gram = shape((1, LANES), f32)
    own = call(
        own_kernel,
        shape((2,) + STATE, f32),
        [vm()] * 4,
        [pltpu.VMEM((2 * TILES * COLS_DEV, 24, LANES), f32)],
    )(pred, prev, row1, row2)
    u0, p0, p1, p2, p3, gram1 = call(
        first_kernel,
        (state,) * 5 + (gram,),
        [vm()] * 7,
        [pltpu.VMEM(STATE, f32), pltpu.VMEM(STATE, f32), pltpu.VMEM(PACKED, f32)],
    )(own, col1, col2, faces, stencil, params, blocks)
    u1, q0, q1, q2, gram2 = call(
        second_kernel,
        (state,) * 4 + (gram,),
        [vm()] * 10,
        [pltpu.VMEM(STATE, f32), pltpu.VMEM(PACKED, f32)],
    )(summed(gram1), u0, p0, p1, p2, p3, faces, stencil, params, blocks)
    out = call(
        last_kernel,
        shape((SPECIES, SLOTS, 2 * LANES), f32),
        [vm()] * 6,
        [pltpu.VMEM((SLOTS * 24, LANES), f32)] * 2,
    )(summed(gram2), u1, q0, q1, q2, flags)
    return jnp.transpose(out, (1, 0, 2))[None, None]


def solution(mesh):
    torus = Mesh(
        mesh.devices.reshape(4, 4, 2, mesh.shape["grp"]), ("patch_0", "patch_1", "patch_2", "grp")
    )
    spec = P("grp", PATCH, None, None, None)
    in_specs = (spec, spec, P(), P(), P(), P(), P())
    return jax.shard_map(
        per_device, mesh=torus, in_specs=in_specs, out_specs=spec, check_vma=False
    )
```

```python
import jax
import jax.numpy as jnp
from jax import lax
from jax.experimental import pallas as pl
from jax.experimental.pallas import tpu as pltpu
from jax.sharding import Mesh
from jax.sharding import PartitionSpec as P

SPECIES = 21
COLS_DEV = 3
ROWS_DEV = 4
MOVE_CAP = 2
PATCH_DEV = 12
BANDS = 4
OWNERS = 32
PATCH = ("patch_0", "patch_1", "patch_2")
EVERY = ("patch_0", "patch_1", "patch_2", "grp")
DEVICES = 128

ROWS = 80
OWN_LO, OWN_HI = 8, 72
LANES = 128
TILES = 10
MSG = TILES + TILES // 2

SIGMA = 32.0
THETA = 14.0
EPSILON = 1e-12
BREAKDOWN = 3e-7

f32 = jnp.float32
bf16 = jnp.bfloat16
STATE = (ROWS, 3, 8, LANES)


def position():
    return lax.axis_index("grp"), lax.axis_index(PATCH)


def lanes_of(shape=(8, LANES)):
    return lax.broadcasted_iota(jnp.int32, shape, len(shape) - 1)


def roll(x, amount):
    return pltpu.roll(x, amount % LANES, axis=x.ndim - 1)


def mix_blocks(rolled):
    group = lanes_of() // 16
    tiles = list(rolled)
    for bit in (1, 2, 4):
        high = (group & bit) != 0
        tiles = [jnp.where(high, tiles[(i + bit) % 8], tiles[i]) for i in range(8)]
    return tiles


def swap_blocks(rolled, wanted):
    tiles = mix_blocks(rolled)
    return {a: roll(tiles[-a % 8], -16 * a) if a else tiles[0] for a in wanted}


STAYS = PATCH_DEV
ARRIVALS = [(r, m) for r in range(ROWS_DEV) for m in range(min(r + 1, MOVE_CAP))]
FLAGS = STAYS + 2 * len(ARRIVALS)


def write_flags(owners_ref, flag_ref, band, owner):
    def put(at, condition):
        flag_ref[at] = jnp.full((8, LANES), jnp.where(condition, 1, 0), jnp.int32)

    for slot in range(PATCH_DEV):
        put(slot, owners_ref[slot, band, owner] == owner)
    sides = (
        (owner > 0, jnp.maximum(owner - 1, 0), COLS_DEV - 1),
        (owner < OWNERS - 1, jnp.minimum(owner + 1, OWNERS - 1), 0),
    )
    for side, (exists, beside, column) in enumerate(sides):
        moving = [
            jnp.where(exists & (owners_ref[r * COLS_DEV + column, band, beside] == owner), 1, 0)
            for r in range(ROWS_DEV)
        ]
        for at, (r, m) in enumerate(ARRIVALS):
            rank = jnp.int32(0)
            for before in range(r):
                rank = rank + moving[before]
            put(STAYS + side * len(ARRIVALS) + at, (moving[r] == 1) & (rank == m))


def write_params(diffusion_ref, decay_ref, param_ref):
    row = lax.broadcasted_iota(jnp.int32, (8, LANES), 0)
    for part in range(3):
        rate = jnp.where(row + 8 * part < SPECIES - 1, 4.0, 0.0)
        diff = decay = jnp.zeros((8, LANES), f32)
        for i in range(min(8, SPECIES - 8 * part)):
            diff = jnp.where(row == i, diffusion_ref[8 * part + i], diff)
            decay = jnp.where(row == i, decay_ref[8 * part + i], decay)
        for at, value in enumerate((rate, diff, decay)):
            param_ref[at, part] = value * (1.0 / SIGMA)


def write_blocks(reaction_ref, block_ref, wide_ref):
    wide_ref[...] = jnp.zeros((24, LANES), f32)
    wide_ref[0:SPECIES, 0:SPECIES] = reaction_ref[...] * (1.0 / SIGMA)
    matrix = wide_ref[...]
    high = matrix.astype(bf16).astype(f32)
    low = matrix - high
    tail = lax.broadcasted_iota(jnp.int32, (24, LANES), 1) < 16
    upper = (high + roll(high, 48)) + roll(low, 96)
    lower = roll(high + roll(high, 48), 24)
    turned = roll(low, 120)
    block_ref[:, 0:LANES] = jnp.concatenate(
        [upper, lower + jnp.where(tail, 0.0, turned)], axis=0
    ).astype(bf16)
    block_ref[:, LANES : 2 * LANES] = jnp.concatenate(
        [jnp.zeros((24, LANES), f32), jnp.where(tail, turned, 0.0)], axis=0
    ).astype(bf16)


def table_kernel(
    levels_ref, owners_ref, diffusion_ref, decay_ref, reaction_ref,
    face_ref, stencil_ref, flag_ref, param_ref, block_ref, wide_ref,
):
    band, owner = position()
    write_flags(owners_ref, flag_ref, band, owner)
    write_params(diffusion_ref, decay_ref, param_ref)
    write_blocks(reaction_ref, block_ref, wide_ref)
    lane_group = lanes_of() // 16
    kappas = []
    for idx in range(6):
        patch_row = band * ROWS_DEV + idx - 1
        row_in = (patch_row >= 0) & (patch_row < BANDS * ROWS_DEV)
        row_safe = jnp.clip(patch_row, 0, BANDS * ROWS_DEV - 1)
        near_band, near_row = row_safe // ROWS_DEV, row_safe % ROWS_DEV
        kap = jnp.zeros((8, LANES), f32)
        for g in range(8):
            near_owner = owner + (g - 2 - (g - 2) % COLS_DEV) // COLS_DEV
            inside = row_in & (near_owner >= 0) & (near_owner < OWNERS)
            safe = jnp.clip(near_owner, 0, OWNERS - 1)
            level = levels_ref[near_row * COLS_DEV + (g - 2) % COLS_DEV, near_band, safe]
            value = jnp.where(level == 0, 1.0, jnp.where(level == 1, 4.0, 16.0))
            value = jnp.where(inside, value, 0.0).astype(f32)
            kap = jnp.where(lane_group == g, value, kap)
        kappas.append(kap)

    def face(own, near):
        return jnp.where(own == 0.0, 0.0, jnp.where(near == 0.0, own, 0.5 * (own + near)))

    source = lax.broadcasted_iota(jnp.int32, (LANES, LANES), 0)
    target = lax.broadcasted_iota(jnp.int32, (LANES, LANES), 1)
    for idx in range(6):
        kap = kappas[idx]
        west, east = face(kap, roll(kap, 1)), face(kap, roll(kap, -1))
        face_ref[idx, 0] = west + east
        face_ref[idx, 1] = face(kap, kappas[max(idx - 1, 0)])
        face_ref[idx, 2] = face(kap, kappas[min(idx + 1, 5)])
        face_ref[idx, 3] = kap
        weights = jnp.where(
            source == target - 1,
            jnp.broadcast_to(west[0:1], (LANES, LANES)),
            jnp.where(source == target + 1, jnp.broadcast_to(east[0:1], (LANES, LANES)), 0.0),
        ).astype(bf16)
        stencil_ref[idx, 0:LANES, :] = weights
        stencil_ref[idx, LANES : 2 * LANES, :] = weights


def half_tile(patch_ref, slot, half):
    return patch_ref[pl.ds(slot * 2 * SPECIES + half, SPECIES, stride=2), :]


ROW_TILES = 2 * COLS_DEV
COL_TILES = 2 * MSG


def dense(tiles):
    return -(-(tiles * SPECIES + 24 - SPECIES) // 8) * 8


def put_tile(ref, at, tile):
    ref[at * SPECIES : (at + 1) * SPECIES, :] = tile


def finish(ref, tiles):
    ref[tiles * SPECIES :, :] = jnp.zeros((dense(tiles) - tiles * SPECIES, LANES), f32)


def get_tile(ref, at):
    tile = ref[at * SPECIES : at * SPECIES + 24, :]
    species = lax.broadcasted_iota(jnp.int32, (24, LANES), 0)
    return jnp.where(species < SPECIES, tile, 0.0)


INPUT_ROWS = PATCH_DEV * 2 * SPECIES
EDGE = 128


def row_strip_kernel(pred_hbm, prev_hbm, pred_ref, prev_ref, first_ref, second_ref, sems):
    band, _ = position()
    even = band % 2 == 0
    top = INPUT_ROWS - EDGE
    spans = ((0, EDGE), (top, EDGE), (EDGE, top - EDGE))
    pairs = ((pred_hbm, pred_ref), (prev_hbm, prev_ref))
    copies = [
        [
            pltpu.make_async_copy(
                source.at[pl.ds(start, size), :],
                target.at[pl.ds(start, size), :],
                sems.at[3 * which + at],
            )
            for at, (start, size) in enumerate(spans)
        ]
        for which, (source, target) in enumerate(pairs)
    ]
    for at in range(3):
        for which in range(2):
            copies[which][at].start()
    for which, (_, patch_ref) in enumerate(pairs):
        copies[which][0].wait()
        copies[which][1].wait()
        for c in range(COLS_DEV):
            up = half_tile(patch_ref, PATCH_DEV - COLS_DEV + c, 1)
            down = half_tile(patch_ref, c, 0)
            put_tile(first_ref, which * COLS_DEV + c, jnp.where(even, up, down))
            put_tile(second_ref, which * COLS_DEV + c, jnp.where(even, down, up))
    finish(first_ref, ROW_TILES)
    finish(second_ref, ROW_TILES)
    copies[0][2].wait()
    copies[1][2].wait()


def tile_of(patch_ref, rows_ref, which, k, c):
    if k in (0, TILES - 1):
        band, _ = position()
        even = band % 2 == 0
        at = (which * COLS_DEV + c) * SPECIES
        first, second = (ref[at : at + SPECIES, :] for ref in rows_ref)
        south, inside = k == 0, (band > 0) if k == 0 else (band < BANDS - 1)
        tile = jnp.where(even, second, first) if south else jnp.where(even, first, second)
        return jnp.where(inside, tile, 0.0)
    return half_tile(patch_ref, ((k - 1) // 2) * COLS_DEV + c, (k - 1) % 2)


def pack_kernel(pred_ref, prev_ref, row1_ref, row2_ref, first_ref, second_ref):
    odd = (lax.broadcasted_iota(jnp.int32, (SPECIES, LANES), 1) // 8) % 2 == 1
    _, owner = position()
    even_owner = owner % 2 == 0
    for which, patch_ref in enumerate((pred_ref, prev_ref)):

        def put(at, right, left, which=which):
            put_tile(first_ref, which * MSG + at, jnp.where(even_owner, right, left))
            put_tile(second_ref, which * MSG + at, jnp.where(even_owner, left, right))

        def tile(k, c, which=which, patch_ref=patch_ref):
            return tile_of(patch_ref, (row1_ref, row2_ref), which, k, c)

        for k in range(TILES):
            put(k, tile(k, 2), tile(k, 0))
        for pair in range(TILES // 2):
            low, high = tile(2 * pair, 1), tile(2 * pair + 1, 1)
            put(
                TILES + pair,
                jnp.where(odd, high, roll(low, -8)),
                jnp.where(odd, roll(high, 8), low),
            )
    finish(first_ref, COL_TILES)
    finish(second_ref, COL_TILES)


def own_kernel(pred_ref, prev_ref, row1_ref, row2_ref, own_ref, tile_ref):
    tile_ref[:, SPECIES:24, :] = jnp.zeros((2 * TILES * COLS_DEV, 24 - SPECIES, LANES), f32)
    for which, patch_ref in enumerate((pred_ref, prev_ref)):
        for k in range(TILES):
            for c in range(COLS_DEV):
                tile_ref[(which * TILES + k) * COLS_DEV + c, 0:SPECIES, :] = tile_of(
                    patch_ref, (row1_ref, row2_ref), which, k, c
                )
    blank = jnp.zeros((3, 8, LANES), f32)
    for which in range(2):
        for k in range(TILES):
            tiles = [blank] * 8
            for c in range(COLS_DEV):
                tile = tile_ref[(which * TILES + k) * COLS_DEV + c].reshape(3, 8, LANES)
                tiles[2 + c] = roll(tile, 16 * (2 + c))
            for a, tile in enumerate(mix_blocks(tiles)):
                own_ref[which, k * 8 + a] = tile


def row_faces(face_ref, row):
    idx = (row + 8) // 16
    kap = face_ref[idx, 3]
    south = face_ref[idx, 1] if row % 16 == 8 else kap
    north = face_ref[idx, 2] if row % 16 == 7 else kap
    return face_ref[idx, 0], south, north


def vertical(source, row, faces):
    _, south, north = faces
    if row % 16 in (7, 8):
        return south * source[row - 1] + north * source[row + 1]
    return south * (source[row - 1] + source[row + 1])


def apply_rows(source, lo, hi, blocks, stencil_ref, face_ref, diff, emit):
    for idx in range(6):
        first, last = max(lo, idx * 16 - 8), min(hi, idx * 16 + 8)
        if first >= last:
            continue
        start, stop = first - first % 2, last + last % 2
        parts = []
        for row in range(start, stop, 2):
            x = source[row : row + 2].reshape(48, LANES)
            high = x.astype(bf16)
            parts.append((high, (x - high.astype(f32)).astype(bf16)))
        beside = jnp.dot(
            jnp.concatenate([jnp.concatenate(part, axis=1) for part in parts], axis=0),
            stencil_ref[idx],
            preferred_element_type=f32,
        ).reshape(stop - start, 3, 8, LANES)
        mixed = []
        for at in range(0, len(parts), 2):
            group = parts[at : at + 2]
            high = jnp.concatenate([part[0] for part in group], axis=1)
            low = jnp.concatenate([part[1] for part in group], axis=1)
            m = jnp.dot(
                blocks, jnp.concatenate([high, low, high], axis=0), preferred_element_type=f32
            ).reshape(2, 3, 8, len(group) * LANES)
            for pair in range(len(group)):
                for off in range(2):
                    mixed.append(m[off, :, :, pair * LANES : (pair + 1) * LANES])
        for row in range(first, last):
            faces = row_faces(face_ref, row)
            near = beside[row - start] + vertical(source, row, faces)
            emit(row, faces, diff * near + mixed[row - start])


PAIRS = [(i, j) for j in range(4) for i in range(j + 1)]


class Dots:
    def __init__(self, packed_ref):
        self.sums = {}
        self.packed_ref = packed_ref
        self.half = None
        lane = lanes_of()
        self.own = (lane >= 32) & (lane < 80)
        self.both = self.own | (lane >= 96) | (lane < 16)

    def add(self, basis, row, value):
        if not OWN_LO <= row < OWN_HI:
            return
        if row % 2 == 0:
            self.half = value
            return
        at = (row - OWN_LO) // 2
        value = jnp.where(self.own, self.half, roll(value, 64))
        if basis < 3:
            self.packed_ref[basis, at] = value
        for before in range(basis + 1):
            other = value if before == basis else self.packed_ref[before, at]
            key, term = (before, basis), other * value
            self.sums[key] = self.sums[key] + term if key in self.sums else term

    def write(self, out_ref):
        lane = lanes_of((1, LANES))
        total = jnp.zeros((1, LANES), f32)
        for at, key in enumerate(PAIRS):
            value = jnp.where(self.both, jnp.sum(self.sums[key], axis=0), 0.0)
            value = jnp.sum(jnp.sum(value, axis=0, keepdims=True), axis=1, keepdims=True)
            total = jnp.where(lane == at, value, total)
        out_ref[...] = total


PACKED = (3, (OWN_HI - OWN_LO) // 2, 3, 8, LANES)


def krylov(refs, diag_ref, tables, diff, dots, reach, last_ref):
    for k in range(3):
        source, target = refs[k], last_ref if k == 2 else refs[k + 1]
        width = reach - k - 1
        lo, hi = OWN_LO - width, OWN_HI + width

        def emit(row, faces, rest, source=source, target=target, k=k):
            new = diag_ref[row] * source[row] - rest
            if target is not None:
                target[row] = new
            dots.add(k + 1, row, new)

        apply_rows(source, lo, hi, *tables, diff, emit)


def row_base(face_ref, rate, diff):
    cache = {}

    def base(row):
        kind = ((row + 8) // 16, {7: 1, 8: 2}.get(row % 16, 0))
        if kind not in cache:
            beside, south, north = row_faces(face_ref, row)
            cache[kind] = rate + diff * (beside + (south + north))
        return cache[kind]

    return base


def first_kernel(
    own_ref, col1_ref, col2_ref, face_ref, stencil_ref, param_ref, block_ref,
    state_ref, p0_ref, p1_ref, p2_ref, p3_ref, gram_ref, old_ref, diag_ref, packed_ref,
):
    _, owner = position()
    even_owner, has_left, has_right = owner % 2 == 0, owner > 0, owner < OWNERS - 1
    blank = jnp.zeros((3, 8, LANES), f32)
    for which, target in enumerate((state_ref, old_ref)):

        def beside(at, which=which):
            first, second = (
                get_tile(ref, which * MSG + at).reshape(3, 8, LANES) for ref in (col1_ref, col2_ref)
            )
            left, right = jnp.where(even_owner, second, first), jnp.where(even_owner, first, second)
            return jnp.where(has_left, left, 0.0), jnp.where(has_right, right, 0.0)

        for k in range(TILES):
            if k % 2 == 0:
                far_left, far_right = beside(TILES + k // 2)
            left, right = beside(k)
            tiles = mix_blocks(
                [
                    far_left if k % 2 else roll(far_left, 8),
                    roll(left, 16),
                    blank,
                    blank,
                    blank,
                    roll(right, 80),
                    roll(far_right, 88 if k % 2 else 96),
                    blank,
                ]
            )
            for a in range(8):
                tile = tiles[-a % 8] + own_ref[which, k * 8 + (-a % 8)]
                target[k * 8 + a] = roll(tile, -16 * a) if a else tile
    rate, diff, decay = param_ref[0], param_ref[1], param_ref[2]
    tables = (block_ref[:, 0:144], stencil_ref, face_ref)
    dots = Dots(packed_ref)
    base_of = row_base(face_ref, rate, diff)

    def emit(row, faces, rest):
        u = state_ref[row]
        base = base_of(row)
        cubic = decay * (u * u)
        new = (base + cubic) * u - rate * old_ref[row] - rest
        diag_ref[row] = (base - THETA / SIGMA) + 3.0 * cubic
        p0_ref[row] = new
        dots.add(0, row, new)

    apply_rows(state_ref, 2, 78, *tables, diff, emit)
    krylov((p0_ref, p1_ref, p2_ref), diag_ref, tables, diff, dots, 6, p3_ref)
    dots.write(gram_ref)


def small_solve(matrix, vector):
    matrix = [list(row) for row in matrix]
    vector = list(vector)
    size = len(vector)
    for col in range(size):
        for target in range(col + 1, size):
            factor = matrix[target][col] / matrix[col][col]
            for at in range(col, size):
                matrix[target][at] = matrix[target][at] - factor * matrix[col][at]
            vector[target] = vector[target] - factor * vector[col]
    answer = [None] * size
    for col in reversed(range(size)):
        running = vector[col]
        for later in range(col + 1, size):
            running = running - matrix[col][later] * answer[later]
        answer[col] = running / matrix[col][col]
    return answer


def combine(parts_ref):
    totals = jnp.sum(parts_ref[...], axis=0, keepdims=True)
    gram = [[None] * 4 for _ in range(4)]
    for at, (i, j) in enumerate(PAIRS):
        gram[i][j] = gram[j][i] = jnp.broadcast_to(totals[:, at : at + 1], (8, LANES))
    zero = jnp.zeros((8, LANES), f32)
    beta = jnp.sqrt(gram[0][0] * (SIGMA * SIGMA) + EPSILON)
    basis = [[-SIGMA / beta]]
    hess = [[zero] * 3 for _ in range(4)]

    def dot(x, y):
        total = x[0] * y[0]
        for at in range(1, len(x)):
            total = total + x[at] * y[at]
        return total

    for j in range(3):
        last = basis[j]
        w = [THETA * last[at] for at in range(j + 1)] + [SIGMA * last[j]]
        for at in range(j):
            w[at + 1] = w[at + 1] + SIGMA * last[at]
        gw = [dot(w, gram[at]) for at in range(j + 2)]
        size = dot(w, gw)
        for i in range(j + 1):
            hess[i][j] = dot(basis[i], gw)
        for i in range(j + 1):
            for at in range(i + 1):
                w[at] = w[at] - hess[i][j] * basis[i][at]
        rest = dot(w, [dot(w, gram[at]) for at in range(j + 2)])
        alive = rest > BREAKDOWN * size
        height = jnp.sqrt(jnp.where(alive, rest, 0.0) + EPSILON)
        hess[j + 1][j] = height
        basis.append([jnp.where(alive, value / height, 0.0) for value in w])
    normal = [[dot([h[i] for h in hess], [h[j] for h in hess]) for j in range(3)] for i in range(3)]
    y = small_solve(normal, [beta * hess[0][i] for i in range(3)])
    out = []
    for at in range(3):
        total = None
        for j in range(at, 3):
            term = y[j] * basis[j][at]
            total = term if total is None else total + term
        out.append(total)
    return out


def second_kernel(
    parts_ref, state_ref, p0_ref, p1_ref, p2_ref, p3_ref, face_ref, stencil_ref, param_ref,
    block_ref, next_ref, q0_ref, q1_ref, q2_ref, gram_ref, diag_ref, packed_ref,
):
    c0, c1, c2 = combine(parts_ref)
    shift = THETA / SIGMA
    rate, diff, decay = param_ref[0], param_ref[1], param_ref[2]
    tables = (block_ref[:, 0:144], stencil_ref, face_ref)
    dots = Dots(packed_ref)
    base_of = row_base(face_ref, rate - shift, diff)
    a0, a1, a2 = 1.0 + shift * c0, c0 + shift * c1, c1 + shift * c2
    triple = 3.0 * decay
    for row in range(5, 75):
        p0, p1, p2, u = p0_ref[row], p1_ref[row], p2_ref[row], state_ref[row]
        d = c0 * p0 + c1 * p1 + c2 * p2
        linear = (a0 * p0 + a1 * p1) + (a2 * p2 + c2 * p3_ref[row])
        new = linear + (decay * (d * d)) * (3.0 * u + d)
        u = u + d
        diag_ref[row] = base_of(row) + triple * (u * u)
        next_ref[row] = u
        q0_ref[row] = new
        dots.add(0, row, new)
    krylov((q0_ref, q1_ref, q2_ref), diag_ref, tables, diff, dots, 3, None)
    dots.write(gram_ref)


SLOTS = PATCH_DEV + 2 * MOVE_CAP


def last_kernel(parts_ref, next_ref, q0_ref, q1_ref, q2_ref, flag_ref, out_ref, low_ref, high_ref):
    c0, c1, c2 = combine(parts_ref)
    slots_ref = (low_ref, high_ref)
    blank = jnp.zeros((3, 8, LANES), f32)

    def put(half, slot, tile):
        slots_ref[half][slot * 24 : slot * 24 + 24, :] = tile.reshape(24, LANES)

    arrived = {}
    for r in range(ROWS_DEV):
        for half in range(2):
            rows = []
            for a in range(8):
                row = OWN_LO + r * 16 + half * 8 + a
                value = next_ref[row] + (c0 * q0_ref[row] + c1 * q1_ref[row] + c2 * q2_ref[row])
                rows.append(roll(value, 16 * a) if a else value)
            tiles = swap_blocks(rows, range(1, 6))
            for c in range(COLS_DEV):
                slot = r * COLS_DEV + c
                put(half, slot, jnp.where(flag_ref[slot] == 1, tiles[2 + c], 0.0))
            for side, g in enumerate((1, 5)):
                for at, (row_of, m) in enumerate(ARRIVALS):
                    if row_of == r:
                        flag = flag_ref[STAYS + side * len(ARRIVALS) + at] == 1
                        key = (half, PATCH_DEV + side * MOVE_CAP + m)
                        arrived[key] = jnp.where(flag, tiles[g], arrived.get(key, blank))
    for (half, slot), tile in arrived.items():
        put(half, slot, tile)

    for s in range(SPECIES):
        for part in range(SLOTS // 8):
            for half in range(2):
                out_ref[s, part * 8 : part * 8 + 8, half * LANES : (half + 1) * LANES] = slots_ref[
                    half
                ][pl.ds(part * 8 * 24 + s, 8, stride=24), :]


def call(kernel, out_shape, in_specs, scratch=(), limit=16):
    return pl.pallas_call(
        kernel,
        out_shape=out_shape,
        in_specs=in_specs,
        out_specs=jax.tree.map(lambda _: pl.BlockSpec(memory_space=pltpu.VMEM), out_shape),
        scratch_shapes=list(scratch),
        compiler_params=pltpu.CompilerParams(vmem_limit_bytes=limit << 20),
    )


def vm():
    return pl.BlockSpec(memory_space=pltpu.VMEM)


def sm():
    return pl.BlockSpec(memory_space=pltpu.SMEM)


def in_hbm(x):
    return pltpu.with_memory_space_constraint(x, pltpu.HBM)


def exchanged(x, along_bands, odd):

    def mate(owner, band):
        at, count = (band, BANDS) if along_bands else (owner, OWNERS)
        near = ((at - odd) ^ 1) + odd
        if not 0 <= near < count:
            return (owner ^ 1, band) if along_bands else (owner, band ^ 1)
        return (owner, near) if along_bands else (near, band)

    pairs = []
    for owner in range(OWNERS):
        for band in range(BANDS):
            to_owner, to_band = mate(owner, band)
            pairs.append((owner * BANDS + band, to_owner * BANDS + to_band))
    return lax.ppermute(x, EVERY, pairs)


def summed(gram):
    spread_out = jnp.broadcast_to(gram[None], (DEVICES, 1, LANES))
    return lax.all_to_all(spread_out, EVERY, 0, 0).reshape(DEVICES, LANES)


def per_device(previous, predicted, new_owner, levels, diffusion, decay, reaction):
    prev, pred = (x.reshape(PATCH_DEV * SPECIES * 2, LANES) for x in (previous, predicted))
    shape = jax.ShapeDtypeStruct
    strip = shape((dense(ROW_TILES), LANES), f32)
    local = shape((INPUT_ROWS + 8, LANES), f32)
    far = pl.BlockSpec(memory_space=pltpu.HBM)
    pred, prev, *strips = call(
        row_strip_kernel,
        (local, local, strip, strip),
        [far, far],
        [pltpu.SemaphoreType.DMA((6,))],
    )(in_hbm(pred), in_hbm(prev))
    row1, row2 = (exchanged(x, True, odd) for odd, x in enumerate(strips))

    message = shape((dense(COL_TILES), LANES), f32)
    messages = call(pack_kernel, (message, message), [vm()] * 4)(pred, prev, row1, row2)
    inputs = (new_owner, levels, diffusion, decay, reaction)
    messages, inputs = lax.optimization_barrier((tuple(messages), inputs))
    new_owner, levels, diffusion, decay, reaction = inputs
    col1, col2 = (exchanged(x, False, odd) for odd, x in enumerate(messages))
    faces, stencil, flags, params, blocks = call(
        table_kernel,
        (
            shape((6, 4, 8, LANES), f32),
            shape((6, 2 * LANES, LANES), bf16),
            shape((FLAGS, 8, LANES), jnp.int32),
            shape((3, 3, 8, LANES), f32),
            shape((48, 2 * LANES), bf16),
        ),
        [sm()] * 4 + [vm()],
        [pltpu.VMEM((24, LANES), f32)],
    )(
        *(
            in_hbm(x)
            for x in (
                levels.transpose(2, 0, 1),
                new_owner.transpose(2, 0, 1),
                diffusion,
                decay,
                reaction,
            )
        )
    )
    state = shape(STATE, f32)
    gram = shape((1, LANES), f32)
    own = call(
        own_kernel,
        shape((2,) + STATE, f32),
        [vm()] * 4,
        [pltpu.VMEM((2 * TILES * COLS_DEV, 24, LANES), f32)],
    )(pred, prev, row1, row2)
    u0, p0, p1, p2, p3, gram1 = call(
        first_kernel,
        (state,) * 5 + (gram,),
        [vm()] * 7,
        [pltpu.VMEM(STATE, f32), pltpu.VMEM(STATE, f32), pltpu.VMEM(PACKED, f32)],
    )(own, col1, col2, faces, stencil, params, blocks)
    u1, q0, q1, q2, gram2 = call(
        second_kernel,
        (state,) * 4 + (gram,),
        [vm()] * 10,
        [pltpu.VMEM(STATE, f32), pltpu.VMEM(PACKED, f32)],
    )(summed(gram1), u0, p0, p1, p2, p3, faces, stencil, params, blocks)
    out = call(
        last_kernel,
        shape((SPECIES, SLOTS, 2 * LANES), f32),
        [vm()] * 6,
        [pltpu.VMEM((SLOTS * 24, LANES), f32)] * 2,
    )(summed(gram2), u1, q0, q1, q2, flags)
    return jnp.transpose(out, (1, 0, 2))[None, None]


def solution(mesh):
    torus = Mesh(
        mesh.devices.reshape(4, 4, 2, mesh.shape["grp"]), ("patch_0", "patch_1", "patch_2", "grp")
    )
    spec = P("grp", PATCH, None, None, None)
    in_specs = (spec, spec, P(), P(), P(), P(), P())
    return jax.shard_map(
        per_device, mesh=torus, in_specs=in_specs, out_specs=spec, check_vma=False
    )
```

```python
import jax
import jax.numpy as jnp
from jax import lax
from jax.experimental import pallas as pl
from jax.experimental.pallas import tpu as pltpu
from jax.sharding import Mesh
from jax.sharding import PartitionSpec as P

SPECIES = 21
COLS_DEV = 3
ROWS_DEV = 4
MOVE_CAP = 2
PATCH_DEV = 12
BANDS = 4
OWNERS = 32
PATCH = ("patch_0", "patch_1", "patch_2")
EVERY = ("patch_0", "patch_1", "patch_2", "grp")
DEVICES = 128

ROWS = 80
OWN_LO, OWN_HI = 8, 72
LANES = 128
TILES = 10
INNER, CORNER = 12, 3

SIGMA = 32.0
THETA = 14.0
EPSILON = 1e-12
BREAKDOWN = 3e-7

f32 = jnp.float32
bf16 = jnp.bfloat16
STATE = (ROWS, 3, 8, LANES)


def position():
    return lax.axis_index("grp"), lax.axis_index(PATCH)


def lanes_of(shape=(8, LANES)):
    return lax.broadcasted_iota(jnp.int32, shape, len(shape) - 1)


def roll(x, amount):
    return pltpu.roll(x, amount % LANES, axis=x.ndim - 1)


def mix_blocks(rolled):
    group = lanes_of() // 16
    tiles = list(rolled)
    for bit in (1, 2, 4):
        high = (group & bit) != 0
        tiles = [jnp.where(high, tiles[(i + bit) % 8], tiles[i]) for i in range(8)]
    return tiles


def swap_blocks(rolled, wanted):
    tiles = mix_blocks(rolled)
    return {a: roll(tiles[-a % 8], -16 * a) if a else tiles[0] for a in wanted}


STAYS = PATCH_DEV
ARRIVALS = [(r, m) for r in range(ROWS_DEV) for m in range(min(r + 1, MOVE_CAP))]
FLAGS = STAYS + 2 * len(ARRIVALS)


def write_flags(owners_ref, flag_ref, band, owner):
    def put(at, condition):
        flag_ref[at] = jnp.full((8, LANES), jnp.where(condition, 1, 0), jnp.int32)

    for slot in range(PATCH_DEV):
        put(slot, owners_ref[slot, band, owner] == owner)
    sides = (
        (owner > 0, jnp.maximum(owner - 1, 0), COLS_DEV - 1),
        (owner < OWNERS - 1, jnp.minimum(owner + 1, OWNERS - 1), 0),
    )
    for side, (exists, beside, column) in enumerate(sides):
        moving = [
            jnp.where(exists & (owners_ref[r * COLS_DEV + column, band, beside] == owner), 1, 0)
            for r in range(ROWS_DEV)
        ]
        for at, (r, m) in enumerate(ARRIVALS):
            rank = jnp.int32(0)
            for before in range(r):
                rank = rank + moving[before]
            put(STAYS + side * len(ARRIVALS) + at, (moving[r] == 1) & (rank == m))


def write_params(diffusion_ref, decay_ref, param_ref):
    row = lax.broadcasted_iota(jnp.int32, (8, LANES), 0)
    for part in range(3):
        rate = jnp.where(row + 8 * part < SPECIES - 1, 4.0, 0.0)
        diff = decay = jnp.zeros((8, LANES), f32)
        for i in range(min(8, SPECIES - 8 * part)):
            diff = jnp.where(row == i, diffusion_ref[8 * part + i], diff)
            decay = jnp.where(row == i, decay_ref[8 * part + i], decay)
        for at, value in enumerate((rate, diff, decay)):
            param_ref[at, part] = value * (1.0 / SIGMA)


def write_blocks(reaction_ref, block_ref, wide_ref):
    wide_ref[...] = jnp.zeros((24, LANES), f32)
    wide_ref[0:SPECIES, 0:SPECIES] = reaction_ref[...] * (1.0 / SIGMA)
    matrix = wide_ref[...]
    high = matrix.astype(bf16).astype(f32)
    low = matrix - high
    tail = lax.broadcasted_iota(jnp.int32, (24, LANES), 1) < 16
    upper = (high + roll(high, 48)) + roll(low, 96)
    lower = roll(high + roll(high, 48), 24)
    turned = roll(low, 120)
    block_ref[:, 0:LANES] = jnp.concatenate(
        [upper, lower + jnp.where(tail, 0.0, turned)], axis=0
    ).astype(bf16)
    block_ref[:, LANES : 2 * LANES] = jnp.concatenate(
        [jnp.zeros((24, LANES), f32), jnp.where(tail, turned, 0.0)], axis=0
    ).astype(bf16)


def table_kernel(
    levels_ref, owners_ref, diffusion_ref, decay_ref, reaction_ref,
    face_ref, stencil_ref, flag_ref, param_ref, block_ref, wide_ref,
):
    band, owner = position()
    write_flags(owners_ref, flag_ref, band, owner)
    write_params(diffusion_ref, decay_ref, param_ref)
    write_blocks(reaction_ref, block_ref, wide_ref)
    lane_group = lanes_of() // 16
    kappas = []
    for idx in range(6):
        patch_row = band * ROWS_DEV + idx - 1
        row_in = (patch_row >= 0) & (patch_row < BANDS * ROWS_DEV)
        row_safe = jnp.clip(patch_row, 0, BANDS * ROWS_DEV - 1)
        near_band, near_row = row_safe // ROWS_DEV, row_safe % ROWS_DEV
        kap = jnp.zeros((8, LANES), f32)
        for g in range(8):
            near_owner = owner + (g - 2 - (g - 2) % COLS_DEV) // COLS_DEV
            inside = row_in & (near_owner >= 0) & (near_owner < OWNERS)
            safe = jnp.clip(near_owner, 0, OWNERS - 1)
            level = levels_ref[near_row * COLS_DEV + (g - 2) % COLS_DEV, near_band, safe]
            value = jnp.where(level == 0, 1.0, jnp.where(level == 1, 4.0, 16.0))
            value = jnp.where(inside, value, 0.0).astype(f32)
            kap = jnp.where(lane_group == g, value, kap)
        kappas.append(kap)

    def face(own, near):
        return jnp.where(own == 0.0, 0.0, jnp.where(near == 0.0, own, 0.5 * (own + near)))

    source = lax.broadcasted_iota(jnp.int32, (LANES, LANES), 0)
    target = lax.broadcasted_iota(jnp.int32, (LANES, LANES), 1)
    for idx in range(6):
        kap = kappas[idx]
        west, east = face(kap, roll(kap, 1)), face(kap, roll(kap, -1))
        face_ref[idx, 0] = west + east
        face_ref[idx, 1] = face(kap, kappas[max(idx - 1, 0)])
        face_ref[idx, 2] = face(kap, kappas[min(idx + 1, 5)])
        face_ref[idx, 3] = kap
        weights = jnp.where(
            source == target - 1,
            jnp.broadcast_to(west[0:1], (LANES, LANES)),
            jnp.where(source == target + 1, jnp.broadcast_to(east[0:1], (LANES, LANES)), 0.0),
        ).astype(bf16)
        stencil_ref[idx, 0:LANES, :] = weights
        stencil_ref[idx, LANES : 2 * LANES, :] = weights


def half_tile(patch_ref, slot, half):
    return patch_ref[pl.ds(slot * 2 * SPECIES + half, SPECIES, stride=2), :]


ROW_TILES = 2 * COLS_DEV


def dense(tiles):
    return -(-(tiles * SPECIES + 24 - SPECIES) // 8) * 8


def put_tile(ref, at, tile):
    ref[at * SPECIES : (at + 1) * SPECIES, :] = tile


def finish(ref, tiles):
    ref[tiles * SPECIES :, :] = jnp.zeros((dense(tiles) - tiles * SPECIES, LANES), f32)


def get_tile(ref, at):
    tile = ref[at * SPECIES : at * SPECIES + 24, :]
    species = lax.broadcasted_iota(jnp.int32, (24, LANES), 0)
    return jnp.where(species < SPECIES, tile, 0.0)


INPUT_ROWS = PATCH_DEV * 2 * SPECIES
EDGE = 128


def packed_pair(low, high):
    odd = (lax.broadcasted_iota(jnp.int32, (SPECIES, LANES), 1) // 8) % 2 == 1
    return lambda: jnp.where(odd, high, roll(low, -8)), lambda: jnp.where(odd, roll(high, 8), low)


def put_columns(first_ref, second_ref, at, right, left):
    _, owner = position()
    put_tile(first_ref, at, jnp.where(owner % 2 == 0, right, left))
    put_tile(second_ref, at, jnp.where(owner % 2 == 0, left, right))


def strip_kernel(
    pred_hbm, prev_hbm, pred_ref, prev_ref, first_ref, second_ref, inner1_ref, inner2_ref, sems
):
    band, _ = position()
    even = band % 2 == 0
    top = INPUT_ROWS - EDGE
    spans = ((0, EDGE), (top, EDGE), (EDGE, top - EDGE))
    pairs = ((pred_hbm, pred_ref), (prev_hbm, prev_ref))
    copies = [
        [
            pltpu.make_async_copy(
                source.at[pl.ds(start, size), :],
                target.at[pl.ds(start, size), :],
                sems.at[3 * which + at],
            )
            for at, (start, size) in enumerate(spans)
        ]
        for which, (source, target) in enumerate(pairs)
    ]
    for at in range(3):
        for which in range(2):
            copies[which][at].start()
    for which, (_, patch_ref) in enumerate(pairs):
        copies[which][0].wait()
        copies[which][1].wait()
        for c in range(COLS_DEV):
            up = half_tile(patch_ref, PATCH_DEV - COLS_DEV + c, 1)
            down = half_tile(patch_ref, c, 0)
            put_tile(first_ref, which * COLS_DEV + c, jnp.where(even, up, down))
            put_tile(second_ref, which * COLS_DEV + c, jnp.where(even, down, up))
    finish(first_ref, ROW_TILES)
    finish(second_ref, ROW_TILES)
    for which, (_, patch_ref) in enumerate(pairs):
        copies[which][2].wait()
        for half in range(2 * ROWS_DEV):
            slot = half // 2 * COLS_DEV
            put_columns(
                inner1_ref,
                inner2_ref,
                which * INNER + half,
                half_tile(patch_ref, slot + 2, half % 2),
                half_tile(patch_ref, slot, half % 2),
            )
        for r in range(ROWS_DEV):
            slot = r * COLS_DEV + 1
            east, west = packed_pair(half_tile(patch_ref, slot, 0), half_tile(patch_ref, slot, 1))
            at = which * INNER + 2 * ROWS_DEV + r
            put_columns(inner1_ref, inner2_ref, at, east(), west())
    finish(inner1_ref, 2 * INNER)
    finish(inner2_ref, 2 * INNER)


def tile_of(patch_ref, rows_ref, which, k, c):
    if k in (0, TILES - 1):
        band, _ = position()
        even = band % 2 == 0
        at = (which * COLS_DEV + c) * SPECIES
        first, second = (ref[at : at + SPECIES, :] for ref in rows_ref)
        south, inside = k == 0, (band > 0) if k == 0 else (band < BANDS - 1)
        tile = jnp.where(even, second, first) if south else jnp.where(even, first, second)
        return jnp.where(inside, tile, 0.0)
    return half_tile(patch_ref, ((k - 1) // 2) * COLS_DEV + c, (k - 1) % 2)


def corner_kernel(row1_ref, row2_ref, first_ref, second_ref):
    for which in range(2):

        def tile(k, c, which=which):
            return tile_of(None, (row1_ref, row2_ref), which, k, c)

        for at, k in enumerate((0, TILES - 1)):
            put_columns(first_ref, second_ref, which * CORNER + at, tile(k, 2), tile(k, 0))
        east, west = packed_pair(tile(0, 1), tile(TILES - 1, 1))
        put_columns(first_ref, second_ref, which * CORNER + 2, east(), west())
    finish(first_ref, 2 * CORNER)
    finish(second_ref, 2 * CORNER)


def own_kernel(pred_ref, prev_ref, row1_ref, row2_ref, own_ref, tile_ref):
    tile_ref[:, SPECIES:24, :] = jnp.zeros((2 * TILES * COLS_DEV, 24 - SPECIES, LANES), f32)
    for which, patch_ref in enumerate((pred_ref, prev_ref)):
        for k in range(TILES):
            for c in range(COLS_DEV):
                tile_ref[(which * TILES + k) * COLS_DEV + c, 0:SPECIES, :] = tile_of(
                    patch_ref, (row1_ref, row2_ref), which, k, c
                )
    blank = jnp.zeros((3, 8, LANES), f32)
    for which in range(2):
        for k in range(TILES):
            tiles = [blank] * 8
            for c in range(COLS_DEV):
                tile = tile_ref[(which * TILES + k) * COLS_DEV + c].reshape(3, 8, LANES)
                tiles[2 + c] = roll(tile, 16 * (2 + c))
            for a, tile in enumerate(mix_blocks(tiles)):
                own_ref[which, k * 8 + a] = tile


def row_faces(face_ref, row):
    idx = (row + 8) // 16
    kap = face_ref[idx, 3]
    south = face_ref[idx, 1] if row % 16 == 8 else kap
    north = face_ref[idx, 2] if row % 16 == 7 else kap
    return face_ref[idx, 0], south, north


def vertical(source, row, faces):
    _, south, north = faces
    if row % 16 in (7, 8):
        return south * source[row - 1] + north * source[row + 1]
    return south * (source[row - 1] + source[row + 1])


def apply_rows(source, lo, hi, blocks, stencil_ref, face_ref, diff, emit):
    for idx in range(6):
        first, last = max(lo, idx * 16 - 8), min(hi, idx * 16 + 8)
        if first >= last:
            continue
        start, stop = first - first % 2, last + last % 2
        parts = []
        for row in range(start, stop, 2):
            x = source[row : row + 2].reshape(48, LANES)
            high = x.astype(bf16)
            parts.append((high, (x - high.astype(f32)).astype(bf16)))
        beside = jnp.dot(
            jnp.concatenate([jnp.concatenate(part, axis=1) for part in parts], axis=0),
            stencil_ref[idx],
            preferred_element_type=f32,
        ).reshape(stop - start, 3, 8, LANES)
        mixed = []
        for at in range(0, len(parts), 2):
            group = parts[at : at + 2]
            high = jnp.concatenate([part[0] for part in group], axis=1)
            low = jnp.concatenate([part[1] for part in group], axis=1)
            m = jnp.dot(
                blocks, jnp.concatenate([high, low, high], axis=0), preferred_element_type=f32
            ).reshape(2, 3, 8, len(group) * LANES)
            for pair in range(len(group)):
                for off in range(2):
                    mixed.append(m[off, :, :, pair * LANES : (pair + 1) * LANES])
        for row in range(first, last):
            faces = row_faces(face_ref, row)
            near = beside[row - start] + vertical(source, row, faces)
            emit(row, faces, diff * near + mixed[row - start])


PAIRS = [(i, j) for j in range(4) for i in range(j + 1)]


class Dots:
    def __init__(self, packed_ref):
        self.sums = {}
        self.packed_ref = packed_ref
        self.half = None
        lane = lanes_of()
        self.own = (lane >= 32) & (lane < 80)
        self.both = self.own | (lane >= 96) | (lane < 16)

    def add(self, basis, row, value):
        if not OWN_LO <= row < OWN_HI:
            return
        if row % 2 == 0:
            self.half = value
            return
        at = (row - OWN_LO) // 2
        value = jnp.where(self.own, self.half, roll(value, 64))
        if basis < 3:
            self.packed_ref[basis, at] = value
        for before in range(basis + 1):
            other = value if before == basis else self.packed_ref[before, at]
            key, term = (before, basis), other * value
            self.sums[key] = self.sums[key] + term if key in self.sums else term

    def write(self, out_ref):
        lane = lanes_of((1, LANES))
        total = jnp.zeros((1, LANES), f32)
        for at, key in enumerate(PAIRS):
            value = jnp.where(self.both, jnp.sum(self.sums[key], axis=0), 0.0)
            value = jnp.sum(jnp.sum(value, axis=0, keepdims=True), axis=1, keepdims=True)
            total = jnp.where(lane == at, value, total)
        out_ref[...] = total


PACKED = (3, (OWN_HI - OWN_LO) // 2, 3, 8, LANES)


def krylov(refs, diag_ref, tables, diff, dots, reach, last_ref):
    for k in range(3):
        source, target = refs[k], last_ref if k == 2 else refs[k + 1]
        width = reach - k - 1
        lo, hi = OWN_LO - width, OWN_HI + width

        def emit(row, faces, rest, source=source, target=target, k=k):
            new = diag_ref[row] * source[row] - rest
            if target is not None:
                target[row] = new
            dots.add(k + 1, row, new)

        apply_rows(source, lo, hi, *tables, diff, emit)


def row_base(face_ref, rate, diff):
    cache = {}

    def base(row):
        kind = ((row + 8) // 16, {7: 1, 8: 2}.get(row % 16, 0))
        if kind not in cache:
            beside, south, north = row_faces(face_ref, row)
            cache[kind] = rate + diff * (beside + (south + north))
        return cache[kind]

    return base


def first_kernel(
    own_ref, inner1_ref, inner2_ref, corner1_ref, corner2_ref, face_ref, stencil_ref, param_ref, block_ref,
    state_ref, p0_ref, p1_ref, p2_ref, p3_ref, gram_ref, old_ref, diag_ref, packed_ref,
):
    _, owner = position()
    even_owner, has_left, has_right = owner % 2 == 0, owner > 0, owner < OWNERS - 1
    blank = jnp.zeros((3, 8, LANES), f32)
    for which, target in enumerate((state_ref, old_ref)):

        def beside(refs, at):
            first, second = (get_tile(ref, at).reshape(3, 8, LANES) for ref in refs)
            left, right = jnp.where(even_owner, second, first), jnp.where(even_owner, first, second)
            return jnp.where(has_left, left, 0.0), jnp.where(has_right, right, 0.0)

        for k in range(TILES):
            if k in (0, TILES - 1):
                refs, at = (corner1_ref, corner2_ref), which * CORNER + (k > 0)
                pair, high = which * CORNER + 2, k > 0
            else:
                refs, at = (inner1_ref, inner2_ref), which * INNER + k - 1
                pair, high = which * INNER + 2 * ROWS_DEV + (k - 1) // 2, k % 2 == 0
            left, right = beside(refs, at)
            far_left, far_right = beside(refs, pair)
            tiles = mix_blocks(
                [
                    far_left if high else roll(far_left, 8),
                    roll(left, 16),
                    blank,
                    blank,
                    blank,
                    roll(right, 80),
                    roll(far_right, 88 if high else 96),
                    blank,
                ]
            )
            for a in range(8):
                tile = tiles[-a % 8] + own_ref[which, k * 8 + (-a % 8)]
                target[k * 8 + a] = roll(tile, -16 * a) if a else tile
    rate, diff, decay = param_ref[0], param_ref[1], param_ref[2]
    tables = (block_ref[:, 0:144], stencil_ref, face_ref)
    dots = Dots(packed_ref)
    base_of = row_base(face_ref, rate, diff)

    def emit(row, faces, rest):
        u = state_ref[row]
        base = base_of(row)
        cubic = decay * (u * u)
        new = (base + cubic) * u - rate * old_ref[row] - rest
        diag_ref[row] = (base - THETA / SIGMA) + 3.0 * cubic
        p0_ref[row] = new
        dots.add(0, row, new)

    apply_rows(state_ref, 2, 78, *tables, diff, emit)
    krylov((p0_ref, p1_ref, p2_ref), diag_ref, tables, diff, dots, 6, p3_ref)
    dots.write(gram_ref)


def small_solve(matrix, vector):
    matrix = [list(row) for row in matrix]
    vector = list(vector)
    size = len(vector)
    for col in range(size):
        for target in range(col + 1, size):
            factor = matrix[target][col] / matrix[col][col]
            for at in range(col, size):
                matrix[target][at] = matrix[target][at] - factor * matrix[col][at]
            vector[target] = vector[target] - factor * vector[col]
    answer = [None] * size
    for col in reversed(range(size)):
        running = vector[col]
        for later in range(col + 1, size):
            running = running - matrix[col][later] * answer[later]
        answer[col] = running / matrix[col][col]
    return answer


def combine(parts_ref):
    totals = jnp.sum(parts_ref[...], axis=0, keepdims=True)
    gram = [[None] * 4 for _ in range(4)]
    for at, (i, j) in enumerate(PAIRS):
        gram[i][j] = gram[j][i] = jnp.broadcast_to(totals[:, at : at + 1], (8, LANES))
    zero = jnp.zeros((8, LANES), f32)
    beta = jnp.sqrt(gram[0][0] * (SIGMA * SIGMA) + EPSILON)
    basis = [[-SIGMA / beta]]
    hess = [[zero] * 3 for _ in range(4)]

    def dot(x, y):
        total = x[0] * y[0]
        for at in range(1, len(x)):
            total = total + x[at] * y[at]
        return total

    for j in range(3):
        last = basis[j]
        w = [THETA * last[at] for at in range(j + 1)] + [SIGMA * last[j]]
        for at in range(j):
            w[at + 1] = w[at + 1] + SIGMA * last[at]
        gw = [dot(w, gram[at]) for at in range(j + 2)]
        size = dot(w, gw)
        for i in range(j + 1):
            hess[i][j] = dot(basis[i], gw)
        for i in range(j + 1):
            for at in range(i + 1):
                w[at] = w[at] - hess[i][j] * basis[i][at]
        rest = dot(w, [dot(w, gram[at]) for at in range(j + 2)])
        alive = rest > BREAKDOWN * size
        height = jnp.sqrt(jnp.where(alive, rest, 0.0) + EPSILON)
        hess[j + 1][j] = height
        basis.append([jnp.where(alive, value / height, 0.0) for value in w])
    normal = [[dot([h[i] for h in hess], [h[j] for h in hess]) for j in range(3)] for i in range(3)]
    y = small_solve(normal, [beta * hess[0][i] for i in range(3)])
    out = []
    for at in range(3):
        total = None
        for j in range(at, 3):
            term = y[j] * basis[j][at]
            total = term if total is None else total + term
        out.append(total)
    return out


def second_kernel(
    parts_ref, state_ref, p0_ref, p1_ref, p2_ref, p3_ref, face_ref, stencil_ref, param_ref,
    block_ref, next_ref, q0_ref, q1_ref, q2_ref, gram_ref, diag_ref, packed_ref,
):
    c0, c1, c2 = combine(parts_ref)
    shift = THETA / SIGMA
    rate, diff, decay = param_ref[0], param_ref[1], param_ref[2]
    tables = (block_ref[:, 0:144], stencil_ref, face_ref)
    dots = Dots(packed_ref)
    base_of = row_base(face_ref, rate - shift, diff)
    a0, a1, a2 = 1.0 + shift * c0, c0 + shift * c1, c1 + shift * c2
    triple = 3.0 * decay
    for row in range(5, 75):
        p0, p1, p2, u = p0_ref[row], p1_ref[row], p2_ref[row], state_ref[row]
        d = c0 * p0 + c1 * p1 + c2 * p2
        linear = (a0 * p0 + a1 * p1) + (a2 * p2 + c2 * p3_ref[row])
        new = linear + (decay * (d * d)) * (3.0 * u + d)
        u = u + d
        diag_ref[row] = base_of(row) + triple * (u * u)
        next_ref[row] = u
        q0_ref[row] = new
        dots.add(0, row, new)
    krylov((q0_ref, q1_ref, q2_ref), diag_ref, tables, diff, dots, 3, None)
    dots.write(gram_ref)


SLOTS = PATCH_DEV + 2 * MOVE_CAP


def last_kernel(parts_ref, next_ref, q0_ref, q1_ref, q2_ref, flag_ref, out_ref, low_ref, high_ref):
    c0, c1, c2 = combine(parts_ref)
    slots_ref = (low_ref, high_ref)
    blank = jnp.zeros((3, 8, LANES), f32)

    def put(half, slot, tile):
        slots_ref[half][slot * 24 : slot * 24 + 24, :] = tile.reshape(24, LANES)

    arrived = {}
    for r in range(ROWS_DEV):
        for half in range(2):
            rows = []
            for a in range(8):
                row = OWN_LO + r * 16 + half * 8 + a
                value = next_ref[row] + (c0 * q0_ref[row] + c1 * q1_ref[row] + c2 * q2_ref[row])
                rows.append(roll(value, 16 * a) if a else value)
            tiles = swap_blocks(rows, range(1, 6))
            for c in range(COLS_DEV):
                slot = r * COLS_DEV + c
                put(half, slot, jnp.where(flag_ref[slot] == 1, tiles[2 + c], 0.0))
            for side, g in enumerate((1, 5)):
                for at, (row_of, m) in enumerate(ARRIVALS):
                    if row_of == r:
                        flag = flag_ref[STAYS + side * len(ARRIVALS) + at] == 1
                        key = (half, PATCH_DEV + side * MOVE_CAP + m)
                        arrived[key] = jnp.where(flag, tiles[g], arrived.get(key, blank))
    for (half, slot), tile in arrived.items():
        put(half, slot, tile)

    for s in range(SPECIES):
        for part in range(SLOTS // 8):
            for half in range(2):
                out_ref[s, part * 8 : part * 8 + 8, half * LANES : (half + 1) * LANES] = slots_ref[
                    half
                ][pl.ds(part * 8 * 24 + s, 8, stride=24), :]


def call(kernel, out_shape, in_specs, scratch=(), limit=16):
    return pl.pallas_call(
        kernel,
        out_shape=out_shape,
        in_specs=in_specs,
        out_specs=jax.tree.map(lambda _: pl.BlockSpec(memory_space=pltpu.VMEM), out_shape),
        scratch_shapes=list(scratch),
        compiler_params=pltpu.CompilerParams(vmem_limit_bytes=limit << 20),
    )


def vm():
    return pl.BlockSpec(memory_space=pltpu.VMEM)


def sm():
    return pl.BlockSpec(memory_space=pltpu.SMEM)


def in_hbm(x):
    return pltpu.with_memory_space_constraint(x, pltpu.HBM)


def exchanged(x, along_bands, odd):

    def mate(owner, band):
        at, count = (band, BANDS) if along_bands else (owner, OWNERS)
        near = ((at - odd) ^ 1) + odd
        if not 0 <= near < count:
            return (owner ^ 1, band) if along_bands else (owner, band ^ 1)
        return (owner, near) if along_bands else (near, band)

    pairs = []
    for owner in range(OWNERS):
        for band in range(BANDS):
            to_owner, to_band = mate(owner, band)
            pairs.append((owner * BANDS + band, to_owner * BANDS + to_band))
    return lax.ppermute(x, EVERY, pairs)


def swapped(pair, along_bands):
    out = []
    for odd, x in enumerate(pair):
        out.append(exchanged(x, along_bands, odd))
    return out


def summed(gram):
    spread_out = jnp.broadcast_to(gram[None], (DEVICES, 1, LANES))
    return lax.all_to_all(spread_out, EVERY, 0, 0).reshape(DEVICES, LANES)


def per_device(previous, predicted, new_owner, levels, diffusion, decay, reaction):
    prev, pred = (x.reshape(PATCH_DEV * SPECIES * 2, LANES) for x in (previous, predicted))
    shape = jax.ShapeDtypeStruct
    strip = shape((dense(ROW_TILES), LANES), f32)
    local = shape((INPUT_ROWS + 8, LANES), f32)
    far = pl.BlockSpec(memory_space=pltpu.HBM)
    inner, corner = (shape((dense(2 * count), LANES), f32) for count in (INNER, CORNER))
    pred, prev, *strips = call(
        strip_kernel,
        (local, local, strip, strip, inner, inner),
        [far, far],
        [pltpu.SemaphoreType.DMA((6,))],
    )(in_hbm(pred), in_hbm(prev))
    row1, row2 = swapped(strips[:2], True)
    inner_cols = swapped(strips[2:], False)
    corners = call(corner_kernel, (corner, corner), [vm()] * 2)(row1, row2)

    inputs = (new_owner, levels, diffusion, decay, reaction)
    corners, inputs = lax.optimization_barrier((tuple(corners), inputs))
    new_owner, levels, diffusion, decay, reaction = inputs
    corner_cols = swapped(corners, False)
    faces, stencil, flags, params, blocks = call(
        table_kernel,
        (
            shape((6, 4, 8, LANES), f32),
            shape((6, 2 * LANES, LANES), bf16),
            shape((FLAGS, 8, LANES), jnp.int32),
            shape((3, 3, 8, LANES), f32),
            shape((48, 2 * LANES), bf16),
        ),
        [sm()] * 4 + [vm()],
        [pltpu.VMEM((24, LANES), f32)],
    )(
        *(
            in_hbm(x)
            for x in (
                levels.transpose(2, 0, 1),
                new_owner.transpose(2, 0, 1),
                diffusion,
                decay,
                reaction,
            )
        )
    )
    state = shape(STATE, f32)
    gram = shape((1, LANES), f32)
    own = call(
        own_kernel,
        shape((2,) + STATE, f32),
        [vm()] * 4,
        [pltpu.VMEM((2 * TILES * COLS_DEV, 24, LANES), f32)],
    )(pred, prev, row1, row2)
    u0, p0, p1, p2, p3, gram1 = call(
        first_kernel,
        (state,) * 5 + (gram,),
        [vm()] * 9,
        [pltpu.VMEM(STATE, f32), pltpu.VMEM(STATE, f32), pltpu.VMEM(PACKED, f32)],
    )(own, *inner_cols, *corner_cols, faces, stencil, params, blocks)
    u1, q0, q1, q2, gram2 = call(
        second_kernel,
        (state,) * 4 + (gram,),
        [vm()] * 10,
        [pltpu.VMEM(STATE, f32), pltpu.VMEM(PACKED, f32)],
    )(summed(gram1), u0, p0, p1, p2, p3, faces, stencil, params, blocks)
    out = call(
        last_kernel,
        shape((SPECIES, SLOTS, 2 * LANES), f32),
        [vm()] * 6,
        [pltpu.VMEM((SLOTS * 24, LANES), f32)] * 2,
    )(summed(gram2), u1, q0, q1, q2, flags)
    return jnp.transpose(out, (1, 0, 2))[None, None]


def solution(mesh):
    torus = Mesh(
        mesh.devices.reshape(4, 4, 2, mesh.shape["grp"]), ("patch_0", "patch_1", "patch_2", "grp")
    )
    spec = P("grp", PATCH, None, None, None)
    in_specs = (spec, spec, P(), P(), P(), P(), P())
    return jax.shard_map(
        per_device, mesh=torus, in_specs=in_specs, out_specs=spec, check_vma=False
    )
```

```python
import jax
import jax.numpy as jnp
from jax import lax
from jax.experimental import pallas as pl
from jax.experimental.pallas import tpu as pltpu
from jax.sharding import Mesh
from jax.sharding import PartitionSpec as P

SPECIES = 21
COLS_DEV = 3
ROWS_DEV = 4
MOVE_CAP = 2
PATCH_DEV = 12
BANDS = 4
OWNERS = 32
PATCH = ("patch_0", "patch_1", "patch_2")
EVERY = ("patch_0", "patch_1", "patch_2", "grp")
DEVICES = 128

ROWS = 80
OWN_LO, OWN_HI = 8, 72
LANES = 128
TILES = 10
INNER, CORNER = 12, 3

SIGMA = 32.0
THETA = 14.0
EPSILON = 1e-12
BREAKDOWN = 3e-7

f32 = jnp.float32
bf16 = jnp.bfloat16
STATE = (ROWS, 3, 8, LANES)


def position():
    return lax.axis_index("grp"), lax.axis_index(PATCH)


def lanes_of(shape=(8, LANES)):
    return lax.broadcasted_iota(jnp.int32, shape, len(shape) - 1)


def roll(x, amount):
    return pltpu.roll(x, amount % LANES, axis=x.ndim - 1)


def mix_blocks(rolled):
    group = lanes_of() // 16
    tiles = list(rolled)
    for bit in (1, 2, 4):
        high = (group & bit) != 0
        tiles = [jnp.where(high, tiles[(i + bit) % 8], tiles[i]) for i in range(8)]
    return tiles


def swap_blocks(rolled, wanted):
    tiles = mix_blocks(rolled)
    return {a: roll(tiles[-a % 8], -16 * a) if a else tiles[0] for a in wanted}


STAYS = PATCH_DEV
ARRIVALS = [(r, m) for r in range(ROWS_DEV) for m in range(min(r + 1, MOVE_CAP))]
FLAGS = STAYS + 2 * len(ARRIVALS)


def write_flags(owners_ref, flag_ref, band, owner):
    def put(at, condition):
        flag_ref[at] = jnp.full((8, LANES), jnp.where(condition, 1, 0), jnp.int32)

    for slot in range(PATCH_DEV):
        put(slot, owners_ref[slot, band, owner] == owner)
    sides = (
        (owner > 0, jnp.maximum(owner - 1, 0), COLS_DEV - 1),
        (owner < OWNERS - 1, jnp.minimum(owner + 1, OWNERS - 1), 0),
    )
    for side, (exists, beside, column) in enumerate(sides):
        moving = [
            jnp.where(exists & (owners_ref[r * COLS_DEV + column, band, beside] == owner), 1, 0)
            for r in range(ROWS_DEV)
        ]
        for at, (r, m) in enumerate(ARRIVALS):
            rank = jnp.int32(0)
            for before in range(r):
                rank = rank + moving[before]
            put(STAYS + side * len(ARRIVALS) + at, (moving[r] == 1) & (rank == m))


def write_params(diffusion_ref, decay_ref, param_ref):
    row = lax.broadcasted_iota(jnp.int32, (8, LANES), 0)
    for part in range(3):
        rate = jnp.where(row + 8 * part < SPECIES - 1, 4.0, 0.0)
        diff = decay = jnp.zeros((8, LANES), f32)
        for i in range(min(8, SPECIES - 8 * part)):
            diff = jnp.where(row == i, diffusion_ref[8 * part + i], diff)
            decay = jnp.where(row == i, decay_ref[8 * part + i], decay)
        for at, value in enumerate((rate, diff, decay)):
            param_ref[at, part] = value * (1.0 / SIGMA)


def write_blocks(reaction_ref, block_ref, wide_ref):
    wide_ref[...] = jnp.zeros((24, LANES), f32)
    wide_ref[0:SPECIES, 0:SPECIES] = reaction_ref[...] * (1.0 / SIGMA)
    matrix = wide_ref[...]
    high = matrix.astype(bf16).astype(f32)
    low = matrix - high
    tail = lax.broadcasted_iota(jnp.int32, (24, LANES), 1) < 16
    upper = (high + roll(high, 48)) + roll(low, 96)
    lower = roll(high + roll(high, 48), 24)
    turned = roll(low, 120)
    block_ref[:, 0:LANES] = jnp.concatenate(
        [upper, lower + jnp.where(tail, 0.0, turned)], axis=0
    ).astype(bf16)
    block_ref[:, LANES : 2 * LANES] = jnp.concatenate(
        [jnp.zeros((24, LANES), f32), jnp.where(tail, turned, 0.0)], axis=0
    ).astype(bf16)


def table_kernel(
    levels_ref, owners_ref, diffusion_ref, decay_ref, reaction_ref,
    face_ref, stencil_ref, flag_ref, param_ref, block_ref, wide_ref,
):
    band, owner = position()
    write_flags(owners_ref, flag_ref, band, owner)
    write_params(diffusion_ref, decay_ref, param_ref)
    write_blocks(reaction_ref, block_ref, wide_ref)
    lane_group = lanes_of() // 16
    kappas = []
    for idx in range(6):
        patch_row = band * ROWS_DEV + idx - 1
        row_in = (patch_row >= 0) & (patch_row < BANDS * ROWS_DEV)
        row_safe = jnp.clip(patch_row, 0, BANDS * ROWS_DEV - 1)
        near_band, near_row = row_safe // ROWS_DEV, row_safe % ROWS_DEV
        kap = jnp.zeros((8, LANES), f32)
        for g in range(8):
            near_owner = owner + (g - 2 - (g - 2) % COLS_DEV) // COLS_DEV
            inside = row_in & (near_owner >= 0) & (near_owner < OWNERS)
            safe = jnp.clip(near_owner, 0, OWNERS - 1)
            level = levels_ref[near_row * COLS_DEV + (g - 2) % COLS_DEV, near_band, safe]
            value = jnp.where(level == 0, 1.0, jnp.where(level == 1, 4.0, 16.0))
            value = jnp.where(inside, value, 0.0).astype(f32)
            kap = jnp.where(lane_group == g, value, kap)
        kappas.append(kap)

    def face(own, near):
        return jnp.where(own == 0.0, 0.0, jnp.where(near == 0.0, own, 0.5 * (own + near)))

    source = lax.broadcasted_iota(jnp.int32, (LANES, LANES), 0)
    target = lax.broadcasted_iota(jnp.int32, (LANES, LANES), 1)
    for idx in range(6):
        kap = kappas[idx]
        west, east = face(kap, roll(kap, 1)), face(kap, roll(kap, -1))
        face_ref[idx, 0] = west + east
        face_ref[idx, 1] = face(kap, kappas[max(idx - 1, 0)])
        face_ref[idx, 2] = face(kap, kappas[min(idx + 1, 5)])
        face_ref[idx, 3] = kap
        weights = jnp.where(
            source == target - 1,
            jnp.broadcast_to(west[0:1], (LANES, LANES)),
            jnp.where(source == target + 1, jnp.broadcast_to(east[0:1], (LANES, LANES)), 0.0),
        ).astype(bf16)
        stencil_ref[idx, 0:LANES, :] = weights
        stencil_ref[idx, LANES : 2 * LANES, :] = weights


def half_tile(patch_ref, slot, half):
    return patch_ref[pl.ds(slot * 2 * SPECIES + half, SPECIES, stride=2), :]


ROW_TILES = 2 * COLS_DEV


def dense(tiles):
    return -(-(tiles * SPECIES + 24 - SPECIES) // 8) * 8


def put_tile(ref, at, tile):
    ref[at * SPECIES : (at + 1) * SPECIES, :] = tile


def finish(ref, tiles):
    ref[tiles * SPECIES :, :] = jnp.zeros((dense(tiles) - tiles * SPECIES, LANES), f32)


def get_tile(ref, at):
    tile = ref[at * SPECIES : at * SPECIES + 24, :]
    species = lax.broadcasted_iota(jnp.int32, (24, LANES), 0)
    return jnp.where(species < SPECIES, tile, 0.0)


INPUT_ROWS = PATCH_DEV * 2 * SPECIES
EDGE = 128


def packed_pair(low, high):
    odd = (lax.broadcasted_iota(jnp.int32, (SPECIES, LANES), 1) // 8) % 2 == 1
    return lambda: jnp.where(odd, high, roll(low, -8)), lambda: jnp.where(odd, roll(high, 8), low)


def put_columns(first_ref, second_ref, at, right, left):
    _, owner = position()
    put_tile(first_ref, at, jnp.where(owner % 2 == 0, right, left))
    put_tile(second_ref, at, jnp.where(owner % 2 == 0, left, right))


def strip_kernel(
    pred_hbm, prev_hbm, pred_ref, prev_ref, first_ref, second_ref, inner1_ref, inner2_ref, sems
):
    band, _ = position()
    even = band % 2 == 0
    top = INPUT_ROWS - EDGE
    spans = ((0, EDGE), (top, EDGE), (EDGE, top - EDGE))
    pairs = ((pred_hbm, pred_ref), (prev_hbm, prev_ref))
    copies = [
        [
            pltpu.make_async_copy(
                source.at[pl.ds(start, size), :],
                target.at[pl.ds(start, size), :],
                sems.at[3 * which + at],
            )
            for at, (start, size) in enumerate(spans)
        ]
        for which, (source, target) in enumerate(pairs)
    ]
    for at in range(3):
        for which in range(2):
            copies[which][at].start()
    for which, (_, patch_ref) in enumerate(pairs):
        copies[which][0].wait()
        copies[which][1].wait()
        for c in range(COLS_DEV):
            up = half_tile(patch_ref, PATCH_DEV - COLS_DEV + c, 1)
            down = half_tile(patch_ref, c, 0)
            put_tile(first_ref, which * COLS_DEV + c, jnp.where(even, up, down))
            put_tile(second_ref, which * COLS_DEV + c, jnp.where(even, down, up))
    finish(first_ref, ROW_TILES)
    finish(second_ref, ROW_TILES)
    for which, (_, patch_ref) in enumerate(pairs):
        copies[which][2].wait()
        for half in range(2 * ROWS_DEV):
            slot = half // 2 * COLS_DEV
            put_columns(
                inner1_ref,
                inner2_ref,
                which * INNER + half,
                half_tile(patch_ref, slot + 2, half % 2),
                half_tile(patch_ref, slot, half % 2),
            )
        for r in range(ROWS_DEV):
            slot = r * COLS_DEV + 1
            east, west = packed_pair(half_tile(patch_ref, slot, 0), half_tile(patch_ref, slot, 1))
            at = which * INNER + 2 * ROWS_DEV + r
            put_columns(inner1_ref, inner2_ref, at, east(), west())
    finish(inner1_ref, 2 * INNER)
    finish(inner2_ref, 2 * INNER)


def tile_of(patch_ref, rows_ref, which, k, c):
    if k in (0, TILES - 1):
        band, _ = position()
        even = band % 2 == 0
        at = (which * COLS_DEV + c) * SPECIES
        first, second = (ref[at : at + SPECIES, :] for ref in rows_ref)
        south, inside = k == 0, (band > 0) if k == 0 else (band < BANDS - 1)
        tile = jnp.where(even, second, first) if south else jnp.where(even, first, second)
        return jnp.where(inside, tile, 0.0)
    return half_tile(patch_ref, ((k - 1) // 2) * COLS_DEV + c, (k - 1) % 2)


def corner_kernel(row1_ref, row2_ref, first_ref, second_ref):
    for which in range(2):

        def tile(k, c, which=which):
            return tile_of(None, (row1_ref, row2_ref), which, k, c)

        for at, k in enumerate((0, TILES - 1)):
            put_columns(first_ref, second_ref, which * CORNER + at, tile(k, 2), tile(k, 0))
        east, west = packed_pair(tile(0, 1), tile(TILES - 1, 1))
        put_columns(first_ref, second_ref, which * CORNER + 2, east(), west())
    finish(first_ref, 2 * CORNER)
    finish(second_ref, 2 * CORNER)


def own_kernel(pred_ref, prev_ref, row1_ref, row2_ref, own_ref, tile_ref):
    tile_ref[:, SPECIES:24, :] = jnp.zeros((2 * TILES * COLS_DEV, 24 - SPECIES, LANES), f32)
    for which, patch_ref in enumerate((pred_ref, prev_ref)):
        for k in range(TILES):
            for c in range(COLS_DEV):
                tile_ref[(which * TILES + k) * COLS_DEV + c, 0:SPECIES, :] = tile_of(
                    patch_ref, (row1_ref, row2_ref), which, k, c
                )
    blank = jnp.zeros((3, 8, LANES), f32)
    for which in range(2):
        for k in range(TILES):
            tiles = [blank] * 8
            for c in range(COLS_DEV):
                tile = tile_ref[(which * TILES + k) * COLS_DEV + c].reshape(3, 8, LANES)
                tiles[2 + c] = roll(tile, 16 * (2 + c))
            for a, tile in enumerate(mix_blocks(tiles)):
                own_ref[which, k * 8 + a] = tile


def row_faces(face_ref, row):
    idx = (row + 8) // 16
    kap = face_ref[idx, 3]
    south = face_ref[idx, 1] if row % 16 == 8 else kap
    north = face_ref[idx, 2] if row % 16 == 7 else kap
    return face_ref[idx, 0], south, north


def vertical(source, row, faces):
    _, south, north = faces
    if row % 16 in (7, 8):
        return south * source[row - 1] + north * source[row + 1]
    return south * (source[row - 1] + source[row + 1])


def apply_rows(source, lo, hi, blocks, stencil_ref, face_ref, diff, emit):
    for idx in range(6):
        first, last = max(lo, idx * 16 - 8), min(hi, idx * 16 + 8)
        if first >= last:
            continue
        start, stop = first - first % 2, last + last % 2
        parts = []
        for row in range(start, stop, 2):
            x = source[row : row + 2].reshape(48, LANES)
            high = x.astype(bf16)
            parts.append((high, (x - high.astype(f32)).astype(bf16)))
        beside = jnp.dot(
            jnp.concatenate([jnp.concatenate(part, axis=1) for part in parts], axis=0),
            stencil_ref[idx],
            preferred_element_type=f32,
        ).reshape(stop - start, 3, 8, LANES)
        mixed = []
        for at in range(0, len(parts), 2):
            group = parts[at : at + 2]
            high = jnp.concatenate([part[0] for part in group], axis=1)
            low = jnp.concatenate([part[1] for part in group], axis=1)
            m = jnp.dot(
                blocks, jnp.concatenate([high, low, high], axis=0), preferred_element_type=f32
            ).reshape(2, 3, 8, len(group) * LANES)
            for pair in range(len(group)):
                for off in range(2):
                    mixed.append(m[off, :, :, pair * LANES : (pair + 1) * LANES])
        for row in range(first, last):
            faces = row_faces(face_ref, row)
            near = beside[row - start] + vertical(source, row, faces)
            emit(row, faces, diff * near + mixed[row - start])


PAIRS = [(i, j) for j in range(4) for i in range(j + 1)]


class Dots:
    def __init__(self, packed_ref):
        self.sums = {}
        self.packed_ref = packed_ref
        self.half = None
        lane = lanes_of()
        self.own = (lane >= 32) & (lane < 80)
        self.both = self.own | (lane >= 96) | (lane < 16)

    def add(self, basis, row, value):
        if not OWN_LO <= row < OWN_HI:
            return
        if row % 2 == 0:
            self.half = value
            return
        at = (row - OWN_LO) // 2
        value = jnp.where(self.own, self.half, roll(value, 64))
        if basis < 3:
            self.packed_ref[basis, at] = value
        for before in range(basis + 1):
            other = value if before == basis else self.packed_ref[before, at]
            key, term = (before, basis), other * value
            self.sums[key] = self.sums[key] + term if key in self.sums else term

    def write(self, out_ref):
        lane = lanes_of((1, LANES))
        total = jnp.zeros((1, LANES), f32)
        for at, key in enumerate(PAIRS):
            value = jnp.where(self.both, jnp.sum(self.sums[key], axis=0), 0.0)
            value = jnp.sum(jnp.sum(value, axis=0, keepdims=True), axis=1, keepdims=True)
            total = jnp.where(lane == at, value, total)
        out_ref[...] = total


PACKED = (3, (OWN_HI - OWN_LO) // 2, 3, 8, LANES)


def krylov(refs, diag_ref, tables, diff, dots, reach, last_ref):
    for k in range(3):
        source, target = refs[k], last_ref if k == 2 else refs[k + 1]
        width = reach - k - 1
        lo, hi = OWN_LO - width, OWN_HI + width

        def emit(row, faces, rest, source=source, target=target, k=k):
            new = diag_ref[row] * source[row] - rest
            if target is not None:
                target[row] = new
            dots.add(k + 1, row, new)

        apply_rows(source, lo, hi, *tables, diff, emit)


def row_base(face_ref, rate, diff):
    cache = {}

    def base(row):
        kind = ((row + 8) // 16, {7: 1, 8: 2}.get(row % 16, 0))
        if kind not in cache:
            beside, south, north = row_faces(face_ref, row)
            cache[kind] = rate + diff * (beside + (south + north))
        return cache[kind]

    return base


def first_kernel(
    own_ref, inner1_ref, inner2_ref, corner1_ref, corner2_ref, face_ref, stencil_ref, param_ref, block_ref,
    state_ref, p0_ref, p1_ref, p2_ref, p3_ref, gram_ref, old_ref, diag_ref, packed_ref,
):
    _, owner = position()
    even_owner, has_left, has_right = owner % 2 == 0, owner > 0, owner < OWNERS - 1
    blank = jnp.zeros((3, 8, LANES), f32)
    for which, target in enumerate((state_ref, old_ref)):

        def beside(refs, at):
            first, second = (get_tile(ref, at).reshape(3, 8, LANES) for ref in refs)
            left, right = jnp.where(even_owner, second, first), jnp.where(even_owner, first, second)
            return jnp.where(has_left, left, 0.0), jnp.where(has_right, right, 0.0)

        for k in range(TILES):
            if k in (0, TILES - 1):
                refs, at = (corner1_ref, corner2_ref), which * CORNER + (k > 0)
                pair, high = which * CORNER + 2, k > 0
            else:
                refs, at = (inner1_ref, inner2_ref), which * INNER + k - 1
                pair, high = which * INNER + 2 * ROWS_DEV + (k - 1) // 2, k % 2 == 0
            left, right = beside(refs, at)
            if k in (0, TILES - 1) or not high:
                far = beside(refs, pair)
            far_left, far_right = far
            tiles = mix_blocks(
                [
                    far_left if high else roll(far_left, 8),
                    roll(left, 16),
                    blank,
                    blank,
                    blank,
                    roll(right, 80),
                    roll(far_right, 88 if high else 96),
                    blank,
                ]
            )
            for a in range(8):
                tile = tiles[-a % 8] + own_ref[which, k * 8 + (-a % 8)]
                target[k * 8 + a] = roll(tile, -16 * a) if a else tile
    rate, diff, decay = param_ref[0], param_ref[1], param_ref[2]
    tables = (block_ref[:, 0:144], stencil_ref, face_ref)
    dots = Dots(packed_ref)
    base_of = row_base(face_ref, rate, diff)

    def emit(row, faces, rest):
        u = state_ref[row]
        base = base_of(row)
        cubic = decay * (u * u)
        new = (base + cubic) * u - rate * old_ref[row] - rest
        diag_ref[row] = (base - THETA / SIGMA) + 3.0 * cubic
        p0_ref[row] = new
        dots.add(0, row, new)

    apply_rows(state_ref, 2, 78, *tables, diff, emit)
    krylov((p0_ref, p1_ref, p2_ref), diag_ref, tables, diff, dots, 6, p3_ref)
    dots.write(gram_ref)


def small_solve(matrix, vector):
    matrix = [list(row) for row in matrix]
    vector = list(vector)
    size = len(vector)
    for col in range(size):
        for target in range(col + 1, size):
            factor = matrix[target][col] / matrix[col][col]
            for at in range(col, size):
                matrix[target][at] = matrix[target][at] - factor * matrix[col][at]
            vector[target] = vector[target] - factor * vector[col]
    answer = [None] * size
    for col in reversed(range(size)):
        running = vector[col]
        for later in range(col + 1, size):
            running = running - matrix[col][later] * answer[later]
        answer[col] = running / matrix[col][col]
    return answer


def combine(parts_ref):
    totals = jnp.sum(parts_ref[...], axis=0, keepdims=True)
    gram = [[None] * 4 for _ in range(4)]
    for at, (i, j) in enumerate(PAIRS):
        gram[i][j] = gram[j][i] = jnp.broadcast_to(totals[:, at : at + 1], (8, LANES))
    zero = jnp.zeros((8, LANES), f32)
    beta = jnp.sqrt(gram[0][0] * (SIGMA * SIGMA) + EPSILON)
    basis = [[-SIGMA / beta]]
    hess = [[zero] * 3 for _ in range(4)]

    def dot(x, y):
        total = x[0] * y[0]
        for at in range(1, len(x)):
            total = total + x[at] * y[at]
        return total

    for j in range(3):
        last = basis[j]
        w = [THETA * last[at] for at in range(j + 1)] + [SIGMA * last[j]]
        for at in range(j):
            w[at + 1] = w[at + 1] + SIGMA * last[at]
        gw = [dot(w, gram[at]) for at in range(j + 2)]
        size = dot(w, gw)
        for i in range(j + 1):
            hess[i][j] = dot(basis[i], gw)
        for i in range(j + 1):
            for at in range(i + 1):
                w[at] = w[at] - hess[i][j] * basis[i][at]
        rest = dot(w, [dot(w, gram[at]) for at in range(j + 2)])
        alive = rest > BREAKDOWN * size
        height = jnp.sqrt(jnp.where(alive, rest, 0.0) + EPSILON)
        hess[j + 1][j] = height
        basis.append([jnp.where(alive, value / height, 0.0) for value in w])
    normal = [[dot([h[i] for h in hess], [h[j] for h in hess]) for j in range(3)] for i in range(3)]
    y = small_solve(normal, [beta * hess[0][i] for i in range(3)])
    out = []
    for at in range(3):
        total = None
        for j in range(at, 3):
            term = y[j] * basis[j][at]
            total = term if total is None else total + term
        out.append(total)
    return out


def second_kernel(
    parts_ref, state_ref, p0_ref, p1_ref, p2_ref, p3_ref, face_ref, stencil_ref, param_ref,
    block_ref, next_ref, q0_ref, q1_ref, q2_ref, gram_ref, diag_ref, packed_ref,
):
    c0, c1, c2 = combine(parts_ref)
    shift = THETA / SIGMA
    rate, diff, decay = param_ref[0], param_ref[1], param_ref[2]
    tables = (block_ref[:, 0:144], stencil_ref, face_ref)
    dots = Dots(packed_ref)
    base_of = row_base(face_ref, rate - shift, diff)
    a0, a1, a2 = 1.0 + shift * c0, c0 + shift * c1, c1 + shift * c2
    triple = 3.0 * decay
    for row in range(5, 75):
        p0, p1, p2, u = p0_ref[row], p1_ref[row], p2_ref[row], state_ref[row]
        d = c0 * p0 + c1 * p1 + c2 * p2
        linear = (a0 * p0 + a1 * p1) + (a2 * p2 + c2 * p3_ref[row])
        new = linear + (decay * (d * d)) * (3.0 * u + d)
        u = u + d
        diag_ref[row] = base_of(row) + triple * (u * u)
        next_ref[row] = u
        q0_ref[row] = new
        dots.add(0, row, new)
    krylov((q0_ref, q1_ref, q2_ref), diag_ref, tables, diff, dots, 3, None)
    dots.write(gram_ref)


SLOTS = PATCH_DEV + 2 * MOVE_CAP


def last_kernel(
    parts_ref, next_ref, q0_ref, q1_ref, q2_ref, flag_ref, out_hbm, low_ref, high_ref, out_ref, sems
):
    c0, c1, c2 = combine(parts_ref)
    slots_ref = (low_ref, high_ref)
    blank = jnp.zeros((3, 8, LANES), f32)

    def put(half, slot, tile):
        slots_ref[half][slot * 24 : slot * 24 + 24, :] = tile.reshape(24, LANES)

    copies = [
        pltpu.make_async_copy(
            out_ref.at[:, pl.ds(part * 8, 8), :], out_hbm.at[:, pl.ds(part * 8, 8), :], sems.at[part]
        )
        for part in range(SLOTS // 8)
    ]

    def send(part):
        for s in range(SPECIES):
            for half in range(2):
                out_ref[s, part * 8 : part * 8 + 8, half * LANES : (half + 1) * LANES] = slots_ref[
                    half
                ][pl.ds(part * 8 * 24 + s, 8, stride=24), :]
        copies[part].start()

    arrived = {}
    for r in range(ROWS_DEV):
        if r * COLS_DEV >= 8:
            send(0)
        for half in range(2):
            rows = []
            for a in range(8):
                row = OWN_LO + r * 16 + half * 8 + a
                value = next_ref[row] + (c0 * q0_ref[row] + c1 * q1_ref[row] + c2 * q2_ref[row])
                rows.append(roll(value, 16 * a) if a else value)
            tiles = swap_blocks(rows, range(1, 6))
            for c in range(COLS_DEV):
                slot = r * COLS_DEV + c
                put(half, slot, jnp.where(flag_ref[slot] == 1, tiles[2 + c], 0.0))
            for side, g in enumerate((1, 5)):
                for at, (row_of, m) in enumerate(ARRIVALS):
                    if row_of == r:
                        flag = flag_ref[STAYS + side * len(ARRIVALS) + at] == 1
                        key = (half, PATCH_DEV + side * MOVE_CAP + m)
                        arrived[key] = jnp.where(flag, tiles[g], arrived.get(key, blank))
    for (half, slot), tile in arrived.items():
        put(half, slot, tile)

    send(1)
    for copy in copies:
        copy.wait()


def call(kernel, out_shape, in_specs, scratch=(), limit=16, out_space=pltpu.VMEM):
    return pl.pallas_call(
        kernel,
        out_shape=out_shape,
        in_specs=in_specs,
        out_specs=jax.tree.map(lambda _: pl.BlockSpec(memory_space=out_space), out_shape),
        scratch_shapes=list(scratch),
        compiler_params=pltpu.CompilerParams(vmem_limit_bytes=limit << 20),
    )


def vm():
    return pl.BlockSpec(memory_space=pltpu.VMEM)


def sm():
    return pl.BlockSpec(memory_space=pltpu.SMEM)


def in_hbm(x):
    return pltpu.with_memory_space_constraint(x, pltpu.HBM)


def exchanged(x, along_bands, odd):

    def mate(owner, band):
        at, count = (band, BANDS) if along_bands else (owner, OWNERS)
        near = ((at - odd) ^ 1) + odd
        if not 0 <= near < count:
            return (owner ^ 1, band) if along_bands else (owner, band ^ 1)
        return (owner, near) if along_bands else (near, band)

    pairs = []
    for owner in range(OWNERS):
        for band in range(BANDS):
            to_owner, to_band = mate(owner, band)
            pairs.append((owner * BANDS + band, to_owner * BANDS + to_band))
    return lax.ppermute(x, EVERY, pairs)


def swapped(pair, along_bands):
    out = []
    for odd, x in enumerate(pair):
        out.append(exchanged(x, along_bands, odd))
    return out


def summed(gram):
    spread_out = jnp.broadcast_to(gram[None], (DEVICES, 1, LANES))
    return lax.all_to_all(spread_out, EVERY, 0, 0).reshape(DEVICES, LANES)


def per_device(previous, predicted, new_owner, levels, diffusion, decay, reaction):
    prev, pred = (x.reshape(PATCH_DEV * SPECIES * 2, LANES) for x in (previous, predicted))
    shape = jax.ShapeDtypeStruct
    strip = shape((dense(ROW_TILES), LANES), f32)
    local = shape((INPUT_ROWS + 8, LANES), f32)
    far = pl.BlockSpec(memory_space=pltpu.HBM)
    inner, corner = (shape((dense(2 * count), LANES), f32) for count in (INNER, CORNER))
    pred, prev, *strips = call(
        strip_kernel,
        (local, local, strip, strip, inner, inner),
        [far, far],
        [pltpu.SemaphoreType.DMA((6,))],
    )(in_hbm(pred), in_hbm(prev))
    row1, row2 = swapped(strips[:2], True)
    inner_cols = swapped(strips[2:], False)
    corners = call(corner_kernel, (corner, corner), [vm()] * 2)(row1, row2)

    inputs = (new_owner, levels, diffusion, decay, reaction)
    corners, inputs = lax.optimization_barrier((tuple(corners), inputs))
    new_owner, levels, diffusion, decay, reaction = inputs
    corner_cols = swapped(corners, False)
    faces, stencil, flags, params, blocks = call(
        table_kernel,
        (
            shape((6, 4, 8, LANES), f32),
            shape((6, 2 * LANES, LANES), bf16),
            shape((FLAGS, 8, LANES), jnp.int32),
            shape((3, 3, 8, LANES), f32),
            shape((48, 2 * LANES), bf16),
        ),
        [sm()] * 4 + [vm()],
        [pltpu.VMEM((24, LANES), f32)],
    )(
        *(
            in_hbm(x)
            for x in (
                levels.transpose(2, 0, 1),
                new_owner.transpose(2, 0, 1),
                diffusion,
                decay,
                reaction,
            )
        )
    )
    state = shape(STATE, f32)
    gram = shape((1, LANES), f32)
    own = call(
        own_kernel,
        shape((2,) + STATE, f32),
        [vm()] * 4,
        [pltpu.VMEM((2 * TILES * COLS_DEV, 24, LANES), f32)],
    )(pred, prev, row1, row2)
    u0, p0, p1, p2, p3, gram1 = call(
        first_kernel,
        (state,) * 5 + (gram,),
        [vm()] * 9,
        [pltpu.VMEM(STATE, f32), pltpu.VMEM(STATE, f32), pltpu.VMEM(PACKED, f32)],
    )(own, *inner_cols, *corner_cols, faces, stencil, params, blocks)
    u1, q0, q1, q2, gram2 = call(
        second_kernel,
        (state,) * 4 + (gram,),
        [vm()] * 10,
        [pltpu.VMEM(STATE, f32), pltpu.VMEM(PACKED, f32)],
    )(summed(gram1), u0, p0, p1, p2, p3, faces, stencil, params, blocks)
    out = call(
        last_kernel,
        shape((SPECIES, SLOTS, 2 * LANES), f32),
        [vm()] * 6,
        [pltpu.VMEM((SLOTS * 24, LANES), f32)] * 2
        + [pltpu.VMEM((SPECIES, SLOTS, 2 * LANES), f32), pltpu.SemaphoreType.DMA((2,))],
        out_space=pltpu.HBM,
    )(summed(gram2), u1, q0, q1, q2, flags)
    return jnp.transpose(out, (1, 0, 2))[None, None]


def solution(mesh):
    torus = Mesh(
        mesh.devices.reshape(4, 4, 2, mesh.shape["grp"]), ("patch_0", "patch_1", "patch_2", "grp")
    )
    spec = P("grp", PATCH, None, None, None)
    in_specs = (spec, spec, P(), P(), P(), P(), P())
    return jax.shard_map(
        per_device, mesh=torus, in_specs=in_specs, out_specs=spec, check_vma=False
    )
```
